32 devices in a mesh: dp: 16 (over z, x, core), seq: 2 (over y).
Axes of the slice: x: 2, y: 2, z: 4, core: 2. Of those that a mesh axis runs over, the one named last changes fastest.
Arguments:
- tokens: float32 [16384, 1024], P(('dp', 'seq')), may hold values from -6 to 6
- lengths: int32 [16, 1], P('dp'), may hold values from 1024 to 1024, as said below
- attn_gain: bfloat16 [1024], P('dp'), may hold values from 0.5 to 1.5
- w_query: bfloat16 [1024, 1024], P('dp'), may hold values from -0.1875 to 0.1875
- w_key: bfloat16 [1024, 512], P('dp'), may hold values from -0.1875 to 0.1875
- w_value: bfloat16 [1024, 512], P('dp'), may hold values from -0.1875 to 0.1875
- query_gain: bfloat16 [64], P('dp'), may hold values from 1 to 2
- key_gain: bfloat16 [64], P('dp'), may hold values from 0.5 to 1.5
- w_out: bfloat16 [1024, 1024], P('dp'), may hold values from -1.5 to 1.5
- ffn_gain: bfloat16 [1024], P('dp'), may hold values from 0.5 to 1.5
- w_gate: bfloat16 [1024, 4608], P('dp'), may hold values from -0.1875 to 0.1875
- w_up: bfloat16 [1024, 4608], P('dp'), may hold values from -0.1875 to 0.1875
- w_down: bfloat16 [4608, 1024], P('dp'), may hold values from -0.09375 to 0.09375
- cotangent: float32 [16384, 1024], P(('dp', 'seq')), may hold values from -6 to 6
Outputs:
- block_out: float32 [16384, 1024], P(('dp', 'seq'))
- d_tokens: float32 [16384, 1024], P(('dp', 'seq'))
- d_attn_gain: float32 [1024], P('dp')
- d_w_query: float32 [1024, 1024], P('dp')
- d_w_key: float32 [1024, 512], P('dp')
- d_w_value: float32 [1024, 512], P('dp')
- d_query_gain: float32 [64], P('dp')
- d_key_gain: float32 [64], P('dp')
- d_w_out: float32 [1024, 1024], P('dp')
- d_ffn_gain: float32 [1024], P('dp')
- d_w_gate: float32 [1024, 4608], P('dp')
- d_w_up: float32 [1024, 4608], P('dp')
- d_w_down: float32 [4608, 1024], P('dp')
The draws below stay inside these ranges and needn't reach their ends.
Inputs may be any that keep to these rules, and one draw needn't show every extreme that they name: `lengths`: every length is at least 1024; in every draw one pack, drawn from the seed, has every sequence of length 1024 and no padding.
All inputs are finite; a program needn't handle non-finite values.
Results may differ from the reference program's by a relative error of at most 0.02.
Values may be sent and summed in bfloat16 or wider, within the bound.
No kernel may reach another device: no remote copies, remote signals or barrier semaphores. Data moves between devices by JAX's collectives and lax.ppermute only.
A program may use at most 192 MiB of HBM per device.

```python
import math
import jax
import jax.numpy as jnp
from jax import lax

D = 1024
H = 16
KV = 8
HD = 64
FF = 4608
MINLEN = 1024
QW = 1024
KW = 512
PACK = 1024
SEQS = 1
PACKS = 16
TOKENS = 16384


def draw_lengths(key, part):
    top_len = PACK // SEQS
    drawn = jax.random.randint(jax.random.fold_in(key, 11), (PACKS, SEQS), MINLEN, top_len + 1, dtype=jnp.int32)
    full_pack = jax.random.randint(jax.random.fold_in(key, 12), (), 0, PACKS, dtype=jnp.int32)
    chosen = jnp.arange(PACKS, dtype=jnp.int32)[:, None] == full_pack
    return jnp.where(chosen, jnp.int32(top_len), drawn).astype(jnp.int32)


def block_levels(rng, extent, pieces, least, largest):
    factor_of, own = 1.0, jax.random.fold_in(rng, 6)
    for position, blocks in pieces:
        steps = jnp.exp(jax.random.uniform(jax.random.fold_in(own, position), (blocks,), jnp.float32, least / len(pieces), largest / len(pieces)))
        factor_of = factor_of * jnp.repeat(steps, extent[position] // blocks).reshape([-1 if axis == position else 1 for axis in range(len(extent))])
    return factor_of


def scatter_about(stream_key, shape, width, most, shards=(), kind=jnp.bfloat16):
    values = jax.random.normal(stream_key, shape, jnp.float32) * width
    if len(shards) > 0:
        values = block_levels(stream_key, shape, shards, -0.22, 0.18) * values
    return jnp.clip(values, min=-most, max=most).astype(kind)


def setup_inputs(seed: int = 0) -> dict:
    keys = jax.random.split(jax.random.key(seed), 15)
    return {
        "tokens": scatter_about(keys[0], (TOKENS, D), 1.0, 6.0, ((0, 32),), jnp.float32),
        "lengths": draw_lengths(jax.random.fold_in(keys[14], 71), 0),
        "attn_gain": jnp.clip(1.0 + 0.1 * jax.random.normal(keys[2], (D,), jnp.float32), 0.5, 1.5).astype(jnp.bfloat16),
        "w_query": scatter_about(keys[3], (D, QW), D ** -0.5, 0.1875, ((0, 16),)),
        "w_key": scatter_about(keys[4], (D, KW), D ** -0.5, 0.1875, ((0, 16),)),
        "w_value": scatter_about(keys[5], (D, KW), D ** -0.5, 0.1875, ((0, 16),)),
        "query_gain": jnp.clip(jnp.exp(math.log(2.0) - 0.6931472 * jax.random.uniform(keys[6], (HD,), jnp.float32) ** block_levels(keys[6], (HD,), ((0, 16),), -0.2, 0.2)), 1.0, 2.0).astype(jnp.bfloat16),
        "key_gain": jnp.clip(1.0 + 0.1 * jax.random.normal(keys[7], (HD,), jnp.float32), 0.5, 1.5).astype(jnp.bfloat16),
        "w_out": scatter_about(keys[8], (QW, D), (HD // 4) ** -0.5, 1.5, ((0, 16),)),
        "ffn_gain": jnp.clip(1.0 + 0.1 * jax.random.normal(keys[9], (D,), jnp.float32), 0.5, 1.5).astype(jnp.bfloat16),
        "w_gate": scatter_about(keys[10], (D, FF), D ** -0.5, 0.1875, ((0, 16),)),
        "w_up": scatter_about(keys[11], (D, FF), D ** -0.5, 0.1875, ((0, 16),)),
        "w_down": scatter_about(keys[12], (FF, D), FF ** -0.5, 0.09375, ((0, 16),)),
        "cotangent": scatter_about(keys[13], (TOKENS, D), 1.0, 6.0, ((0, 32),), jnp.float32),
    }


@jax.custom_vjp
def low(v):
    return lax.optimization_barrier(v.astype(jnp.bfloat16)).astype(jnp.float32)

@jax.custom_vjp
def low_back(v):
    return v

def low_keep(v):
    return (low(v), None)

def low_pass(kept, grad):
    return (grad,)

def back_keep(v):
    return (v, None)

def back_low(kept, grad):
    return (low(grad),)
low.defvjp(low_keep, low_pass)
low_back.defvjp(back_keep, back_low)
EPSILON = 1e-05
ROPE_BASE = 1000000.0
MASKED_SCORE = -1e+30

def dot_high(left, right):
    return jnp.dot(left, right, precision=lax.Precision.HIGHEST, preferred_element_type=jnp.float32)

def rms_norm(values, gain_vec):
    return values * lax.rsqrt(lax.optimization_barrier(jnp.mean(values * values, axis=-1, keepdims=True)) + EPSILON) * gain_vec

def rope_tables(positions, head_size):
    half_size = head_size // 2
    freqs = ROPE_BASE ** (-(jnp.arange(half_size, dtype=jnp.float32) * (2.0 / head_size)))
    angles = positions.astype(jnp.float32)[:, None] * freqs[None, :]
    return (jnp.cos(angles), jnp.sin(angles))

def rotate(values, cos_tab, sin_tab):
    half_size = values.shape[-1] // 2
    first = values[..., :half_size]
    second = values[..., half_size:]
    cos_b = cos_tab[:, None, :]
    sin_b = sin_tab[:, None, :]
    return jnp.concatenate([first * cos_b - second * sin_b, second * cos_b + first * sin_b], axis=-1)

def qk_prep(linear, gain_vec, cos_tab, sin_tab, heads):
    shaped = linear.reshape(linear.shape[0], heads, -1)
    return rotate(rms_norm(shaped, gain_vec), cos_tab, sin_tab)

def swiglu(gate_act, up_act):
    return jax.nn.silu(gate_act) * up_act

def pack_layout(seq_lens, total):
    places = jnp.arange(total, dtype=jnp.int32)
    ends = jnp.cumsum(seq_lens).astype(jnp.int32)
    starts = (ends - seq_lens).astype(jnp.int32)
    segment = lax.optimization_barrier(jnp.sum((places[:, None] >= ends[None, :]).astype(jnp.int32), axis=1)).astype(jnp.int32)
    starts_ext = jnp.concatenate([starts, ends[-1:]]).astype(jnp.int32)
    labels = jnp.arange(seq_lens.shape[0] + 1, dtype=jnp.int32)
    offset = lax.optimization_barrier(jnp.sum(jnp.where(segment[:, None] == labels[None, :], starts_ext[None, :], 0), axis=1)).astype(jnp.int32)
    return (places, segment, (places - offset).astype(jnp.int32), segment < seq_lens.shape[0])

def block_forward(x_in, weights, places, segment, positions, valid):
    gain_attn, query_w, key_w, value_w, gain_query, gain_key, out_w, gain_ffn, gate_w, up_w, down_w = weights
    rows = x_in.shape[0]
    group = H // KV
    score_scale = 1.0 / math.sqrt(HD)
    normed = low(rms_norm(x_in, gain_attn))
    cos_tab, sin_tab = rope_tables(positions, HD)
    queries = low(low_back(qk_prep(low_back(dot_high(normed, query_w)), gain_query, cos_tab, sin_tab, H)))
    key_rows = low(low_back(qk_prep(low_back(dot_high(normed, key_w)), gain_key, cos_tab, sin_tab, KV)))
    value_rows = low(low_back(dot_high(normed, value_w))).reshape(rows, KV, HD)
    blk_rows = min(512, rows)
    blocks = rows // blk_rows
    query_blocks = queries.reshape(blocks, blk_rows, KV, group, HD)

    def attend(inputs):
        query_blk, seg_blk, place_blk = inputs
        scores = jnp.einsum('qkgd,skd->kgqs', query_blk, key_rows, precision=lax.Precision.HIGHEST) * score_scale
        scores = low_back(scores)
        allowed = (seg_blk[:, None] == segment[None, :]) & (places[None, :] <= place_blk[:, None])
        scores = jnp.where(allowed[None, None], scores, MASKED_SCORE)
        top_val = lax.optimization_barrier(jnp.max(scores, axis=-1, keepdims=True))
        expo = jnp.exp(scores - top_val)
        probs = low(expo / lax.optimization_barrier(jnp.sum(expo, axis=-1, keepdims=True)))
        return jnp.einsum('kgqs,skd->qkgd', probs, value_rows, precision=lax.Precision.HIGHEST)
    attended = lax.map(jax.checkpoint(attend), (query_blocks, segment.reshape(blocks, blk_rows), places.reshape(blocks, blk_rows)))
    attended = low(low_back(attended.reshape(rows, H * HD)))
    resid = x_in + low_back(dot_high(attended, out_w))
    ffn_in = low(rms_norm(resid, gain_ffn))
    gate_act = low_back(dot_high(ffn_in, gate_w))
    up_act = low_back(dot_high(ffn_in, up_w))
    hidden = low(swiglu(gate_act, up_act))
    result = resid + low_back(dot_high(hidden, down_w))
    return result * valid.astype(jnp.float32)[:, None]

def reference(tokens, lengths, attn_gain, w_query, w_key, w_value, query_gain, key_gain, w_out, ffn_gain, w_gate, w_up, w_down, cotangent):
    params = tuple((param.astype(jnp.float32) for param in (attn_gain, w_query, w_key, w_value, query_gain, key_gain, w_out, ffn_gain, w_gate, w_up, w_down)))
    packs = lengths.shape[0]
    pack_len = tokens.shape[0] // packs
    x_packs = tokens.reshape(packs, pack_len, -1)
    cot_packs = cotangent.reshape(packs, pack_len, -1)

    def one_pack(totals, inputs):
        x_pack, cot_pack, seq_lens = inputs
        places, segment, positions, valid = pack_layout(seq_lens, pack_len)

        def forward(x_in, *weights):
            return block_forward(x_in, weights, places, segment, positions, valid)
        result, pull = jax.vjp(forward, x_pack, *params)
        grads = pull(cot_pack)
        totals = tuple((old_sum + new_grad for old_sum, new_grad in zip(totals, grads[1:])))
        return (totals, (result, grads[0]))
    zeros = tuple((jnp.zeros_like(param) for param in params))
    totals, (results, d_input) = lax.scan(one_pack, zeros, (x_packs, cot_packs, lengths))
    return (results.reshape(tokens.shape), d_input.reshape(tokens.shape), totals[0], totals[1], totals[2], totals[3], totals[4], totals[5], totals[6], totals[7], totals[8], totals[9], totals[10])
```

```python
from functools import partial
import math

import jax
import jax.numpy as jnp
from jax import lax
from jax.experimental import pallas as pl
from jax.experimental.pallas import tpu as pltpu
from jax.sharding import PartitionSpec as P

H = 16
KV = 8
HD = 64
GROUP = H // KV
MINLEN = 1024

EPSILON = 1e-05
ROPE_BASE = 1000000.0
MASKED_SCORE = -1e30
BF = jnp.bfloat16
F32 = jnp.float32


def dot(left, right, lc, rc):
    return lax.dot_general(left, right, (((lc,), (rc,)), ((), ())), preferred_element_type=F32)


def masked(scores, q0, k0, segs):
    row = lax.broadcasted_iota(jnp.int32, scores.shape, 0) + k0
    col = lax.broadcasted_iota(jnp.int32, scores.shape, 1) + q0
    allowed = row <= col
    if segs is not None:
        allowed = allowed & (segs[0] == segs[1])
    return jnp.where(allowed, scores, MASKED_SCORE)


def attn_fwd_kernel(blk, static, *refs):
    if static:
        q_ref, k_ref, v_ref, o_ref, lse_ref = refs
    else:
        q_ref, k_ref, v_ref, sc_ref, sr_ref, o_ref, lse_ref = refs
    length = q_ref.shape[1]
    keys = k_ref[...].T

    def finish(q0, parts):
        top = parts[0][0].max(axis=0, keepdims=True)
        for s, _ in parts[1:]:
            top = jnp.maximum(top, s.max(axis=0, keepdims=True))
        total, out = 0.0, 0.0
        for s, v in parts:
            p = jnp.exp(s - top)
            total = total + p.sum(axis=0, keepdims=True)
            out = out + dot(v, p.astype(BF), 1, 0)
        o_ref[:, pl.ds(q0, blk)] = (out / total).astype(BF)
        lse_ref[0, :, pl.ds(q0, blk)] = top + jnp.log(total)

    if static:
        for qb in range(length // blk):
            q0 = qb * blk
            q = q_ref[:, q0 : q0 + blk]
            parts = []
            if qb:
                parts.append((dot(keys[:q0], q, 1, 0), v_ref[:, :q0]))
            diag = masked(dot(keys[q0 : q0 + blk], q, 1, 0), 0, 0, None)
            parts.append((diag, v_ref[:, q0 : q0 + blk]))
            finish(q0, parts)
    else:

        @pl.loop(0, length // blk)
        def _(qb):
            q0 = pl.multiple_of(qb * blk, blk)
            s = dot(keys, q_ref[:, pl.ds(q0, blk)], 1, 0)
            s = masked(s, q0, 0, (sc_ref[...], sr_ref[:, pl.ds(q0, blk)]))
            finish(q0, [(s, v_ref[...])])


def attn_bwd_kernel(blk, static, *refs):
    if static:
        q_ref, k_ref, v_ref, do_ref, o_ref, lse_ref, dq_ref, dk_ref, dv_ref, dk_acc, dv_acc = refs
    else:
        (q_ref, k_ref, v_ref, do_ref, o_ref, lse_ref, sc_ref, sr_ref,
         dq_ref, dk_ref, dv_ref, dk_acc, dv_acc) = refs
    length = q_ref.shape[1]
    member = lax.rem(pl.program_id(0), GROUP)
    keys = k_ref[...].T
    values = v_ref[...].T

    @pl.when(member == 0)
    def _():
        dk_acc[...] = jnp.zeros_like(dk_acc)
        dv_acc[...] = jnp.zeros_like(dv_acc)

    def part(q, d_out, lse, delta, k_lo, k_n, q0, segs, mask):
        rows = pl.ds(k_lo, k_n)
        k_blk, v_blk = keys[k_lo : k_lo + k_n], values[k_lo : k_lo + k_n]
        s = dot(k_blk, q, 1, 0)
        if mask:
            s = masked(s, q0, k_lo, segs)
        p = jnp.exp(s - lse)
        dv_acc[rows, :] += dot(p.astype(BF), d_out, 1, 1)
        dp = dot(v_blk, d_out, 1, 0)
        ds = (p * (dp - delta)).astype(BF)
        dk_acc[rows, :] += dot(ds, q, 1, 1)
        return dot(k_ref[:, rows], ds, 1, 0)

    def prepare(q0):
        cols = pl.ds(q0, blk)
        d_out = do_ref[:, cols]
        delta = (d_out.astype(F32) * o_ref[:, cols].astype(F32)).sum(axis=0, keepdims=True)
        return cols, q_ref[:, cols], d_out, lse_ref[0, :, cols], delta

    scale = 1.0 / math.sqrt(HD)
    if static:
        for qb in range(length // blk):
            q0 = qb * blk
            cols, q, d_out, lse, delta = prepare(q0)
            dq = part(q, d_out, lse, delta, q0, blk, q0, None, True)
            if qb:
                dq = dq + part(q, d_out, lse, delta, 0, q0, q0, None, False)
            dq_ref[:, cols] = (dq * scale).astype(BF)
    else:

        @pl.loop(0, length // blk)
        def _(qb):
            q0 = pl.multiple_of(qb * blk, blk)
            cols, q, d_out, lse, delta = prepare(q0)
            dq = part(q, d_out, lse, delta, 0, length, q0, (sc_ref[...], sr_ref[:, cols]), True)
            dq_ref[:, cols] = (dq * scale).astype(BF)

    @pl.when(member == GROUP - 1)
    def _():
        dk_ref[...] = dk_acc[...].T.astype(BF)
        dv_ref[...] = dv_acc[...].T.astype(BF)


def attn_specs(length):
    q_spec = pl.BlockSpec((HD, length), lambda h: (h, 0))
    kv_spec = pl.BlockSpec((HD, length), lambda h: (h // GROUP, 0))
    lse_spec = pl.BlockSpec((1, 1, length), lambda h: (h, 0, 0))
    seg_specs = [
        pl.BlockSpec((length, 1), lambda h: (0, 0)),
        pl.BlockSpec((1, length), lambda h: (0, 0)),
    ]
    return q_spec, kv_spec, lse_spec, seg_specs


def attn_fwd(q, k, v, segs):
    rows, length = q.shape
    heads = rows // HD
    static = segs is None
    q_spec, kv_spec, lse_spec, seg_specs = attn_specs(length)
    extra = () if static else (segs[:, None], segs[None, :])
    return pl.pallas_call(
        partial(attn_fwd_kernel, min(256, length), static),
        grid=(heads,),
        in_specs=[q_spec, kv_spec, kv_spec] + ([] if static else seg_specs),
        out_specs=[q_spec, lse_spec],
        out_shape=[
            jax.ShapeDtypeStruct((rows, length), BF),
            jax.ShapeDtypeStruct((heads, 1, length), F32),
        ],
        cost_estimate=pl.CostEstimate(
            flops=4 * heads * length * length * HD,
            transcendentals=heads * length * length,
            bytes_accessed=4 * rows * length * 2,
        ),
        name="attn_fwd",
    )(q, k, v, *extra)


def attn_bwd(q, k, v, d_out, out, lse, segs):
    rows, length = q.shape
    heads = rows // HD
    static = segs is None
    q_spec, kv_spec, lse_spec, seg_specs = attn_specs(length)
    extra = () if static else (segs[:, None], segs[None, :])
    return pl.pallas_call(
        partial(attn_bwd_kernel, min(256, length), static),
        grid=(heads,),
        in_specs=[q_spec, kv_spec, kv_spec, q_spec, q_spec, lse_spec]
        + ([] if static else seg_specs),
        out_specs=[q_spec, kv_spec, kv_spec],
        out_shape=[
            jax.ShapeDtypeStruct((rows, length), BF),
            jax.ShapeDtypeStruct(k.shape, BF),
            jax.ShapeDtypeStruct(v.shape, BF),
        ],
        scratch_shapes=[pltpu.VMEM((length, HD), F32), pltpu.VMEM((length, HD), F32)],
        cost_estimate=pl.CostEstimate(
            flops=10 * heads * length * length * HD,
            transcendentals=heads * length * length,
            bytes_accessed=7 * rows * length * 2,
        ),
        name="attn_bwd",
    )(q, k, v, d_out, out, lse, *extra)


def pick(arr, index, axis):
    return lax.dynamic_index_in_dim(arr, index, axis, keepdims=False)


def ordered(mine, other, rank, axis):
    low_ = jnp.where(rank == 0, mine, other)
    high = jnp.where(rank == 0, other, mine)
    return jnp.stack([low_, high], axis=axis)


def dp_gather(shard):
    count = lax.axis_size("dp")
    if count != 16:
        return lax.all_gather(shard, "dp", axis=0, tiled=False)
    index = lax.axis_index("dp")
    z, x, core = index // 4, (index // 2) % 2, index % 2
    got = [shard] + [
        lax.ppermute(shard, "dp", [(j, (j - 4 * s) % 16) for j in range(16)]) for s in (1, 2, 3)
    ]
    ring = jnp.stack(got + got[:3])
    column = lax.dynamic_slice_in_dim(ring, (4 - z) % 4, 4, 0)
    over_x = lax.ppermute(column, "dp", [(j, j ^ 2) for j in range(16)])
    plane = ordered(column, over_x, x, 1)
    over_core = lax.ppermute(plane, "dp", [(j, j ^ 1) for j in range(16)])
    return ordered(plane, over_core, core, 2).reshape((16,) + shard.shape)


def dp_scatter(parts):
    count = lax.axis_size("dp")
    if count != 16:
        flat = parts.reshape((-1,) + parts.shape[2:])
        return lax.psum_scatter(flat, "dp", scatter_dimension=0, tiled=True).astype(F32)
    index = lax.axis_index("dp")
    z, x, core = index // 4, (index // 2) % 2, index % 2
    cube = parts.reshape((4, 2, 2) + parts.shape[1:])
    got = lax.ppermute(pick(cube, 1 - core, 2), "dp", [(j, j ^ 1) for j in range(16)])
    square = (pick(cube, core, 2).astype(F32) + got.astype(F32)).astype(BF)
    got = lax.ppermute(pick(square, 1 - x, 1), "dp", [(j, j ^ 2) for j in range(16)])
    line = (pick(square, x, 1).astype(F32) + got.astype(F32)).astype(BF)
    total = pick(line, z, 0).astype(F32)
    for s in (1, 2, 3):
        got = lax.ppermute(
            pick(line, (z + s) % 4, 0), "dp", [(j, (j + 4 * s) % 16) for j in range(16)]
        )
        total = total + got.astype(F32)
    return total


def seq_swap(arr):
    return lax.ppermute(arr, "seq", [(0, 1), (1, 0)])


def seq_tokens(rows):
    if lax.axis_size("seq") == 2:
        return jnp.concatenate([rows, seq_swap(rows)], axis=0)
    return lax.all_gather(rows, "seq", axis=0, tiled=True)


def seq_tokens_sum(parts):
    if lax.axis_size("seq") == 2:
        own = parts.shape[0] // 2
        return parts[:own] + seq_swap(parts[own:].astype(BF)).astype(F32)
    return lax.psum_scatter(parts.astype(BF), "seq", scatter_dimension=0, tiled=True).astype(F32)


def seq_stack(arr):
    if lax.axis_size("seq") == 2:
        return ordered(arr, seq_swap(arr), lax.axis_index("seq"), 0)
    return lax.all_gather(arr, "seq", axis=0, tiled=False)


def heads_to_tokens(arr):
    count = lax.axis_size("seq")
    rows, length = arr.shape
    if count == 2:
        rank = lax.axis_index("seq")
        own = length // 2
        mine = lax.dynamic_slice_in_dim(arr, rank * own, own, 1)
        theirs = seq_swap(lax.dynamic_slice_in_dim(arr, (1 - rank) * own, own, 1))
        return ordered(mine, theirs, rank, 0).reshape(2 * rows, own)
    return lax.all_to_all(arr, "seq", split_axis=1, concat_axis=0, tiled=True)


def tokens_to_heads(arr):
    count = lax.axis_size("seq")
    rows, own = arr.shape
    if count == 2:
        rank = lax.axis_index("seq")
        half = rows // 2
        mine = lax.dynamic_slice_in_dim(arr, rank * half, half, 0)
        theirs = seq_swap(lax.dynamic_slice_in_dim(arr, (1 - rank) * half, half, 0))
        first = jnp.where(rank == 0, mine, theirs)
        second = jnp.where(rank == 0, theirs, mine)
        return jnp.concatenate([first, second], axis=1)
    return lax.all_to_all(arr, "seq", split_axis=0, concat_axis=1, tiled=True)


def pack_layout(seq_lens, total):
    places = jnp.arange(total, dtype=jnp.int32)
    ends = jnp.cumsum(seq_lens)
    starts = ends - seq_lens
    segment = jnp.sum((places[:, None] >= ends[None, :]).astype(jnp.int32), axis=1)
    starts_ext = jnp.concatenate([starts, ends[-1:]])
    labels = jnp.arange(seq_lens.shape[0] + 1, dtype=jnp.int32)
    offset = jnp.sum(jnp.where(segment[:, None] == labels[None, :], starts_ext[None, :], 0), axis=1)
    return segment, places - offset, segment < seq_lens.shape[0]


def unit_rms(values):
    inv = lax.rsqrt(jnp.mean(values * values, axis=-1, keepdims=True) + EPSILON)
    return values * inv, inv


def unit_rms_back(y, xhat, inv):
    return inv * (y - xhat * jnp.mean(y * xhat, axis=-1, keepdims=True))


def head_prep(lin, gain, cos_tab, sin_tab, scale):
    u = lin.reshape(-1, HD, lin.shape[1])
    inv = lax.rsqrt(jnp.mean(u * u, axis=1, keepdims=True) + EPSILON)
    u = u * inv * gain[None, :, None]
    first, second = u[:, : HD // 2], u[:, HD // 2 :]
    out = jnp.concatenate(
        [first * cos_tab - second * sin_tab, second * cos_tab + first * sin_tab], axis=1
    )
    return (out * scale).astype(BF).reshape(lin.shape)


def head_prep_back(grad, lin, gain, cos_tab, sin_tab):
    y = grad.astype(F32).reshape(-1, HD, lin.shape[1])
    first, second = y[:, : HD // 2], y[:, HD // 2 :]
    y = jnp.concatenate(
        [first * cos_tab + second * sin_tab, second * cos_tab - first * sin_tab], axis=1
    )
    u = lin.reshape(y.shape)
    inv = lax.rsqrt(jnp.mean(u * u, axis=1, keepdims=True) + EPSILON)
    xhat = u * inv
    d_gain = jnp.sum(y * xhat, axis=(0, 2))
    y = y * gain[None, :, None]
    d_lin = inv * (y - xhat * jnp.mean(y * xhat, axis=1, keepdims=True))
    return d_lin.astype(BF).reshape(lin.shape), d_gain


def body(
    tokens, lengths, attn_gain, w_query, w_key, w_value, query_gain, key_gain, w_out,
    ffn_gain, w_gate, w_up, w_down, cotangent,
):
    seq_n = lax.axis_size("seq")
    dp_n = lax.axis_size("dp")
    rank = lax.axis_index("seq")
    dp_rank = lax.axis_index("dp")
    own, width = tokens.shape
    length = own * seq_n
    q_w, kv_w = H * HD // seq_n, KV * HD // seq_n
    ff_dp = w_down.shape[0]
    ff_w = ff_dp // seq_n
    ff = ff_w * dp_n
    d_dp = w_query.shape[0]

    full = length == MINLEN * lengths.shape[1]
    segment, positions, valid = pack_layout(lengths[0], length)
    segs = None if full and lengths.shape[1] == 1 else segment
    my_valid = lax.dynamic_slice_in_dim(valid, rank * own, own).astype(F32)[:, None]

    def keep_valid(arr):
        return arr if full else arr * my_valid

    gain_a = attn_gain.astype(F32)[:, None]
    gain_f = ffn_gain.astype(F32)[:, None]

    def my_cols(w, n):
        return lax.dynamic_slice_in_dim(w, rank * n, n, 1)

    qkv_part = jnp.concatenate(
        [my_cols(w_query, q_w), my_cols(w_key, kv_w), my_cols(w_value, kv_w)], axis=1
    )
    qkv_part = (qkv_part.astype(F32) * gain_a).astype(BF)
    gains = jnp.concatenate([query_gain, key_gain])
    gains = jnp.pad(gains[None, :], ((0, 7), (0, qkv_part.shape[1] - gains.shape[0])))
    pick_ff = lambda w: pick(w.reshape(d_dp, dp_n, seq_n, ff_w), rank, 2).reshape(d_dp, ff)
    gu_part = jnp.concatenate([pick_ff(w_gate), pick_ff(w_up)], axis=1)
    gu_part = (gu_part.astype(F32) * gain_f).astype(BF)
    down_part = pick(w_down.reshape(seq_n, ff_w, width), rank, 0)

    gu_full = lax.all_gather(gu_part, "dp", axis=0, tiled=True)
    down_full = lax.all_gather(down_part, "dp", axis=0, tiled=True)
    got = dp_gather(jnp.concatenate([qkv_part, gains], axis=0))
    qkv_full = got[:, :d_dp].reshape(width, -1)
    per = query_gain.shape[0]
    gain_q = got[:, d_dp, :per].reshape(-1).astype(F32)
    gain_k = got[:, d_dp, per : 2 * per].reshape(-1).astype(F32)
    out_full = dp_gather(w_out).reshape(H * HD, width)

    xhat_a, inv_a = unit_rms(tokens)
    low_own = xhat_a.astype(BF)
    if seq_n == 2:
        low_a = ordered(low_own, seq_swap(low_own), rank, 0).reshape(length, width)
    else:
        low_a = lax.all_gather(low_own, "seq", axis=0, tiled=True)
    lin = dot(qkv_full, low_a, 0, 1)
    q_lin, k_lin = lin[:q_w], lin[q_w : q_w + kv_w]
    values = lin[q_w + kv_w :].astype(BF)
    freqs = ROPE_BASE ** (-(jnp.arange(HD // 2, dtype=F32) * (2.0 / HD)))
    angles = freqs[:, None] * positions.astype(F32)[None, :]
    cos_tab, sin_tab = jnp.cos(angles), jnp.sin(angles)
    queries = head_prep(q_lin, gain_q, cos_tab, sin_tab, 1.0 / math.sqrt(HD))
    keys = head_prep(k_lin, gain_k, cos_tab, sin_tab, 1.0)
    att_heads, lse = attn_fwd(queries, keys, values, segs)
    attended = heads_to_tokens(att_heads)
    resid = tokens + dot(attended, out_full, 0, 0)

    xhat_f, inv_f = unit_rms(resid)
    grad = keep_valid(cotangent)
    x_all = seq_tokens(xhat_f.astype(BF))
    g_all = seq_tokens(grad.astype(BF))
    gate = dot(x_all, gu_full[:, :ff], 1, 0)
    up = dot(x_all, gu_full[:, ff:], 1, 0)
    d_hidden = dot(g_all, down_full, 1, 1)
    sig = jax.nn.sigmoid(gate)
    silu = gate * sig
    hidden = (silu * up).astype(BF)
    d_gate = (d_hidden * up * sig * (1.0 + gate * (1.0 - sig))).astype(BF)
    d_up = (d_hidden * silu).astype(BF)
    d_ffn = dot(d_gate, gu_full[:, :ff], 1, 1) + dot(d_up, gu_full[:, ff:], 1, 1)
    d_ffn = seq_tokens_sum(d_ffn)
    d_resid = grad + unit_rms_back(d_ffn, xhat_f, inv_f)

    block_out = keep_valid(resid + seq_tokens_sum(dot(hidden, down_full, 1, 0)))
    d_w_g = dp_scatter(dot(x_all, d_gate, 0, 0).astype(BF).reshape(dp_n, d_dp, ff))
    d_w_u = dp_scatter(dot(x_all, d_up, 0, 0).astype(BF).reshape(dp_n, d_dp, ff))
    d_w_d = dp_scatter(dot(hidden, g_all, 0, 0).astype(BF).reshape(dp_n, ff_w, width))

    def full_ff(shard):
        both = seq_stack(shard.astype(BF)).reshape(seq_n, d_dp, dp_n, ff_w)
        return both.transpose(1, 2, 0, 3).reshape(d_dp, dp_n * seq_n * ff_w).astype(F32)

    d_w_g, d_w_u = full_ff(d_w_g), full_ff(d_w_u)
    d_w_d = seq_stack(d_w_d.astype(BF)).reshape(ff_dp, width).astype(F32)
    d_ffn_gain = jnp.sum(w_gate.astype(F32) * d_w_g + w_up.astype(F32) * d_w_u, axis=1)

    r_low = d_resid.astype(BF)
    d_att = tokens_to_heads(dot(out_full, r_low, 1, 1).astype(BF))
    d_w_o = dp_scatter(dot(attended, r_low, 1, 0).astype(BF).reshape(dp_n, d_dp, width))
    d_q, d_k, d_v = attn_bwd(queries, keys, values, d_att, att_heads, lse, segs)
    d_q, d_gq = head_prep_back(d_q, q_lin, gain_q, cos_tab, sin_tab)
    d_k, d_gk = head_prep_back(d_k, k_lin, gain_k, cos_tab, sin_tab)
    d_lin = jnp.concatenate([d_q, d_k, d_v], axis=0)
    d_norm = dot(d_lin, qkv_full, 0, 1)
    if seq_n == 2:
        other = lax.dynamic_slice_in_dim(d_norm, (1 - rank) * own, own, 0)
        d_norm = lax.dynamic_slice_in_dim(d_norm, rank * own, own, 0)
        d_norm = d_norm + seq_swap(other.astype(BF)).astype(F32)
    else:
        d_norm = seq_tokens_sum(d_norm)
    d_tokens = d_resid + unit_rms_back(d_norm, xhat_a, inv_a)

    d_w_x = dot(low_a, d_lin, 0, 1).astype(BF).reshape(dp_n, d_dp, -1)
    d_g = jnp.concatenate([d_gq, d_gk]).astype(BF)
    d_g = jnp.pad(d_g[None, :], ((0, 7), (0, d_w_x.shape[2] - d_g.shape[0])))
    d_g = jnp.broadcast_to(d_g[None], (dp_n,) + d_g.shape)
    d_w_x = dp_scatter(jnp.concatenate([d_w_x, d_g], axis=1))
    d_w_x = seq_stack(d_w_x.astype(BF)).astype(F32)
    both = d_w_x[:, :d_dp]
    join = lambda lo, n: both[:, :, lo : lo + n].transpose(1, 0, 2).reshape(d_dp, seq_n * n)
    d_w_q, d_w_k, d_w_v = join(0, q_w), join(q_w, kv_w), join(q_w + kv_w, kv_w)
    d_gains = jnp.sum(d_w_x[:, d_dp, : 2 * HD], axis=0)
    d_gq = lax.dynamic_slice_in_dim(d_gains, dp_rank * per, per)
    d_gk = lax.dynamic_slice_in_dim(d_gains, HD + dp_rank * per, per)
    d_attn_gain = jnp.sum(w_query.astype(F32) * d_w_q, axis=1) + jnp.sum(
        w_key.astype(F32) * d_w_k + w_value.astype(F32) * d_w_v, axis=1
    )
    d_w_o = jnp.sum(seq_stack(d_w_o.astype(BF)).astype(F32), axis=0)
    return (
        block_out,
        d_tokens,
        d_attn_gain,
        d_w_q * gain_a,
        d_w_k * gain_a,
        d_w_v * gain_a,
        d_gq,
        d_gk,
        d_w_o,
        d_ffn_gain,
        d_w_g * gain_f,
        d_w_u * gain_f,
        d_w_d,
    )


def solution(mesh):
    rows, shard, vec = P(("dp", "seq"), None), P("dp", None), P("dp")
    return jax.shard_map(
        body,
        mesh=mesh,
        in_specs=(
            rows, shard, vec, shard, shard, shard, vec, vec, shard, vec, shard, shard, shard, rows,
        ),
        out_specs=(
            rows, rows, vec, shard, shard, shard, vec, vec, shard, vec, shard, shard, shard,
        ),
        check_vma=False,
    )
```

```python
from functools import partial
import math

import jax
import jax.numpy as jnp
from jax import lax
from jax.experimental import pallas as pl
from jax.experimental.pallas import tpu as pltpu
from jax.sharding import PartitionSpec as P

H = 16
KV = 8
HD = 64
GROUP = H // KV
MINLEN = 1024

EPSILON = 1e-05
ROPE_BASE = 1000000.0
MASKED_SCORE = -1e30
BF = jnp.bfloat16
F32 = jnp.float32


def dot(left, right, lc, rc):
    return lax.dot_general(left, right, (((lc,), (rc,)), ((), ())), preferred_element_type=F32)


def masked(scores, q0, k0, segs):
    row = lax.broadcasted_iota(jnp.int32, scores.shape, 0) + k0
    col = lax.broadcasted_iota(jnp.int32, scores.shape, 1) + q0
    allowed = row <= col
    if segs is not None:
        allowed = allowed & (segs[0] == segs[1])
    return jnp.where(allowed, scores, MASKED_SCORE)


def attn_fwd_kernel(blk, static, *refs):
    if static:
        q_ref, k_ref, v_ref, o_ref, lse_ref = refs
    else:
        q_ref, k_ref, v_ref, sc_ref, sr_ref, o_ref, lse_ref = refs
    length = q_ref.shape[1]
    keys = k_ref[...].T

    def finish(q0, parts):
        top = parts[0][0].max(axis=0, keepdims=True)
        for s, _ in parts[1:]:
            top = jnp.maximum(top, s.max(axis=0, keepdims=True))
        total, out = 0.0, 0.0
        for s, v in parts:
            p = jnp.exp(s - top)
            total = total + p.sum(axis=0, keepdims=True)
            out = out + dot(v, p.astype(BF), 1, 0)
        o_ref[:, pl.ds(q0, blk)] = (out / total).astype(BF)
        lse_ref[0, :, pl.ds(q0, blk)] = top + jnp.log(total)

    if static:
        for qb in range(length // blk):
            q0 = qb * blk
            q = q_ref[:, q0 : q0 + blk]
            parts = []
            if qb:
                parts.append((dot(keys[:q0], q, 1, 0), v_ref[:, :q0]))
            diag = masked(dot(keys[q0 : q0 + blk], q, 1, 0), 0, 0, None)
            parts.append((diag, v_ref[:, q0 : q0 + blk]))
            finish(q0, parts)
    else:

        @pl.loop(0, length // blk)
        def _(qb):
            q0 = pl.multiple_of(qb * blk, blk)
            s = dot(keys, q_ref[:, pl.ds(q0, blk)], 1, 0)
            s = masked(s, q0, 0, (sc_ref[...], sr_ref[:, pl.ds(q0, blk)]))
            finish(q0, [(s, v_ref[...])])


def attn_bwd_kernel(blk, static, *refs):
    if static:
        q_ref, k_ref, v_ref, do_ref, o_ref, lse_ref, dq_ref, dk_ref, dv_ref, dk_acc, dv_acc = refs
    else:
        (q_ref, k_ref, v_ref, do_ref, o_ref, lse_ref, sc_ref, sr_ref,
         dq_ref, dk_ref, dv_ref, dk_acc, dv_acc) = refs
    length = q_ref.shape[1]
    member = lax.rem(pl.program_id(0), GROUP)
    keys = k_ref[...].T
    values = v_ref[...].T

    @pl.when(member == 0)
    def _():
        dk_acc[...] = jnp.zeros_like(dk_acc)
        dv_acc[...] = jnp.zeros_like(dv_acc)

    def part(q, d_out, lse, delta, k_lo, k_n, q0, segs, mask):
        rows = pl.ds(k_lo, k_n)
        k_blk, v_blk = keys[k_lo : k_lo + k_n], values[k_lo : k_lo + k_n]
        s = dot(k_blk, q, 1, 0)
        if mask:
            s = masked(s, q0, k_lo, segs)
        p = jnp.exp(s - lse)
        dv_acc[rows, :] += dot(p.astype(BF), d_out, 1, 1)
        dp = dot(v_blk, d_out, 1, 0)
        ds = (p * (dp - delta)).astype(BF)
        dk_acc[rows, :] += dot(ds, q, 1, 1)
        return dot(k_ref[:, rows], ds, 1, 0)

    def prepare(q0):
        cols = pl.ds(q0, blk)
        d_out = do_ref[:, cols]
        delta = (d_out.astype(F32) * o_ref[:, cols].astype(F32)).sum(axis=0, keepdims=True)
        return cols, q_ref[:, cols], d_out, lse_ref[0, :, cols], delta

    scale = 1.0 / math.sqrt(HD)
    if static:
        for qb in range(length // blk):
            q0 = qb * blk
            cols, q, d_out, lse, delta = prepare(q0)
            dq = part(q, d_out, lse, delta, q0, blk, q0, None, True)
            if qb:
                dq = dq + part(q, d_out, lse, delta, 0, q0, q0, None, False)
            dq_ref[:, cols] = (dq * scale).astype(BF)
    else:

        @pl.loop(0, length // blk)
        def _(qb):
            q0 = pl.multiple_of(qb * blk, blk)
            cols, q, d_out, lse, delta = prepare(q0)
            dq = part(q, d_out, lse, delta, 0, length, q0, (sc_ref[...], sr_ref[:, cols]), True)
            dq_ref[:, cols] = (dq * scale).astype(BF)

    @pl.when(member == GROUP - 1)
    def _():
        dk_ref[...] = dk_acc[...].T.astype(BF)
        dv_ref[...] = dv_acc[...].T.astype(BF)


def attn_specs(length):
    q_spec = pl.BlockSpec((HD, length), lambda h: (h, 0))
    kv_spec = pl.BlockSpec((HD, length), lambda h: (h // GROUP, 0))
    lse_spec = pl.BlockSpec((1, 1, length), lambda h: (h, 0, 0))
    seg_specs = [
        pl.BlockSpec((length, 1), lambda h: (0, 0)),
        pl.BlockSpec((1, length), lambda h: (0, 0)),
    ]
    return q_spec, kv_spec, lse_spec, seg_specs


def attn_fwd(q, k, v, segs):
    rows, length = q.shape
    heads = rows // HD
    static = segs is None
    q_spec, kv_spec, lse_spec, seg_specs = attn_specs(length)
    extra = () if static else (segs[:, None], segs[None, :])
    return pl.pallas_call(
        partial(attn_fwd_kernel, min(256, length), static),
        grid=(heads,),
        in_specs=[q_spec, kv_spec, kv_spec] + ([] if static else seg_specs),
        out_specs=[q_spec, lse_spec],
        out_shape=[
            jax.ShapeDtypeStruct((rows, length), BF),
            jax.ShapeDtypeStruct((heads, 1, length), F32),
        ],
        cost_estimate=pl.CostEstimate(
            flops=4 * heads * length * length * HD,
            transcendentals=heads * length * length,
            bytes_accessed=4 * rows * length * 2,
        ),
        name="attn_fwd",
    )(q, k, v, *extra)


def attn_bwd(q, k, v, d_out, out, lse, segs):
    rows, length = q.shape
    heads = rows // HD
    static = segs is None
    q_spec, kv_spec, lse_spec, seg_specs = attn_specs(length)
    extra = () if static else (segs[:, None], segs[None, :])
    return pl.pallas_call(
        partial(attn_bwd_kernel, min(256, length), static),
        grid=(heads,),
        in_specs=[q_spec, kv_spec, kv_spec, q_spec, q_spec, lse_spec]
        + ([] if static else seg_specs),
        out_specs=[q_spec, kv_spec, kv_spec],
        out_shape=[
            jax.ShapeDtypeStruct((rows, length), BF),
            jax.ShapeDtypeStruct(k.shape, BF),
            jax.ShapeDtypeStruct(v.shape, BF),
        ],
        scratch_shapes=[pltpu.VMEM((length, HD), F32), pltpu.VMEM((length, HD), F32)],
        cost_estimate=pl.CostEstimate(
            flops=10 * heads * length * length * HD,
            transcendentals=heads * length * length,
            bytes_accessed=7 * rows * length * 2,
        ),
        name="attn_bwd",
    )(q, k, v, d_out, out, lse, *extra)


def ff_prep_kernel(rank_ref, gate_ref, up_ref, down_ref, gain_ref, out_ref):
    first = rank_ref[0] == 0
    d_dp, ff_all = gate_ref.shape
    ff_w = down_ref.shape[0] // 2
    dp_n = ff_all // (2 * ff_w)
    gain = gain_ref[...]
    for half, ref in enumerate((gate_ref, up_ref)):
        for i in range(dp_n):
            lo = ref[:, 2 * i * ff_w : (2 * i + 1) * ff_w].astype(F32)
            hi = ref[:, (2 * i + 1) * ff_w : (2 * i + 2) * ff_w].astype(F32)
            at = (half * dp_n + i) * ff_w
            out_ref[:d_dp, at : at + ff_w] = (jnp.where(first, lo, hi) * gain).astype(BF)
    for b in range(ff_w // 16):
        lo = down_ref[16 * b : 16 * b + 16, :]
        hi = down_ref[ff_w + 16 * b : ff_w + 16 * b + 16, :]
        rows = jnp.where(first, lo.astype(F32), hi.astype(F32)).astype(BF)
        for band, at, frm, to in down_places(b, rows.shape[1], ff_all):
            out_ref[d_dp + 16 * band : d_dp + 16 * band + 16, at : at + to - frm] = rows[:, frm:to]


def down_places(b, width, ff_all):
    places, start = [], b * width
    while start < (b + 1) * width:
        band = start // ff_all
        end = min((band + 1) * ff_all, (b + 1) * width)
        places.append((band, start - band * ff_all, start - b * width, end - b * width))
        start = end
    return places


def ff_prep(rank, w_gate, w_up, w_down, gain):
    d_dp, ff_all = w_gate.shape
    bands = w_down.shape[0] // 2 * w_down.shape[1] // ff_all
    whole = lambda arr: pl.BlockSpec(arr.shape, lambda i, r: (0, 0))
    return pl.pallas_call(
        ff_prep_kernel,
        grid_spec=pltpu.PrefetchScalarGridSpec(
            num_scalar_prefetch=1,
            grid=(1,),
            in_specs=[whole(w_gate), whole(w_up), whole(w_down), whole(gain)],
            out_specs=pl.BlockSpec((d_dp + bands, ff_all), lambda i, r: (0, 0)),
        ),
        out_shape=jax.ShapeDtypeStruct((d_dp + bands, ff_all), BF),
        name="ff_prep",
    )(rank[None], w_gate, w_up, w_down, gain)


def ffn_core_kernel(sub, fresh, *refs):
    x_ref, g_ref, wg_ref, wu_ref, wd_ref = refs[:5]
    hid_ref, dg_ref, du_ref, dx_ref, out_ref, down = refs[5:] if fresh else refs[8:]
    dp_n, d_dp, blk = wg_ref.shape
    width = g_ref.shape[1]
    ff_all = wd_ref.shape[2]
    ff_w = down.shape[0] // dp_n
    step = pl.program_id(0)

    @pl.when(step == 0)
    def _():
        dx_ref[...] = jnp.zeros_like(dx_ref)
        out_ref[...] = jnp.zeros_like(out_ref)

        @pl.loop(0, dp_n)
        def _(i):
            for b in range(ff_w // 16):
                rows = pl.ds(pl.multiple_of(i * ff_w + 16 * b, 16), 16)
                for band, at, frm, to in down_places(b, width, ff_all):
                    down[rows, frm:to] = wd_ref[i, 16 * band : 16 * band + 16, at : at + to - frm]

    @pl.loop(0, blk // sub)
    def _(s):
        cols = pl.ds(pl.multiple_of(s * sub, 128), sub)
        rows = pl.ds(pl.multiple_of(step * blk + s * sub, 128), sub)
        x = x_ref[...]
        w_gate = wg_ref[:, :, cols].reshape(dp_n * d_dp, sub)
        w_up = wu_ref[:, :, cols].reshape(dp_n * d_dp, sub)
        w_down = down[rows, :]
        gate = dot(x, w_gate, 1, 0)
        up = dot(x, w_up, 1, 0)
        d_hid = dot(g_ref[...], w_down, 1, 1)
        sig = 1.0 / (1.0 + jnp.exp(-gate))
        silu = gate * sig
        hidden = (silu * up).astype(BF)
        d_gate = (d_hid * up * (sig * (1.0 + gate * (1.0 - sig)))).astype(BF)
        d_up = (d_hid * silu).astype(BF)
        hid_ref[:, cols] = hidden
        dg_ref[:, cols] = d_gate
        du_ref[:, cols] = d_up
        dx_ref[...] += dot(d_gate, w_gate, 1, 1) + dot(d_up, w_up, 1, 1)
        out_ref[...] += dot(hidden, w_down, 1, 0)


def ffn_core(x, g, packed, earlier, half, dp_n, d_dp, ff_w):
    rows, width = x.shape
    ff = dp_n * ff_w
    blk = ff // 2
    fresh = earlier is None
    whole = pl.BlockSpec((rows, width), lambda j: (0, 0))
    wide = pl.BlockSpec((rows, blk), lambda j: (half, j))
    bands = packed.shape[1] - d_dp
    keep = pl.BlockSpec(memory_space=pl.ANY)
    wide_shape = jax.ShapeDtypeStruct((2 * rows, ff), BF)
    return pl.pallas_call(
        partial(ffn_core_kernel, 384, fresh),
        grid=(2,),
        in_specs=[
            whole,
            whole,
            pl.BlockSpec((dp_n, d_dp, blk), lambda j: (0, 0, j)),
            pl.BlockSpec((dp_n, d_dp, blk), lambda j: (0, 0, 2 + j)),
            pl.BlockSpec(
                (dp_n, bands, 2 * ff), lambda j: (0, d_dp // bands, 0), pipeline_mode=pl.Buffered(1)
            ),
        ]
        + ([] if fresh else [keep] * 3),
        out_specs=[wide, wide, wide, whole, whole],
        out_shape=[wide_shape] * 3 + [jax.ShapeDtypeStruct((rows, width), F32)] * 2,
        scratch_shapes=[pltpu.VMEM((ff, width), BF)],
        input_output_aliases={} if fresh else {5: 0, 6: 1, 7: 2},
        compiler_params=pltpu.CompilerParams(vmem_limit_bytes=60 << 20),
        cost_estimate=pl.CostEstimate(
            flops=12 * rows * width * ff,
            transcendentals=rows * ff,
            bytes_accessed=6 * width * ff + 6 * rows * ff + 12 * rows * width,
        ),
        name="ffn_core",
    )(x, g, packed, packed, packed, *(() if fresh else earlier))


def assemble_kernel(place_ref, *refs):
    out_ref = refs[-1]
    rows = refs[0].shape[0]
    z, x, core = place_ref[0], place_ref[1], place_ref[2]
    for n, ref in enumerate(refs[:-1]):
        b, a, s = n // 8, n // 4 % 2, n % 4
        at = (lax.rem(z + s, 4) * 2 + (a + x - 2 * a * x)) * 2 + (b + core - 2 * b * core)
        out_ref[at] = ref[...]


def assemble(place, pieces):
    shape = pieces[0].shape
    return pl.pallas_call(
        assemble_kernel,
        grid_spec=pltpu.PrefetchScalarGridSpec(
            num_scalar_prefetch=1,
            grid=(1,),
            in_specs=[pl.BlockSpec(shape, lambda i, p: (0, 0))] * 16,
            out_specs=pl.BlockSpec((16,) + shape, lambda i, p: (0, 0, 0)),
        ),
        out_shape=jax.ShapeDtypeStruct((16,) + shape, BF),
        name="assemble",
    )(place, *pieces)


def pick(arr, index, axis):
    return lax.dynamic_index_in_dim(arr, index, axis, keepdims=False)


def ordered(mine, other, rank, axis):
    low_ = jnp.where(rank == 0, mine, other)
    high = jnp.where(rank == 0, other, mine)
    return jnp.stack([low_, high], axis=axis)


def dp_gather(shard):
    return lax.all_gather(shard, "dp", axis=0, tiled=False)


def dp_scatter(parts):
    flat = parts.reshape((-1,) + parts.shape[2:])
    return lax.psum_scatter(flat, "dp", scatter_dimension=0, tiled=True).astype(F32)


def dp_place():
    index = lax.axis_index("dp")
    return index // 4, (index // 2) % 2, index % 2


def to_core(arr):
    return lax.ppermute(arr, "dp", [(j, j ^ 1) for j in range(16)])


def to_x(arr):
    return lax.ppermute(arr, "dp", [(j, j ^ 2) for j in range(16)])


def to_z(arr, s):
    return lax.ppermute(arr, "dp", [(j, (j + 4 * s) % 16) for j in range(16)])


def gather_z(shard):
    return [shard] + [to_z(shard, 4 - s) for s in (1, 2, 3)]


def gather_rest(line):
    plane = line + [to_x(piece) for piece in line]
    return plane + [to_core(piece) for piece in plane]


def sum_core(parts):
    core = dp_place()[2]
    cube = parts.reshape((4, 2, 2) + parts.shape[1:])
    return pick(cube, core, 2), to_core(pick(cube, 1 - core, 2))


def sum_x(kept, got):
    x = dp_place()[1]
    square = (kept.astype(F32) + got.astype(F32)).astype(BF)
    return pick(square, x, 1), to_x(pick(square, 1 - x, 1))


def sum_z(kept, got):
    z = dp_place()[0]
    line = (kept.astype(F32) + got.astype(F32)).astype(BF)
    return pick(line, z, 0), [to_z(pick(line, (z + s) % 4, 0), s) for s in (1, 2, 3)]


def sum_end(kept, got):
    total = kept.astype(F32)
    for term in got:
        total = total + term.astype(F32)
    return total


def after(value, *others):
    return lax.optimization_barrier((value,) + tuple(others))[0]


def seq_swap(arr):
    return lax.ppermute(arr, "seq", [(0, 1), (1, 0)])


def seq_tokens(rows):
    if lax.axis_size("seq") == 2:
        return jnp.concatenate([rows, seq_swap(rows)], axis=0)
    return lax.all_gather(rows, "seq", axis=0, tiled=True)


def seq_tokens_sum(parts):
    if lax.axis_size("seq") == 2:
        own = parts.shape[0] // 2
        return parts[:own] + seq_swap(parts[own:].astype(BF)).astype(F32)
    return lax.psum_scatter(parts.astype(BF), "seq", scatter_dimension=0, tiled=True).astype(F32)


def seq_stack(arr):
    if lax.axis_size("seq") == 2:
        return ordered(arr, seq_swap(arr), lax.axis_index("seq"), 0)
    return lax.all_gather(arr, "seq", axis=0, tiled=False)


def heads_to_tokens(arr):
    count = lax.axis_size("seq")
    rows, length = arr.shape
    if count == 2:
        rank = lax.axis_index("seq")
        own = length // 2
        mine = lax.dynamic_slice_in_dim(arr, rank * own, own, 1)
        theirs = seq_swap(lax.dynamic_slice_in_dim(arr, (1 - rank) * own, own, 1))
        return ordered(mine, theirs, rank, 0).reshape(2 * rows, own)
    return lax.all_to_all(arr, "seq", split_axis=1, concat_axis=0, tiled=True)


def tokens_to_heads(arr):
    count = lax.axis_size("seq")
    rows, own = arr.shape
    if count == 2:
        rank = lax.axis_index("seq")
        half = rows // 2
        mine = lax.dynamic_slice_in_dim(arr, rank * half, half, 0)
        theirs = seq_swap(lax.dynamic_slice_in_dim(arr, (1 - rank) * half, half, 0))
        first = jnp.where(rank == 0, mine, theirs)
        second = jnp.where(rank == 0, theirs, mine)
        return jnp.concatenate([first, second], axis=1)
    return lax.all_to_all(arr, "seq", split_axis=0, concat_axis=1, tiled=True)


def pack_layout(seq_lens, total):
    places = jnp.arange(total, dtype=jnp.int32)
    ends = jnp.cumsum(seq_lens)
    starts = ends - seq_lens
    segment = jnp.sum((places[:, None] >= ends[None, :]).astype(jnp.int32), axis=1)
    starts_ext = jnp.concatenate([starts, ends[-1:]])
    labels = jnp.arange(seq_lens.shape[0] + 1, dtype=jnp.int32)
    offset = jnp.sum(jnp.where(segment[:, None] == labels[None, :], starts_ext[None, :], 0), axis=1)
    return segment, places - offset, segment < seq_lens.shape[0]


def unit_rms(values):
    inv = lax.rsqrt(jnp.mean(values * values, axis=-1, keepdims=True) + EPSILON)
    return values * inv, inv


def unit_rms_back(y, xhat, inv):
    return inv * (y - xhat * jnp.mean(y * xhat, axis=-1, keepdims=True))


def head_prep(lin, gain, cos_tab, sin_tab, scale):
    u = lin.reshape(-1, HD, lin.shape[1])
    inv = lax.rsqrt(jnp.mean(u * u, axis=1, keepdims=True) + EPSILON)
    u = u * inv * gain[None, :, None]
    first, second = u[:, : HD // 2], u[:, HD // 2 :]
    out = jnp.concatenate(
        [first * cos_tab - second * sin_tab, second * cos_tab + first * sin_tab], axis=1
    )
    return (out * scale).astype(BF).reshape(lin.shape)


def head_prep_back(grad, lin, gain, cos_tab, sin_tab):
    y = grad.astype(F32).reshape(-1, HD, lin.shape[1])
    first, second = y[:, : HD // 2], y[:, HD // 2 :]
    y = jnp.concatenate(
        [first * cos_tab + second * sin_tab, second * cos_tab - first * sin_tab], axis=1
    )
    u = lin.reshape(y.shape)
    inv = lax.rsqrt(jnp.mean(u * u, axis=1, keepdims=True) + EPSILON)
    xhat = u * inv
    d_gain = jnp.sum(y * xhat, axis=(0, 2))
    y = y * gain[None, :, None]
    d_lin = inv * (y - xhat * jnp.mean(y * xhat, axis=1, keepdims=True))
    return d_lin.astype(BF).reshape(lin.shape), d_gain


def body(
    tokens, lengths, attn_gain, w_query, w_key, w_value, query_gain, key_gain, w_out,
    ffn_gain, w_gate, w_up, w_down, cotangent,
):
    seq_n = lax.axis_size("seq")
    dp_n = lax.axis_size("dp")
    rank = lax.axis_index("seq")
    dp_rank = lax.axis_index("dp")
    own, width = tokens.shape
    length = own * seq_n
    q_w, kv_w = H * HD // seq_n, KV * HD // seq_n
    ff_dp = w_down.shape[0]
    ff_w = ff_dp // seq_n
    ff = ff_w * dp_n
    d_dp = w_query.shape[0]

    full = length == MINLEN * lengths.shape[1]
    segment, positions, valid = pack_layout(lengths[0], length)
    segs = None if full and lengths.shape[1] == 1 else segment
    my_valid = lax.dynamic_slice_in_dim(valid, rank * own, own).astype(F32)[:, None]

    def keep_valid(arr):
        return arr if full else arr * my_valid

    gain_a = attn_gain.astype(F32)[:, None]
    gain_f = ffn_gain.astype(F32)[:, None]

    def my_cols(w, n):
        return lax.dynamic_slice_in_dim(w, rank * n, n, 1)

    qkv_part = jnp.concatenate(
        [my_cols(w_query, q_w), my_cols(w_key, kv_w), my_cols(w_value, kv_w)], axis=1
    )
    qkv_part = (qkv_part.astype(F32) * gain_a).astype(BF)
    gains = jnp.concatenate([query_gain, key_gain])
    gains = jnp.pad(gains[None, :], ((0, 7), (0, qkv_part.shape[1] - gains.shape[0])))
    pick_ff = lambda w: pick(w.reshape(d_dp, dp_n, seq_n, ff_w), rank, 2).reshape(d_dp, ff)
    gu_part = jnp.concatenate([pick_ff(w_gate), pick_ff(w_up)], axis=1)
    gu_part = (gu_part.astype(F32) * gain_f).astype(BF)
    down_part = pick(w_down.reshape(seq_n, ff_w, width), rank, 0)

    gu_full = lax.all_gather(gu_part, "dp", axis=0, tiled=True)
    down_full = lax.all_gather(down_part, "dp", axis=0, tiled=True)
    got = dp_gather(jnp.concatenate([qkv_part, gains], axis=0))
    qkv_full = got[:, :d_dp].reshape(width, -1)
    per = query_gain.shape[0]
    gain_q = got[:, d_dp, :per].reshape(-1).astype(F32)
    gain_k = got[:, d_dp, per : 2 * per].reshape(-1).astype(F32)
    out_full = dp_gather(w_out).reshape(H * HD, width)

    xhat_a, inv_a = unit_rms(tokens)
    low_own = xhat_a.astype(BF)
    if seq_n == 2:
        low_a = ordered(low_own, seq_swap(low_own), rank, 0).reshape(length, width)
    else:
        low_a = lax.all_gather(low_own, "seq", axis=0, tiled=True)
    lin = dot(qkv_full, low_a, 0, 1)
    q_lin, k_lin = lin[:q_w], lin[q_w : q_w + kv_w]
    values = lin[q_w + kv_w :].astype(BF)
    freqs = ROPE_BASE ** (-(jnp.arange(HD // 2, dtype=F32) * (2.0 / HD)))
    angles = freqs[:, None] * positions.astype(F32)[None, :]
    cos_tab, sin_tab = jnp.cos(angles), jnp.sin(angles)
    queries = head_prep(q_lin, gain_q, cos_tab, sin_tab, 1.0 / math.sqrt(HD))
    keys = head_prep(k_lin, gain_k, cos_tab, sin_tab, 1.0)
    att_heads, lse = attn_fwd(queries, keys, values, segs)
    attended = heads_to_tokens(att_heads)
    resid = tokens + dot(attended, out_full, 0, 0)

    xhat_f, inv_f = unit_rms(resid)
    grad = keep_valid(cotangent)
    x_all = seq_tokens(xhat_f.astype(BF))
    g_all = seq_tokens(grad.astype(BF))
    gate = dot(x_all, gu_full[:, :ff], 1, 0)
    up = dot(x_all, gu_full[:, ff:], 1, 0)
    d_hidden = dot(g_all, down_full, 1, 1)
    sig = jax.nn.sigmoid(gate)
    silu = gate * sig
    hidden = (silu * up).astype(BF)
    d_gate = (d_hidden * up * sig * (1.0 + gate * (1.0 - sig))).astype(BF)
    d_up = (d_hidden * silu).astype(BF)
    d_ffn = dot(d_gate, gu_full[:, :ff], 1, 1) + dot(d_up, gu_full[:, ff:], 1, 1)
    d_ffn = seq_tokens_sum(d_ffn)
    d_resid = grad + unit_rms_back(d_ffn, xhat_f, inv_f)

    block_out = keep_valid(resid + seq_tokens_sum(dot(hidden, down_full, 1, 0)))
    d_w_g = dp_scatter(dot(x_all, d_gate, 0, 0).astype(BF).reshape(dp_n, d_dp, ff))
    d_w_u = dp_scatter(dot(x_all, d_up, 0, 0).astype(BF).reshape(dp_n, d_dp, ff))
    d_w_d = dp_scatter(dot(hidden, g_all, 0, 0).astype(BF).reshape(dp_n, ff_w, width))

    def full_ff(shard):
        both = seq_stack(shard.astype(BF)).reshape(seq_n, d_dp, dp_n, ff_w)
        return both.transpose(1, 2, 0, 3).reshape(d_dp, dp_n * seq_n * ff_w).astype(F32)

    d_w_g, d_w_u = full_ff(d_w_g), full_ff(d_w_u)
    d_w_d = seq_stack(d_w_d.astype(BF)).reshape(ff_dp, width).astype(F32)
    d_ffn_gain = jnp.sum(w_gate.astype(F32) * d_w_g + w_up.astype(F32) * d_w_u, axis=1)

    r_low = d_resid.astype(BF)
    d_att = tokens_to_heads(dot(out_full, r_low, 1, 1).astype(BF))
    d_w_o = dp_scatter(dot(attended, r_low, 1, 0).astype(BF).reshape(dp_n, d_dp, width))
    d_q, d_k, d_v = attn_bwd(queries, keys, values, d_att, att_heads, lse, segs)
    d_q, d_gq = head_prep_back(d_q, q_lin, gain_q, cos_tab, sin_tab)
    d_k, d_gk = head_prep_back(d_k, k_lin, gain_k, cos_tab, sin_tab)
    d_lin = jnp.concatenate([d_q, d_k, d_v], axis=0)
    d_norm = dot(d_lin, qkv_full, 0, 1)
    if seq_n == 2:
        other = lax.dynamic_slice_in_dim(d_norm, (1 - rank) * own, own, 0)
        d_norm = lax.dynamic_slice_in_dim(d_norm, rank * own, own, 0)
        d_norm = d_norm + seq_swap(other.astype(BF)).astype(F32)
    else:
        d_norm = seq_tokens_sum(d_norm)
    d_tokens = d_resid + unit_rms_back(d_norm, xhat_a, inv_a)

    d_w_x = dot(low_a, d_lin, 0, 1).astype(BF).reshape(dp_n, d_dp, -1)
    d_g = jnp.concatenate([d_gq, d_gk]).astype(BF)
    d_g = jnp.pad(d_g[None, :], ((0, 7), (0, d_w_x.shape[2] - d_g.shape[0])))
    d_g = jnp.broadcast_to(d_g[None], (dp_n,) + d_g.shape)
    d_w_x = dp_scatter(jnp.concatenate([d_w_x, d_g], axis=1))
    d_w_x = seq_stack(d_w_x.astype(BF)).astype(F32)
    both = d_w_x[:, :d_dp]
    join = lambda lo, n: both[:, :, lo : lo + n].transpose(1, 0, 2).reshape(d_dp, seq_n * n)
    d_w_q, d_w_k, d_w_v = join(0, q_w), join(q_w, kv_w), join(q_w + kv_w, kv_w)
    d_gains = jnp.sum(d_w_x[:, d_dp, : 2 * HD], axis=0)
    d_gq = lax.dynamic_slice_in_dim(d_gains, dp_rank * per, per)
    d_gk = lax.dynamic_slice_in_dim(d_gains, HD + dp_rank * per, per)
    d_attn_gain = jnp.sum(w_query.astype(F32) * d_w_q, axis=1) + jnp.sum(
        w_key.astype(F32) * d_w_k + w_value.astype(F32) * d_w_v, axis=1
    )
    d_w_o = jnp.sum(seq_stack(d_w_o.astype(BF)).astype(F32), axis=0)
    return (
        block_out,
        d_tokens,
        d_attn_gain,
        d_w_q * gain_a,
        d_w_k * gain_a,
        d_w_v * gain_a,
        d_gq,
        d_gk,
        d_w_o,
        d_ffn_gain,
        d_w_g * gain_f,
        d_w_u * gain_f,
        d_w_d,
    )


def body_fast(
    tokens, lengths, attn_gain, w_query, w_key, w_value, query_gain, key_gain, w_out,
    ffn_gain, w_gate, w_up, w_down, cotangent,
):
    seq_n, dp_n = 2, 16
    rank = lax.axis_index("seq")
    dp_rank = lax.axis_index("dp")
    place = jnp.stack(dp_place()).astype(jnp.int32)
    own, width = tokens.shape
    length = own * seq_n
    q_w, kv_w = H * HD // seq_n, KV * HD // seq_n
    ff_dp = w_down.shape[0]
    ff_w = ff_dp // seq_n
    ff = ff_w * dp_n
    d_dp = w_query.shape[0]
    gain_a = attn_gain.astype(F32)[:, None]
    gain_f = ffn_gain.astype(F32)[:, None]
    per = query_gain.shape[0]

    packed = ff_prep(rank, w_gate, w_up, w_down, gain_f)
    ff_full = lax.all_gather(packed, "dp", axis=0, tiled=False)

    def my_cols(w, n):
        return lax.dynamic_slice_in_dim(w, rank * n, n, 1)

    qkv_part = jnp.concatenate(
        [my_cols(w_query, q_w), my_cols(w_key, kv_w), my_cols(w_value, kv_w)], axis=1
    )
    qkv_part = (qkv_part.astype(F32) * gain_a).astype(BF)
    gains = jnp.concatenate([query_gain, key_gain])
    gains = jnp.pad(gains[None, :], ((0, 7), (0, qkv_part.shape[1] - gains.shape[0])))
    qkv_line = gather_z(jnp.concatenate([qkv_part, gains], axis=0))
    xhat_a, inv_a = unit_rms(tokens)
    low_own = xhat_a.astype(BF)
    low_other = seq_swap(low_own)
    got = assemble(place, gather_rest(qkv_line))
    qkv_full = got[:, :d_dp].reshape(width, -1)
    gain_q = got[:, d_dp, :per].reshape(-1).astype(F32)
    gain_k = got[:, d_dp, per : 2 * per].reshape(-1).astype(F32)
    out_pieces = gather_rest(gather_z(after(w_out, *qkv_line)))
    g_own = cotangent.astype(BF)
    g_other = seq_swap(after(g_own, low_other))

    low_a = ordered(low_own, low_other, rank, 0).reshape(length, width)
    lin = dot(qkv_full, low_a, 0, 1)
    q_lin, k_lin = lin[:q_w], lin[q_w : q_w + kv_w]
    values = lin[q_w + kv_w :].astype(BF)
    freqs = ROPE_BASE ** (-(jnp.arange(HD // 2, dtype=F32) * (2.0 / HD)))
    angles = freqs[:, None] * jnp.arange(length, dtype=jnp.int32).astype(F32)[None, :]
    cos_tab, sin_tab = jnp.cos(angles), jnp.sin(angles)
    queries = head_prep(q_lin, gain_q, cos_tab, sin_tab, 1.0 / math.sqrt(HD))
    keys = head_prep(k_lin, gain_k, cos_tab, sin_tab, 1.0)
    att_heads, lse = attn_fwd(queries, keys, values, None)
    attended = heads_to_tokens(att_heads)
    out_full = assemble(place, out_pieces).reshape(H * HD, width)
    resid = tokens + dot(attended, out_full, 0, 0)

    xhat_f, inv_f = unit_rms(resid)
    x_own = xhat_f.astype(BF)
    x_other = seq_swap(x_own)
    sizes = (dp_n, d_dp, ff_w)
    *wide, dx_own, out_own = ffn_core(x_own, g_own, ff_full, None, 0, *sizes)
    *wide, dx_other, out_other = ffn_core(x_other, g_other, ff_full, wide, 1, *sizes)
    hidden, d_gate, d_up = wide
    dx_got = seq_swap(dx_other.astype(BF))
    x_all = jnp.concatenate([x_own, x_other], axis=0)
    g_all = jnp.concatenate([g_own, g_other], axis=0)
    g1 = sum_core(dot(x_all, d_gate, 0, 0).astype(BF).reshape(dp_n, d_dp, ff))
    u1 = sum_core(dot(x_all, d_up, 0, 0).astype(BF).reshape(dp_n, d_dp, ff))
    g2 = sum_x(*g1)
    d1 = sum_core(dot(after(hidden, g1[1]), g_all, 0, 0).astype(BF).reshape(dp_n, ff_w, width))
    u2 = sum_x(*u1)

    d_ffn = dx_own + dx_got.astype(F32)
    d_resid = cotangent + unit_rms_back(after(d_ffn, u1[1]), xhat_f, inv_f)
    r_low = d_resid.astype(BF)
    d_att = tokens_to_heads(dot(out_full, r_low, 1, 1).astype(BF))
    o1 = sum_core(dot(attended, r_low, 1, 0).astype(BF).reshape(dp_n, d_dp, width))
    g3 = sum_z(*g2)
    d2 = sum_x(*d1)
    d_att = after(d_att, g2[1], d1[1], o1[1])
    d_q, d_k, d_v = attn_bwd(queries, keys, values, d_att, att_heads, lse, None)
    u3 = sum_z(*u2)
    o2 = sum_x(*o1)
    d_q = after(d_q, u2[1])
    d_q, d_gq = head_prep_back(d_q, q_lin, gain_q, cos_tab, sin_tab)
    d_k, d_gk = head_prep_back(d_k, k_lin, gain_k, cos_tab, sin_tab)
    d_lin = jnp.concatenate([d_q, d_k, d_v], axis=0)
    d_lin = after(d_lin, *g3[1])
    d_norm = dot(d_lin, qkv_full, 0, 1)
    other = lax.dynamic_slice_in_dim(d_norm, (1 - rank) * own, own, 0)
    d_norm = lax.dynamic_slice_in_dim(d_norm, rank * own, own, 0)
    d_norm = d_norm + seq_swap(other.astype(BF)).astype(F32)
    d_tokens = d_resid + unit_rms_back(d_norm, xhat_a, inv_a)

    d_w_x = dot(low_a, d_lin, 0, 1).astype(BF).reshape(dp_n, d_dp, -1)
    d_g = jnp.concatenate([d_gq, d_gk]).astype(BF)
    d_g = jnp.pad(d_g[None, :], ((0, 7), (0, d_w_x.shape[2] - d_g.shape[0])))
    d_g = jnp.broadcast_to(d_g[None], (dp_n,) + d_g.shape)
    x1 = sum_core(jnp.concatenate([d_w_x, d_g], axis=1))
    d3 = sum_z(*d2)
    x2 = sum_x(*x1)
    o3 = sum_z(*o2)
    x3 = sum_z(*x2)
    block_out = resid + out_own + seq_swap(out_other.astype(BF)).astype(F32)

    def full_ff(shard):
        both = seq_stack(shard.astype(BF)).reshape(seq_n, d_dp, dp_n, ff_w)
        return both.transpose(1, 2, 0, 3).reshape(d_dp, dp_n * seq_n * ff_w).astype(F32)

    d_w_g, d_w_u = full_ff(sum_end(*g3)), full_ff(sum_end(*u3))
    d_w_d = seq_stack(sum_end(*d3).astype(BF)).reshape(ff_dp, width).astype(F32)
    d_ffn_gain = jnp.sum(w_gate.astype(F32) * d_w_g + w_up.astype(F32) * d_w_u, axis=1)
    d_w_x = seq_stack(sum_end(*x3).astype(BF)).astype(F32)
    both = d_w_x[:, :d_dp]
    join = lambda lo, n: both[:, :, lo : lo + n].transpose(1, 0, 2).reshape(d_dp, seq_n * n)
    d_w_q, d_w_k, d_w_v = join(0, q_w), join(q_w, kv_w), join(q_w + kv_w, kv_w)
    d_gains = jnp.sum(d_w_x[:, d_dp, : 2 * HD], axis=0)
    d_gq = lax.dynamic_slice_in_dim(d_gains, dp_rank * per, per)
    d_gk = lax.dynamic_slice_in_dim(d_gains, HD + dp_rank * per, per)
    d_attn_gain = jnp.sum(w_query.astype(F32) * d_w_q, axis=1) + jnp.sum(
        w_key.astype(F32) * d_w_k + w_value.astype(F32) * d_w_v, axis=1
    )
    d_w_o = jnp.sum(seq_stack(sum_end(*o3).astype(BF)).astype(F32), axis=0)
    return (
        block_out,
        d_tokens,
        d_attn_gain,
        d_w_q * gain_a,
        d_w_k * gain_a,
        d_w_v * gain_a,
        d_gq,
        d_gk,
        d_w_o,
        d_ffn_gain,
        d_w_g * gain_f,
        d_w_u * gain_f,
        d_w_d,
    )


def body_for(*args):
    tokens, lengths = args[:2]
    sizes = (lax.axis_size("dp"), lax.axis_size("seq"))
    exact = lengths.shape[1] == 1 and tokens.shape[0] * sizes[1] == MINLEN
    return (body_fast if sizes == (16, 2) and exact else body)(*args)


def solution(mesh):
    rows, shard, vec = P(("dp", "seq"), None), P("dp", None), P("dp")
    return jax.shard_map(
        body_for,
        mesh=mesh,
        in_specs=(
            rows, shard, vec, shard, shard, shard, vec, vec, shard, vec, shard, shard, shard, rows,
        ),
        out_specs=(
            rows, rows, vec, shard, shard, shard, vec, vec, shard, vec, shard, shard, shard,
        ),
        check_vma=False,
    )
```

```python
from functools import partial
import math

import jax
import jax.numpy as jnp
from jax import lax
from jax.experimental import pallas as pl
from jax.experimental.pallas import tpu as pltpu
from jax.sharding import PartitionSpec as P

H = 16
KV = 8
HD = 64
GROUP = H // KV
MINLEN = 1024

EPSILON = 1e-05
ROPE_BASE = 1000000.0
MASKED_SCORE = -1e30
BF = jnp.bfloat16
F32 = jnp.float32


LONG = pl.CostEstimate(flops=40 << 30, transcendentals=0, bytes_accessed=96 << 20)
SHORT = pl.CostEstimate(flops=1 << 20, transcendentals=0, bytes_accessed=1 << 14)


def dot(left, right, lc, rc):
    return lax.dot_general(left, right, (((lc,), (rc,)), ((), ())), preferred_element_type=F32)


def masked(scores, q0, k0, segs):
    row = lax.broadcasted_iota(jnp.int32, scores.shape, 0) + k0
    col = lax.broadcasted_iota(jnp.int32, scores.shape, 1) + q0
    allowed = row <= col
    if segs is not None:
        allowed = allowed & (segs[0] == segs[1])
    return jnp.where(allowed, scores, MASKED_SCORE)


def attn_fwd_kernel(blk, static, *refs):
    if static:
        q_ref, k_ref, v_ref, o_ref, lse_ref = refs
    else:
        q_ref, k_ref, v_ref, sc_ref, sr_ref, o_ref, lse_ref = refs
    length = q_ref.shape[1]
    keys = k_ref[...].T

    def finish(q0, parts):
        top = parts[0][0].max(axis=0, keepdims=True)
        for s, _ in parts[1:]:
            top = jnp.maximum(top, s.max(axis=0, keepdims=True))
        total, out = 0.0, 0.0
        for s, v in parts:
            p = jnp.exp(s - top)
            total = total + p.sum(axis=0, keepdims=True)
            out = out + dot(v, p.astype(BF), 1, 0)
        o_ref[:, pl.ds(q0, blk)] = (out / total).astype(BF)
        lse_ref[0, :, pl.ds(q0, blk)] = top + jnp.log(total)

    if static:
        for qb in range(length // blk):
            q0 = qb * blk
            q = q_ref[:, q0 : q0 + blk]
            parts = []
            if qb:
                parts.append((dot(keys[:q0], q, 1, 0), v_ref[:, :q0]))
            diag = masked(dot(keys[q0 : q0 + blk], q, 1, 0), 0, 0, None)
            parts.append((diag, v_ref[:, q0 : q0 + blk]))
            finish(q0, parts)
    else:

        @pl.loop(0, length // blk)
        def _(qb):
            q0 = pl.multiple_of(qb * blk, blk)
            s = dot(keys, q_ref[:, pl.ds(q0, blk)], 1, 0)
            s = masked(s, q0, 0, (sc_ref[...], sr_ref[:, pl.ds(q0, blk)]))
            finish(q0, [(s, v_ref[...])])


def lin_back(y, lin, gain, cos_tab, sin_tab):
    first, second = y[: HD // 2], y[HD // 2 :]
    y = jnp.concatenate(
        [first * cos_tab + second * sin_tab, second * cos_tab - first * sin_tab], axis=0
    )
    inv = lax.rsqrt(jnp.mean(lin * lin, axis=0, keepdims=True) + EPSILON)
    xhat = lin * inv
    d_gain = jnp.sum(y * xhat, axis=1, keepdims=True)
    y = y * gain
    return inv * (y - xhat * jnp.mean(y * xhat, axis=0, keepdims=True)), d_gain


def attn_bwd_kernel(blk, static, *refs):
    lin_refs = None
    if static:
        q_ref, k_ref, v_ref, do_ref, o_ref, lse_ref = refs[:6]
        lin_refs = refs[6:12]
        dq_ref, dk_ref, dv_ref, dgq_ref, dgk_ref, dk_acc, dv_acc = refs[12:]
        ql_ref, kl_ref, gq_ref, gk_ref, cos_ref, sin_ref = lin_refs
    else:
        (q_ref, k_ref, v_ref, do_ref, o_ref, lse_ref, sc_ref, sr_ref,
         dq_ref, dk_ref, dv_ref, dk_acc, dv_acc) = refs
    length = q_ref.shape[1]
    member = lax.rem(pl.program_id(0), GROUP)
    keys = k_ref[...].T
    values = v_ref[...].T

    @pl.when(member == 0)
    def _():
        dk_acc[...] = jnp.zeros_like(dk_acc)
        dv_acc[...] = jnp.zeros_like(dv_acc)

    def part(q, d_out, lse, delta, k_lo, k_n, q0, segs, mask):
        rows = pl.ds(k_lo, k_n)
        k_blk, v_blk = keys[k_lo : k_lo + k_n], values[k_lo : k_lo + k_n]
        s = dot(k_blk, q, 1, 0)
        if mask:
            s = masked(s, q0, k_lo, segs)
        p = jnp.exp(s - lse)
        dv_acc[rows, :] += dot(p.astype(BF), d_out, 1, 1)
        dp = dot(v_blk, d_out, 1, 0)
        ds = (p * (dp - delta)).astype(BF)
        dk_acc[rows, :] += dot(ds, q, 1, 1)
        return dot(k_ref[:, rows], ds, 1, 0)

    def prepare(q0):
        cols = pl.ds(q0, blk)
        d_out = do_ref[:, cols]
        delta = (d_out.astype(F32) * o_ref[:, cols].astype(F32)).sum(axis=0, keepdims=True)
        return cols, q_ref[:, cols], d_out, lse_ref[0, :, cols], delta

    scale = 1.0 / math.sqrt(HD)
    if static:
        for qb in range(length // blk):
            q0 = qb * blk
            cols, q, d_out, lse, delta = prepare(q0)
            dq = part(q, d_out, lse, delta, q0, blk, q0, None, True)
            if qb:
                dq = dq + part(q, d_out, lse, delta, 0, q0, q0, None, False)
            d_lin, d_gain = lin_back(
                dq * scale, ql_ref[:, cols], gq_ref[...], cos_ref[:, cols], sin_ref[:, cols]
            )
            dq_ref[:, cols] = d_lin.astype(BF)
            dgq_ref[0] = d_gain if qb == 0 else dgq_ref[0] + d_gain
    else:

        @pl.loop(0, length // blk)
        def _(qb):
            q0 = pl.multiple_of(qb * blk, blk)
            cols, q, d_out, lse, delta = prepare(q0)
            dq = part(q, d_out, lse, delta, 0, length, q0, (sc_ref[...], sr_ref[:, cols]), True)
            dq_ref[:, cols] = (dq * scale).astype(BF)

    @pl.when(member == GROUP - 1)
    def _():
        dk = dk_acc[...].T
        if static:
            dk, d_gain = lin_back(dk, kl_ref[...], gk_ref[...], cos_ref[...], sin_ref[...])
            dgk_ref[0] = d_gain
        dk_ref[...] = dk.astype(BF)
        dv_ref[...] = dv_acc[...].T.astype(BF)


def attn_specs(length):
    q_spec = pl.BlockSpec((HD, length), lambda h: (h, 0))
    kv_spec = pl.BlockSpec((HD, length), lambda h: (h // GROUP, 0))
    lse_spec = pl.BlockSpec((1, 1, length), lambda h: (h, 0, 0))
    seg_specs = [
        pl.BlockSpec((length, 1), lambda h: (0, 0)),
        pl.BlockSpec((1, length), lambda h: (0, 0)),
    ]
    return q_spec, kv_spec, lse_spec, seg_specs


def attn_fwd(q, k, v, segs):
    rows, length = q.shape
    heads = rows // HD
    static = segs is None
    q_spec, kv_spec, lse_spec, seg_specs = attn_specs(length)
    extra = () if static else (segs[:, None], segs[None, :])
    return pl.pallas_call(
        partial(attn_fwd_kernel, min(256, length), static),
        grid=(heads,),
        in_specs=[q_spec, kv_spec, kv_spec] + ([] if static else seg_specs),
        out_specs=[q_spec, lse_spec],
        out_shape=[
            jax.ShapeDtypeStruct((rows, length), BF),
            jax.ShapeDtypeStruct((heads, 1, length), F32),
        ],
        cost_estimate=SHORT,
        name="attn_fwd",
    )(q, k, v, *extra)


def attn_bwd(q, k, v, d_out, out, lse, segs, lins=()):
    rows, length = q.shape
    heads = rows // HD
    static = segs is None
    q_spec, kv_spec, lse_spec, seg_specs = attn_specs(length)
    extra = tuple(lins) if static else (segs[:, None], segs[None, :])
    whole = lambda arr: pl.BlockSpec(arr.shape, lambda h: (0, 0))
    lin_specs = [q_spec, pl.BlockSpec((HD, length), lambda h: (heads + h // GROUP, 0))]
    lin_specs += [whole(arr) for arr in lins[2:]]
    gain_specs = [
        pl.BlockSpec((1, HD, 1), lambda h: (h, 0, 0)),
        pl.BlockSpec((1, HD, 1), lambda h: (h // GROUP, 0, 0)),
    ]
    gain_shapes = [
        jax.ShapeDtypeStruct((heads, HD, 1), F32),
        jax.ShapeDtypeStruct((heads // GROUP, HD, 1), F32),
    ]
    return pl.pallas_call(
        partial(attn_bwd_kernel, min(256, length), static),
        grid=(heads,),
        in_specs=[q_spec, kv_spec, kv_spec, q_spec, q_spec, lse_spec]
        + (lin_specs if static else seg_specs),
        out_specs=[q_spec, kv_spec, kv_spec] + (gain_specs if static else []),
        out_shape=[
            jax.ShapeDtypeStruct((rows, length), BF),
            jax.ShapeDtypeStruct(k.shape, BF),
            jax.ShapeDtypeStruct(v.shape, BF),
        ]
        + (gain_shapes if static else []),
        scratch_shapes=[pltpu.VMEM((length, HD), F32), pltpu.VMEM((length, HD), F32)],
        cost_estimate=LONG,
        name="attn_bwd",
    )(q, k, v, d_out, out, lse, *extra)


def ff_prep_kernel(rank_ref, gate_ref, up_ref, down_ref, gain_ref, out_ref):
    first = rank_ref[0] == 0
    d_dp, ff_all = gate_ref.shape
    ff_w = down_ref.shape[0] // 2
    dp_n = ff_all // (2 * ff_w)
    gain = gain_ref[...]
    for half, ref in enumerate((gate_ref, up_ref)):
        for i in range(dp_n):
            lo = ref[:, 2 * i * ff_w : (2 * i + 1) * ff_w].astype(F32)
            hi = ref[:, (2 * i + 1) * ff_w : (2 * i + 2) * ff_w].astype(F32)
            at = (half * dp_n + hidden_place(i)) * ff_w
            out_ref[:d_dp, at : at + ff_w] = (jnp.where(first, lo, hi) * gain).astype(BF)
    for b in range(ff_w // 16):
        lo = down_ref[16 * b : 16 * b + 16, :]
        hi = down_ref[ff_w + 16 * b : ff_w + 16 * b + 16, :]
        rows = jnp.where(first, lo.astype(F32), hi.astype(F32)).astype(BF)
        for band, at, frm, to in down_places(b, rows.shape[1], ff_all):
            out_ref[d_dp + 16 * band : d_dp + 16 * band + 16, at : at + to - frm] = rows[:, frm:to]


def hidden_place(i):
    return (i % 2 * 2 + i // 2 % 2) * 4 + i // 4


def down_places(b, width, ff_all):
    places, start = [], b * width
    while start < (b + 1) * width:
        band = start // ff_all
        end = min((band + 1) * ff_all, (b + 1) * width)
        places.append((band, start - band * ff_all, start - b * width, end - b * width))
        start = end
    return places


def ff_prep(rank, w_gate, w_up, w_down, gain):
    d_dp, ff_all = w_gate.shape
    bands = w_down.shape[0] // 2 * w_down.shape[1] // ff_all
    whole = lambda arr: pl.BlockSpec(arr.shape, lambda i, r: (0, 0))
    return pl.pallas_call(
        ff_prep_kernel,
        grid_spec=pltpu.PrefetchScalarGridSpec(
            num_scalar_prefetch=1,
            grid=(1,),
            in_specs=[whole(w_gate), whole(w_up), whole(w_down), whole(gain)],
            out_specs=pl.BlockSpec((d_dp + bands, ff_all), lambda i, r: (0, 0)),
        ),
        out_shape=jax.ShapeDtypeStruct((d_dp + bands, ff_all), BF),
        name="ff_prep",
    )(rank[None], w_gate, w_up, w_down, gain)


def ffn_core_kernel(sub, fresh, *refs):
    x_ref, g_ref, wg_ref, wu_ref, wd_ref = refs[:5]
    hid_ref, dg_ref, du_ref, dx_ref, out_ref, down = refs[5:] if fresh else refs[8:]
    dp_n, d_dp, blk = wg_ref.shape
    width = g_ref.shape[1]
    ff_all = wd_ref.shape[2]
    ff_w = down.shape[0] // dp_n
    step = pl.program_id(0)

    @pl.when(step == 0)
    def _():
        dx_ref[...] = jnp.zeros_like(dx_ref)
        out_ref[...] = jnp.zeros_like(out_ref)

        @pl.loop(0, dp_n)
        def _(i):
            for b in range(ff_w // 16):
                at_i = (lax.rem(i, 2) * 2 + lax.rem(lax.div(i, 2), 2)) * 4 + lax.div(i, 4)
                rows = pl.ds(pl.multiple_of(at_i * ff_w + 16 * b, 16), 16)
                for band, at, frm, to in down_places(b, width, ff_all):
                    down[rows, frm:to] = wd_ref[i, 16 * band : 16 * band + 16, at : at + to - frm]

    @pl.loop(0, blk // sub)
    def _(s):
        cols = pl.ds(pl.multiple_of(s * sub, 128), sub)
        rows = pl.ds(pl.multiple_of(step * blk + s * sub, 128), sub)
        x = x_ref[...]
        w_gate = wg_ref[:, :, cols].reshape(dp_n * d_dp, sub)
        w_up = wu_ref[:, :, cols].reshape(dp_n * d_dp, sub)
        w_down = down[rows, :]
        gate = dot(x, w_gate, 1, 0)
        up = dot(x, w_up, 1, 0)
        d_hid = dot(g_ref[...], w_down, 1, 1)
        sig = 1.0 / (1.0 + jnp.exp(-gate))
        silu = gate * sig
        hidden = (silu * up).astype(BF)
        d_gate = (d_hid * up * (sig * (1.0 + gate * (1.0 - sig)))).astype(BF)
        d_up = (d_hid * silu).astype(BF)
        hid_ref[:, cols] = hidden
        dg_ref[:, cols] = d_gate
        du_ref[:, cols] = d_up
        dx_ref[...] += dot(d_gate, w_gate, 1, 1) + dot(d_up, w_up, 1, 1)
        out_ref[...] += dot(hidden, w_down, 1, 0)


def ffn_core(x, g, packed, earlier, half, dp_n, d_dp, ff_w):
    rows, width = x.shape
    ff = dp_n * ff_w
    blk = ff // 2
    fresh = earlier is None
    whole = pl.BlockSpec((rows, width), lambda j: (0, 0))
    wide = pl.BlockSpec((rows, blk), lambda j: (half, j))
    bands = packed.shape[1] - d_dp
    keep = pl.BlockSpec(memory_space=pl.ANY)
    wide_shape = jax.ShapeDtypeStruct((2 * rows, ff), BF)
    return pl.pallas_call(
        partial(ffn_core_kernel, 384, fresh),
        grid=(2,),
        in_specs=[
            whole,
            whole,
            pl.BlockSpec((dp_n, d_dp, blk), lambda j: (0, 0, j)),
            pl.BlockSpec((dp_n, d_dp, blk), lambda j: (0, 0, 2 + j)),
            pl.BlockSpec(
                (dp_n, bands, 2 * ff), lambda j: (0, d_dp // bands, 0), pipeline_mode=pl.Buffered(1)
            ),
        ]
        + ([] if fresh else [keep] * 3),
        out_specs=[wide, wide, wide, whole, whole],
        out_shape=[wide_shape] * 3 + [jax.ShapeDtypeStruct((rows, width), F32)] * 2,
        scratch_shapes=[pltpu.VMEM((ff, width), BF)],
        input_output_aliases={} if fresh else {5: 0, 6: 1, 7: 2},
        compiler_params=pltpu.CompilerParams(vmem_limit_bytes=60 << 20),
        cost_estimate=SHORT,
        name="ffn_core",
    )(x, g, packed, packed, packed, *(() if fresh else earlier))


def mm_kernel(lc, rc, first_ref, a_ref, b_ref, *refs):
    total = dot(a_ref[...], b_ref[...], lc, rc)
    if len(refs) == 2:
        total = total + refs[0][...].astype(F32)
    refs[-1][...] = total.astype(refs[-1].dtype)


def mm(a, b, lc, rc, first, count, rows, dtype, add=None, add_first=0):
    cols = b.shape[1 - rc]
    a_spec = (
        pl.BlockSpec((rows, a.shape[1]), lambda i, f: (f[0] + i, 0))
        if lc
        else pl.BlockSpec((a.shape[0], rows), lambda i, f: (0, f[0] + i))
    )
    in_specs = [a_spec, pl.BlockSpec(b.shape, lambda i, f: (0, 0))]
    args = [a, b]
    if add is not None:
        in_specs.append(pl.BlockSpec((rows, cols), lambda i, f: (add_first + i, 0)))
        args.append(add)
    return pl.pallas_call(
        partial(mm_kernel, lc, rc),
        grid_spec=pltpu.PrefetchScalarGridSpec(
            num_scalar_prefetch=1,
            grid=(count,),
            in_specs=in_specs,
            out_specs=pl.BlockSpec((rows, cols), lambda i, f: (i, 0)),
        ),
        out_shape=jax.ShapeDtypeStruct((count * rows, cols), dtype),
        compiler_params=pltpu.CompilerParams(vmem_limit_bytes=48 << 20),
        cost_estimate=SHORT,
        name="mm",
    )(jnp.asarray(first, jnp.int32)[None], *args)


def ff_finish_kernel(rank_ref, mine_ref, theirs_ref, w_ref, gain_ref, out_ref, d_gain_ref):
    first = rank_ref[0] == 0
    mine, theirs = mine_ref[...].astype(F32), theirs_ref[...].astype(F32)
    low_ = jnp.where(first, mine, theirs)
    high = jnp.where(first, theirs, mine)
    gain = gain_ref[...]
    dp_n = gain_ref.shape[1]
    n = mine.shape[1] // dp_n
    total = jnp.zeros((mine.shape[0], 2 * n), F32)
    for i in range(dp_n):
        cols = slice(2 * i * n, 2 * (i + 1) * n)
        at = hidden_place(i) * n
        pair = jnp.concatenate([low_[:, at : at + n], high[:, at : at + n]], axis=1)
        total = total + pair * w_ref[:, cols].astype(F32)
        out_ref[:, cols] = pair * gain[:, :1]
    d_gain_ref[...] = total.sum(axis=1, keepdims=True)


def ff_finish(rank, mine, theirs, weight, gain, dp_n):
    gain = jnp.broadcast_to(gain, (gain.shape[0], dp_n))
    whole = lambda arr: pl.BlockSpec(arr.shape, lambda i, r: (0, 0))
    return pl.pallas_call(
        ff_finish_kernel,
        grid_spec=pltpu.PrefetchScalarGridSpec(
            num_scalar_prefetch=1,
            grid=(1,),
            in_specs=[whole(mine), whole(theirs), whole(weight), whole(gain)],
            out_specs=[
                pl.BlockSpec(weight.shape, lambda i, r: (0, 0)),
                pl.BlockSpec((weight.shape[0], 1), lambda i, r: (0, 0)),
            ],
        ),
        out_shape=[
            jax.ShapeDtypeStruct(weight.shape, F32),
            jax.ShapeDtypeStruct((weight.shape[0], 1), F32),
        ],
        name="ff_finish",
    )(rank[None], mine, theirs, weight, gain)


def assemble_kernel(place_ref, *refs):
    out_ref = refs[-1]
    rows = refs[0].shape[0]
    z, x, core = place_ref[0], place_ref[1], place_ref[2]
    for n, ref in enumerate(refs[:-1]):
        b, a, s = n // 8, n // 4 % 2, n % 4
        at = (lax.rem(z + s, 4) * 2 + (a + x - 2 * a * x)) * 2 + (b + core - 2 * b * core)
        out_ref[at] = ref[...]


def assemble(place, pieces):
    shape = pieces[0].shape
    return pl.pallas_call(
        assemble_kernel,
        grid_spec=pltpu.PrefetchScalarGridSpec(
            num_scalar_prefetch=1,
            grid=(1,),
            in_specs=[pl.BlockSpec(shape, lambda i, p: (0, 0))] * 16,
            out_specs=pl.BlockSpec((16,) + shape, lambda i, p: (0, 0, 0)),
        ),
        out_shape=jax.ShapeDtypeStruct((16,) + shape, BF),
        name="assemble",
    )(place, *pieces)


def pick(arr, index, axis):
    return lax.dynamic_index_in_dim(arr, index, axis, keepdims=False)


def ordered(mine, other, rank, axis):
    low_ = jnp.where(rank == 0, mine, other)
    high = jnp.where(rank == 0, other, mine)
    return jnp.stack([low_, high], axis=axis)


def dp_gather(shard):
    return lax.all_gather(shard, "dp", axis=0, tiled=False)


def dp_scatter(parts):
    flat = parts.reshape((-1,) + parts.shape[2:])
    return lax.psum_scatter(flat, "dp", scatter_dimension=0, tiled=True).astype(F32)


def dp_place():
    index = lax.axis_index("dp")
    return index // 4, (index // 2) % 2, index % 2


def to_core(arr):
    return lax.ppermute(arr, "dp", [(j, j ^ 1) for j in range(16)])


def to_x(arr):
    return lax.ppermute(arr, "dp", [(j, j ^ 2) for j in range(16)])


def to_z(arr, s):
    return lax.ppermute(arr, "dp", [(j, (j + 4 * s) % 16) for j in range(16)])


def gather_z(shard):
    return [shard] + [to_z(shard, 4 - s) for s in (1, 2, 3)]


def gather_rest(line):
    plane = line + [to_x(piece) for piece in line]
    return plane + [to_core(piece) for piece in plane]


def place_matrix(width):
    z, x, core = dp_place()
    n = jnp.arange(width, dtype=jnp.int32)
    part = width // 16
    block = (
        (z + n // part % 4) % 4 * 4
        + jnp.bitwise_xor(x, n // (4 * part) % 2) * 2
        + jnp.bitwise_xor(core, n // (8 * part))
    )
    source = block * part + n % part
    return (n[:, None] == source[None, :]).astype(BF)


def phase(*values):
    return lax.optimization_barrier(values)


def z_parts(kept, got):
    r = kept.shape[0] // 4
    sums = [kept[s * r : s * r + r] + got[s * r : s * r + r].astype(F32) for s in range(4)]
    return sums[0], [part.astype(BF) for part in sums[1:]]


def z_send(parts):
    return [to_z(part, s + 1) for s, part in enumerate(parts)]


def z_total(kept, got):
    total = kept
    for term in got:
        total = total + term.astype(F32)
    return total


def after(value, *others):
    return lax.optimization_barrier((value,) + tuple(others))[0]


def seq_swap(arr):
    return lax.ppermute(arr, "seq", [(0, 1), (1, 0)])


def seq_tokens(rows):
    if lax.axis_size("seq") == 2:
        return jnp.concatenate([rows, seq_swap(rows)], axis=0)
    return lax.all_gather(rows, "seq", axis=0, tiled=True)


def seq_tokens_sum(parts):
    if lax.axis_size("seq") == 2:
        own = parts.shape[0] // 2
        return parts[:own] + seq_swap(parts[own:].astype(BF)).astype(F32)
    return lax.psum_scatter(parts.astype(BF), "seq", scatter_dimension=0, tiled=True).astype(F32)


def seq_stack(arr):
    if lax.axis_size("seq") == 2:
        return ordered(arr, seq_swap(arr), lax.axis_index("seq"), 0)
    return lax.all_gather(arr, "seq", axis=0, tiled=False)


def heads_to_tokens(arr):
    count = lax.axis_size("seq")
    rows, length = arr.shape
    if count == 2:
        rank = lax.axis_index("seq")
        own = length // 2
        mine = lax.dynamic_slice_in_dim(arr, rank * own, own, 1)
        theirs = seq_swap(lax.dynamic_slice_in_dim(arr, (1 - rank) * own, own, 1))
        return ordered(mine, theirs, rank, 0).reshape(2 * rows, own)
    return lax.all_to_all(arr, "seq", split_axis=1, concat_axis=0, tiled=True)


def tokens_to_heads(arr):
    count = lax.axis_size("seq")
    rows, own = arr.shape
    if count == 2:
        rank = lax.axis_index("seq")
        half = rows // 2
        mine = lax.dynamic_slice_in_dim(arr, rank * half, half, 0)
        theirs = seq_swap(lax.dynamic_slice_in_dim(arr, (1 - rank) * half, half, 0))
        first = jnp.where(rank == 0, mine, theirs)
        second = jnp.where(rank == 0, theirs, mine)
        return jnp.concatenate([first, second], axis=1)
    return lax.all_to_all(arr, "seq", split_axis=0, concat_axis=1, tiled=True)


def pack_layout(seq_lens, total):
    places = jnp.arange(total, dtype=jnp.int32)
    ends = jnp.cumsum(seq_lens)
    starts = ends - seq_lens
    segment = jnp.sum((places[:, None] >= ends[None, :]).astype(jnp.int32), axis=1)
    starts_ext = jnp.concatenate([starts, ends[-1:]])
    labels = jnp.arange(seq_lens.shape[0] + 1, dtype=jnp.int32)
    offset = jnp.sum(jnp.where(segment[:, None] == labels[None, :], starts_ext[None, :], 0), axis=1)
    return segment, places - offset, segment < seq_lens.shape[0]


def unit_rms(values):
    inv = lax.rsqrt(jnp.mean(values * values, axis=-1, keepdims=True) + EPSILON)
    return values * inv, inv


def unit_rms_back(y, xhat, inv):
    return inv * (y - xhat * jnp.mean(y * xhat, axis=-1, keepdims=True))


def head_prep(lin, gain, cos_tab, sin_tab, scale):
    u = lin.reshape(-1, HD, lin.shape[1])
    inv = lax.rsqrt(jnp.mean(u * u, axis=1, keepdims=True) + EPSILON)
    u = u * inv * gain[None, :, None]
    first, second = u[:, : HD // 2], u[:, HD // 2 :]
    out = jnp.concatenate(
        [first * cos_tab - second * sin_tab, second * cos_tab + first * sin_tab], axis=1
    )
    return (out * scale).astype(BF).reshape(lin.shape)


def head_prep_back(grad, lin, gain, cos_tab, sin_tab):
    y = grad.astype(F32).reshape(-1, HD, lin.shape[1])
    first, second = y[:, : HD // 2], y[:, HD // 2 :]
    y = jnp.concatenate(
        [first * cos_tab + second * sin_tab, second * cos_tab - first * sin_tab], axis=1
    )
    u = lin.reshape(y.shape)
    inv = lax.rsqrt(jnp.mean(u * u, axis=1, keepdims=True) + EPSILON)
    xhat = u * inv
    d_gain = jnp.sum(y * xhat, axis=(0, 2))
    y = y * gain[None, :, None]
    d_lin = inv * (y - xhat * jnp.mean(y * xhat, axis=1, keepdims=True))
    return d_lin.astype(BF).reshape(lin.shape), d_gain


def body(
    tokens, lengths, attn_gain, w_query, w_key, w_value, query_gain, key_gain, w_out,
    ffn_gain, w_gate, w_up, w_down, cotangent,
):
    seq_n = lax.axis_size("seq")
    dp_n = lax.axis_size("dp")
    rank = lax.axis_index("seq")
    dp_rank = lax.axis_index("dp")
    own, width = tokens.shape
    length = own * seq_n
    q_w, kv_w = H * HD // seq_n, KV * HD // seq_n
    ff_dp = w_down.shape[0]
    ff_w = ff_dp // seq_n
    ff = ff_w * dp_n
    d_dp = w_query.shape[0]

    full = length == MINLEN * lengths.shape[1]
    segment, positions, valid = pack_layout(lengths[0], length)
    segs = None if full and lengths.shape[1] == 1 else segment
    my_valid = lax.dynamic_slice_in_dim(valid, rank * own, own).astype(F32)[:, None]

    def keep_valid(arr):
        return arr if full else arr * my_valid

    gain_a = attn_gain.astype(F32)[:, None]
    gain_f = ffn_gain.astype(F32)[:, None]

    def my_cols(w, n):
        return lax.dynamic_slice_in_dim(w, rank * n, n, 1)

    qkv_part = jnp.concatenate(
        [my_cols(w_query, q_w), my_cols(w_key, kv_w), my_cols(w_value, kv_w)], axis=1
    )
    qkv_part = (qkv_part.astype(F32) * gain_a).astype(BF)
    gains = jnp.concatenate([query_gain, key_gain])
    gains = jnp.pad(gains[None, :], ((0, 7), (0, qkv_part.shape[1] - gains.shape[0])))
    pick_ff = lambda w: pick(w.reshape(d_dp, dp_n, seq_n, ff_w), rank, 2).reshape(d_dp, ff)
    gu_part = jnp.concatenate([pick_ff(w_gate), pick_ff(w_up)], axis=1)
    gu_part = (gu_part.astype(F32) * gain_f).astype(BF)
    down_part = pick(w_down.reshape(seq_n, ff_w, width), rank, 0)

    gu_full = lax.all_gather(gu_part, "dp", axis=0, tiled=True)
    down_full = lax.all_gather(down_part, "dp", axis=0, tiled=True)
    got = dp_gather(jnp.concatenate([qkv_part, gains], axis=0))
    qkv_full = got[:, :d_dp].reshape(width, -1)
    per = query_gain.shape[0]
    gain_q = got[:, d_dp, :per].reshape(-1).astype(F32)
    gain_k = got[:, d_dp, per : 2 * per].reshape(-1).astype(F32)
    out_full = dp_gather(w_out).reshape(H * HD, width)

    xhat_a, inv_a = unit_rms(tokens)
    low_own = xhat_a.astype(BF)
    if seq_n == 2:
        low_a = ordered(low_own, seq_swap(low_own), rank, 0).reshape(length, width)
    else:
        low_a = lax.all_gather(low_own, "seq", axis=0, tiled=True)
    lin = dot(qkv_full, low_a, 0, 1)
    q_lin, k_lin = lin[:q_w], lin[q_w : q_w + kv_w]
    values = lin[q_w + kv_w :].astype(BF)
    freqs = ROPE_BASE ** (-(jnp.arange(HD // 2, dtype=F32) * (2.0 / HD)))
    angles = freqs[:, None] * positions.astype(F32)[None, :]
    cos_tab, sin_tab = jnp.cos(angles), jnp.sin(angles)
    queries = head_prep(q_lin, gain_q, cos_tab, sin_tab, 1.0 / math.sqrt(HD))
    keys = head_prep(k_lin, gain_k, cos_tab, sin_tab, 1.0)
    att_heads, lse = attn_fwd(queries, keys, values, segs)
    attended = heads_to_tokens(att_heads)
    resid = tokens + dot(attended, out_full, 0, 0)

    xhat_f, inv_f = unit_rms(resid)
    grad = keep_valid(cotangent)
    x_all = seq_tokens(xhat_f.astype(BF))
    g_all = seq_tokens(grad.astype(BF))
    gate = dot(x_all, gu_full[:, :ff], 1, 0)
    up = dot(x_all, gu_full[:, ff:], 1, 0)
    d_hidden = dot(g_all, down_full, 1, 1)
    sig = jax.nn.sigmoid(gate)
    silu = gate * sig
    hidden = (silu * up).astype(BF)
    d_gate = (d_hidden * up * sig * (1.0 + gate * (1.0 - sig))).astype(BF)
    d_up = (d_hidden * silu).astype(BF)
    d_ffn = dot(d_gate, gu_full[:, :ff], 1, 1) + dot(d_up, gu_full[:, ff:], 1, 1)
    d_ffn = seq_tokens_sum(d_ffn)
    d_resid = grad + unit_rms_back(d_ffn, xhat_f, inv_f)

    block_out = keep_valid(resid + seq_tokens_sum(dot(hidden, down_full, 1, 0)))
    d_w_g = dp_scatter(dot(x_all, d_gate, 0, 0).astype(BF).reshape(dp_n, d_dp, ff))
    d_w_u = dp_scatter(dot(x_all, d_up, 0, 0).astype(BF).reshape(dp_n, d_dp, ff))
    d_w_d = dp_scatter(dot(hidden, g_all, 0, 0).astype(BF).reshape(dp_n, ff_w, width))

    def full_ff(shard):
        both = seq_stack(shard.astype(BF)).reshape(seq_n, d_dp, dp_n, ff_w)
        return both.transpose(1, 2, 0, 3).reshape(d_dp, dp_n * seq_n * ff_w).astype(F32)

    d_w_g, d_w_u = full_ff(d_w_g), full_ff(d_w_u)
    d_w_d = seq_stack(d_w_d.astype(BF)).reshape(ff_dp, width).astype(F32)
    d_ffn_gain = jnp.sum(w_gate.astype(F32) * d_w_g + w_up.astype(F32) * d_w_u, axis=1)

    r_low = d_resid.astype(BF)
    d_att = tokens_to_heads(dot(out_full, r_low, 1, 1).astype(BF))
    d_w_o = dp_scatter(dot(attended, r_low, 1, 0).astype(BF).reshape(dp_n, d_dp, width))
    if segs is None:
        lins = (lin, lin, gain_q[:, None], gain_k[:, None], cos_tab, sin_tab)
        d_q, d_k, d_v, d_gq, d_gk = attn_bwd(queries, keys, values, d_att, att_heads, lse, None, lins)
        d_gq, d_gk = d_gq.sum(axis=(0, 2)), d_gk.sum(axis=(0, 2))
    else:
        d_q, d_k, d_v = attn_bwd(queries, keys, values, d_att, att_heads, lse, segs)
        d_q, d_gq = head_prep_back(d_q, q_lin, gain_q, cos_tab, sin_tab)
        d_k, d_gk = head_prep_back(d_k, k_lin, gain_k, cos_tab, sin_tab)
    d_lin = jnp.concatenate([d_q, d_k, d_v], axis=0)
    d_norm = dot(d_lin, qkv_full, 0, 1)
    if seq_n == 2:
        other = lax.dynamic_slice_in_dim(d_norm, (1 - rank) * own, own, 0)
        d_norm = lax.dynamic_slice_in_dim(d_norm, rank * own, own, 0)
        d_norm = d_norm + seq_swap(other.astype(BF)).astype(F32)
    else:
        d_norm = seq_tokens_sum(d_norm)
    d_tokens = d_resid + unit_rms_back(d_norm, xhat_a, inv_a)

    d_w_x = dot(low_a, d_lin, 0, 1).astype(BF).reshape(dp_n, d_dp, -1)
    d_g = jnp.concatenate([d_gq, d_gk]).astype(BF)
    d_g = jnp.pad(d_g[None, :], ((0, 7), (0, d_w_x.shape[2] - d_g.shape[0])))
    d_g = jnp.broadcast_to(d_g[None], (dp_n,) + d_g.shape)
    d_w_x = dp_scatter(jnp.concatenate([d_w_x, d_g], axis=1))
    d_w_x = seq_stack(d_w_x.astype(BF)).astype(F32)
    both = d_w_x[:, :d_dp]
    join = lambda lo, n: both[:, :, lo : lo + n].transpose(1, 0, 2).reshape(d_dp, seq_n * n)
    d_w_q, d_w_k, d_w_v = join(0, q_w), join(q_w, kv_w), join(q_w + kv_w, kv_w)
    d_gains = jnp.sum(d_w_x[:, d_dp, : 2 * HD], axis=0)
    d_gq = lax.dynamic_slice_in_dim(d_gains, dp_rank * per, per)
    d_gk = lax.dynamic_slice_in_dim(d_gains, HD + dp_rank * per, per)
    d_attn_gain = jnp.sum(w_query.astype(F32) * d_w_q, axis=1) + jnp.sum(
        w_key.astype(F32) * d_w_k + w_value.astype(F32) * d_w_v, axis=1
    )
    d_w_o = jnp.sum(seq_stack(d_w_o.astype(BF)).astype(F32), axis=0)
    return (
        block_out,
        d_tokens,
        d_attn_gain,
        d_w_q * gain_a,
        d_w_k * gain_a,
        d_w_v * gain_a,
        d_gq,
        d_gk,
        d_w_o,
        d_ffn_gain,
        d_w_g * gain_f,
        d_w_u * gain_f,
        d_w_d,
    )


def body_fast(
    tokens, lengths, attn_gain, w_query, w_key, w_value, query_gain, key_gain, w_out,
    ffn_gain, w_gate, w_up, w_down, cotangent,
):
    seq_n, dp_n = 2, 16
    rank = lax.axis_index("seq")
    dp_rank = lax.axis_index("dp")
    place = jnp.stack(dp_place()).astype(jnp.int32)
    own, width = tokens.shape
    length = own * seq_n
    q_w, kv_w = H * HD // seq_n, KV * HD // seq_n
    ff_dp = w_down.shape[0]
    ff_w = ff_dp // seq_n
    ff = ff_w * dp_n
    d_dp = w_query.shape[0]
    gain_a = attn_gain.astype(F32)[:, None]
    gain_f = ffn_gain.astype(F32)[:, None]
    per = query_gain.shape[0]

    packed = ff_prep(rank, w_gate, w_up, w_down, gain_f)
    ff_full = lax.all_gather(packed, "dp", axis=0, tiled=False)

    def my_cols(w, n):
        return lax.dynamic_slice_in_dim(w, rank * n, n, 1)

    qkv_part = jnp.concatenate(
        [my_cols(w_query, q_w), my_cols(w_key, kv_w), my_cols(w_value, kv_w)], axis=1
    )
    qkv_part = (qkv_part.astype(F32) * gain_a).astype(BF)
    gains = jnp.concatenate([query_gain, key_gain])
    gains = jnp.pad(gains[None, :], ((0, 7), (0, qkv_part.shape[1] - gains.shape[0])))
    qkv_line = gather_z(jnp.concatenate([qkv_part, gains], axis=0))
    xhat_a, inv_a = unit_rms(tokens)
    low_own = xhat_a.astype(BF)
    low_other = seq_swap(low_own)
    qkv_pieces = gather_rest(qkv_line)
    g_own = cotangent.astype(BF)
    g_other = seq_swap(after(g_own, low_other))
    got = assemble(place, qkv_pieces)
    qkv_full = got[:, :d_dp].reshape(width, -1)
    gain_q = got[:, d_dp, :per].reshape(-1).astype(F32)
    gain_k = got[:, d_dp, per : 2 * per].reshape(-1).astype(F32)
    out_line = gather_z(after(w_out, *qkv_line))

    low_a = ordered(low_own, low_other, rank, 0).reshape(length, width)
    lin = dot(qkv_full, low_a, 0, 1)
    q_lin, k_lin = lin[:q_w], lin[q_w : q_w + kv_w]
    values = lin[q_w + kv_w :].astype(BF)
    freqs = ROPE_BASE ** (-(jnp.arange(HD // 2, dtype=F32) * (2.0 / HD)))
    angles = freqs[:, None] * jnp.arange(length, dtype=jnp.int32).astype(F32)[None, :]
    cos_tab, sin_tab = jnp.cos(angles), jnp.sin(angles)
    queries = head_prep(q_lin, gain_q, cos_tab, sin_tab, 1.0 / math.sqrt(HD))
    keys = head_prep(k_lin, gain_k, cos_tab, sin_tab, 1.0)
    place_mat = place_matrix(width)
    low_placed = dot(place_mat, low_a, 0, 1).astype(BF)
    queries, low_placed, g_other, *out_line = phase(queries, low_placed, g_other, *out_line)
    out_pieces = gather_rest(out_line)
    att_heads, lse = attn_fwd(queries, keys, values, None)
    attended = heads_to_tokens(att_heads)
    out_full = assemble(place, out_pieces).reshape(H * HD, width)
    resid = tokens + dot(attended, out_full, 0, 0)

    z, x, core = dp_place()
    half, quarter = width // 2, width // 4
    xhat_f, inv_f = unit_rms(resid)
    x_own = xhat_f.astype(BF)
    x_other = seq_swap(x_own)
    sizes = (dp_n, d_dp, ff_w)
    *wide, dx_own, out_own = ffn_core(x_own, g_own, ff_full, None, 0, *sizes)
    x_other, g_both, wide[0] = phase(x_other, g_other, wide[0])
    x_placed = dot(place_mat, jnp.concatenate([x_own, x_other], axis=0), 0, 1).astype(BF)
    g_all = jnp.concatenate([g_own, g_both], axis=0)
    x_placed, x_other, g_all = phase(x_placed, x_other, g_all)
    *wide, dx_other, out_other = ffn_core(x_other, g_other, ff_full, wide, 1, *sizes)
    hidden, d_gate, d_up = wide

    dx_send, d_gate = phase(dx_other.astype(BF), d_gate)
    dx_got = seq_swap(dx_send)
    g_far = mm(x_placed, d_gate, 1, 0, 2, 2, quarter, BF)
    g_far, d_up = phase(g_far, d_up)
    g_got = to_core(g_far)
    u_far = mm(x_placed, d_up, 1, 0, 2, 2, quarter, BF)
    u_far, g_got, d_gate = phase(u_far, g_got, d_gate)
    u_got = to_core(u_far)
    g_xs = mm(x_placed, d_gate, 1, 0, 1, 1, quarter, BF, g_got, 1)
    g_xs, d_up, u_got = phase(g_xs, d_up, u_got)
    g_xgot = to_x(g_xs)
    u_xs = mm(x_placed, d_up, 1, 0, 1, 1, quarter, BF, u_got, 1)
    u_xs, d_gate, d_up = phase(u_xs, d_gate, d_up)
    g_kept = mm(x_placed, d_gate, 1, 0, 0, 1, quarter, F32, g_got)
    u_kept = mm(x_placed, d_up, 1, 0, 0, 1, quarter, F32, u_got)
    u_xs, dx_got, g_xgot, g_kept, u_kept = phase(u_xs, dx_got, g_xgot, g_kept, u_kept)
    u_xgot = to_x(u_xs)

    d_ffn = dx_own + dx_got.astype(F32)
    d_resid = cotangent + unit_rms_back(d_ffn, xhat_f, inv_f)
    r_low = d_resid.astype(BF)
    d_att_all = dot(out_full, r_low, 1, 1).astype(BF)
    d_att_send = lax.dynamic_slice_in_dim(d_att_all, (1 - rank) * q_w, q_w, 0)
    g_own_part, g_zs = z_parts(g_kept, g_xgot)
    d_att_send, hidden, g_own_part, *g_zs = phase(d_att_send, hidden, g_own_part, *g_zs)
    d_att_got = seq_swap(d_att_send)
    g_zgot = z_send(g_zs)
    third = ff // 6
    d_far = mm(hidden, g_all, 0, 0, (1 - core) * 3, 3, third, BF)
    d_far, attended = phase(d_far, attended)
    d_got = to_core(d_far)
    att_placed = dot(place_mat, attended, 0, 0).astype(BF)
    o_far = mm(att_placed, r_low, 1, 0, 2, 2, quarter, BF)
    o_far, d_got, hidden = phase(o_far, d_got, hidden)
    o_got = to_core(o_far)
    d_sum = mm(hidden, g_all, 0, 0, core * 3, 3, third, BF, d_got).reshape(2, ff // 4, width)
    d_xs = pick(d_sum, 1 - x, 0)
    d_xs, o_got, u_xgot, d_att_got = phase(d_xs, o_got, u_xgot, d_att_got)
    d_xgot = to_x(d_xs)
    o_sum = mm(att_placed, r_low, 1, 0, 0, 2, quarter, F32, o_got)
    o_xs = o_sum[quarter:].astype(BF)
    u_own_part, u_zs = z_parts(u_kept, u_xgot)
    vals = phase(o_xs, u_own_part, *u_zs, *g_zgot)
    o_xs, u_own_part = vals[:2]
    u_zs, g_zgot = vals[2:5], vals[5:]

    d_att_mine = lax.dynamic_slice_in_dim(d_att_all, rank * q_w, q_w, 0)
    d_att = jnp.concatenate(
        [jnp.where(rank == 0, d_att_mine, d_att_got), jnp.where(rank == 0, d_att_got, d_att_mine)],
        axis=1,
    )
    d_att, o_xs, out_send, *u_zs = phase(d_att, o_xs, out_other.astype(BF), *u_zs)
    u_zgot = z_send(u_zs)
    o_xgot = to_x(o_xs)
    out_got = seq_swap(out_send)
    lins = (lin, lin, gain_q[:, None], gain_k[:, None], cos_tab, sin_tab)
    d_q, d_k, d_v, d_gq, d_gk = attn_bwd(queries, keys, values, d_att, att_heads, lse, None, lins)
    vals = phase(d_q, d_k, d_v, d_gq, d_gk, d_xgot, out_got, *u_zgot)
    d_q, d_k, d_v, d_gq, d_gk, d_xgot, out_got = vals[:7]
    u_zgot = vals[7:]

    d_sum_kept = pick(d_sum, x, 0).astype(F32) + d_xgot.astype(F32)
    d_line = d_sum_kept.reshape(4, ff_w, width)
    d_own_part = pick(d_line, z, 0)
    d_zs = [pick(d_line, (z + s) % 4, 0).astype(BF) for s in (1, 2, 3)]
    d_lin = jnp.concatenate([d_q, d_k, d_v], axis=0)
    d_g = jnp.concatenate([d_gq.sum(axis=(0, 2)), d_gk.sum(axis=(0, 2))])

    def with_gains(arr, gains):
        high = gains.astype(BF)
        row = jnp.concatenate([high, (gains - high.astype(F32)).astype(BF)])[None]
        return jnp.concatenate([arr, jnp.pad(row, ((0, 7), (0, arr.shape[1] - row.shape[1])))], axis=0)

    def gains_of(arr):
        row = arr[-8].astype(F32)
        return row[: 2 * HD] + row[2 * HD : 4 * HD]

    x_far = with_gains(mm(low_placed, d_lin, 1, 1, 2, 2, quarter, BF), d_g)
    x_far, d_lin, d_own_part, *d_zs = phase(x_far, d_lin, d_own_part, *d_zs)
    x_got = to_core(x_far)
    d_zgot = z_send(d_zs)
    d_norm_send = mm(d_lin, qkv_full, 0, 1, (1 - rank) * 2, 2, own // 2, BF)
    d_norm_send, x_got, o_xgot = phase(d_norm_send, x_got, o_xgot)
    d_norm_got = seq_swap(d_norm_send)
    x_sum = mm(low_placed, d_lin, 1, 1, 0, 2, quarter, F32, x_got)
    d_g = d_g + gains_of(x_got)
    x_xs = with_gains(x_sum[quarter:].astype(BF), d_g)
    o_own_part, o_zs = z_parts(o_sum[:quarter], o_xgot)
    x_xs, o_own_part, *o_zs = phase(x_xs, o_own_part, *o_zs)
    x_xgot = to_x(x_xs)
    o_zgot = z_send(o_zs)
    gu_end = jnp.concatenate([z_total(g_own_part, g_zgot), z_total(u_own_part, u_zgot)], axis=0)
    gu_end = gu_end.astype(BF)
    block_out = resid + out_own + out_got.astype(F32)
    d_norm_got, gu_end, x_xgot, block_out, *d_zgot = phase(
        d_norm_got, gu_end, x_xgot, block_out, *d_zgot
    )
    x_own_part, x_zs = z_parts(x_sum[:quarter], x_xgot[:quarter])
    d_g = d_g + gains_of(x_xgot)
    x_own_part, gu_end, *x_zs = phase(x_own_part, gu_end, *[with_gains(part, d_g) for part in x_zs])
    x_zgot = z_send(x_zs)
    gu_swap = seq_swap(gu_end)
    d_norm = mm(d_lin, qkv_full, 0, 1, rank * 2, 2, own // 2, F32, d_norm_got)
    d_tokens = d_resid + unit_rms_back(d_norm, xhat_a, inv_a)
    d_end = z_total(d_own_part, d_zgot).astype(BF)
    o_end = z_total(o_own_part, o_zgot).astype(BF)
    d_tokens, d_end, o_end, *x_zgot = phase(d_tokens, d_end, o_end, *x_zgot)
    for got_s in x_zgot:
        d_g = d_g + gains_of(got_s)
    x_end = z_total(x_own_part, [got_s[:d_dp] for got_s in x_zgot]).astype(BF)
    ends = jnp.concatenate([d_end, o_end, with_gains(x_end, d_g)], axis=0)
    ends, gu_swap = phase(ends, gu_swap)
    swaps = seq_swap(ends)
    d_w_g, dg_g = ff_finish(rank, gu_end[:d_dp], gu_swap[:d_dp], w_gate, gain_f, dp_n)
    d_w_u, dg_u = ff_finish(rank, gu_end[d_dp:], gu_swap[d_dp:], w_up, gain_f, dp_n)
    d_ffn_gain = (dg_g + dg_u)[:, 0]
    d_w_d = ordered(d_end, swaps[:ff_w], rank, 0).reshape(ff_dp, width).astype(F32)
    d_w_o = o_end.astype(F32) + swaps[ff_w : ff_w + d_dp].astype(F32)
    d_gains = d_g + gains_of(swaps)
    both = ordered(x_end, swaps[ff_w + d_dp : -8], rank, 0).astype(F32)
    join = lambda lo, n: both[:, :, lo : lo + n].transpose(1, 0, 2).reshape(d_dp, seq_n * n)
    d_w_q, d_w_k, d_w_v = join(0, q_w), join(q_w, kv_w), join(q_w + kv_w, kv_w)
    d_gq = lax.dynamic_slice_in_dim(d_gains, dp_rank * per, per)
    d_gk = lax.dynamic_slice_in_dim(d_gains, HD + dp_rank * per, per)
    d_attn_gain = jnp.sum(w_query.astype(F32) * d_w_q, axis=1) + jnp.sum(
        w_key.astype(F32) * d_w_k + w_value.astype(F32) * d_w_v, axis=1
    )
    return (
        block_out,
        d_tokens,
        d_attn_gain,
        d_w_q * gain_a,
        d_w_k * gain_a,
        d_w_v * gain_a,
        d_gq,
        d_gk,
        d_w_o,
        d_ffn_gain,
        d_w_g,
        d_w_u,
        d_w_d,
    )


def body_for(*args):
    tokens, lengths = args[:2]
    sizes = (lax.axis_size("dp"), lax.axis_size("seq"))
    exact = lengths.shape[1] == 1 and tokens.shape[0] * sizes[1] == MINLEN
    return (body_fast if sizes == (16, 2) and exact else body)(*args)


def solution(mesh):
    rows, shard, vec = P(("dp", "seq"), None), P("dp", None), P("dp")
    return jax.shard_map(
        body_for,
        mesh=mesh,
        in_specs=(
            rows, shard, vec, shard, shard, shard, vec, vec, shard, vec, shard, shard, shard, rows,
        ),
        out_specs=(
            rows, rows, vec, shard, shard, shard, vec, vec, shard, vec, shard, shard, shard,
        ),
        check_vma=False,
    )
```

```python
from functools import partial
import math

import jax
import jax.numpy as jnp
from jax import lax
from jax.experimental import pallas as pl
from jax.experimental.pallas import tpu as pltpu
from jax.sharding import PartitionSpec as P

H = 16
KV = 8
HD = 64
GROUP = H // KV
MINLEN = 1024

EPSILON = 1e-05
ROPE_BASE = 1000000.0
MASKED_SCORE = -1e30
BF = jnp.bfloat16
F32 = jnp.float32


LONG = pl.CostEstimate(flops=40 << 30, transcendentals=0, bytes_accessed=96 << 20)
SHORT = pl.CostEstimate(flops=1 << 20, transcendentals=0, bytes_accessed=1 << 14)


def dot(left, right, lc, rc):
    return lax.dot_general(left, right, (((lc,), (rc,)), ((), ())), preferred_element_type=F32)


def masked(scores, q0, k0, segs):
    row = lax.broadcasted_iota(jnp.int32, scores.shape, 0) + k0
    col = lax.broadcasted_iota(jnp.int32, scores.shape, 1) + q0
    allowed = row <= col
    if segs is not None:
        allowed = allowed & (segs[0] == segs[1])
    return jnp.where(allowed, scores, MASKED_SCORE)


def attn_fwd_kernel(blk, static, *refs):
    if static:
        q_ref, k_ref, v_ref, o_ref, lse_ref = refs
    else:
        q_ref, k_ref, v_ref, sc_ref, sr_ref, o_ref, lse_ref = refs
    length = q_ref.shape[1]
    keys = k_ref[...].T

    def finish(q0, parts):
        top = parts[0][0].max(axis=0, keepdims=True)
        for s, _ in parts[1:]:
            top = jnp.maximum(top, s.max(axis=0, keepdims=True))
        total, out = 0.0, 0.0
        for s, v in parts:
            p = jnp.exp(s - top)
            total = total + p.sum(axis=0, keepdims=True)
            out = out + dot(v, p.astype(BF), 1, 0)
        o_ref[:, pl.ds(q0, blk)] = (out / total).astype(BF)
        lse_ref[0, :, pl.ds(q0, blk)] = top + jnp.log(total)

    if static:
        for qb in range(length // blk):
            q0 = qb * blk
            q = q_ref[:, q0 : q0 + blk]
            parts = []
            if qb:
                parts.append((dot(keys[:q0], q, 1, 0), v_ref[:, :q0]))
            diag = masked(dot(keys[q0 : q0 + blk], q, 1, 0), 0, 0, None)
            parts.append((diag, v_ref[:, q0 : q0 + blk]))
            finish(q0, parts)
    else:

        @pl.loop(0, length // blk)
        def _(qb):
            q0 = pl.multiple_of(qb * blk, blk)
            s = dot(keys, q_ref[:, pl.ds(q0, blk)], 1, 0)
            s = masked(s, q0, 0, (sc_ref[...], sr_ref[:, pl.ds(q0, blk)]))
            finish(q0, [(s, v_ref[...])])


def lin_back(y, lin, gain, cos_tab, sin_tab):
    first, second = y[: HD // 2], y[HD // 2 :]
    y = jnp.concatenate(
        [first * cos_tab + second * sin_tab, second * cos_tab - first * sin_tab], axis=0
    )
    inv = lax.rsqrt(jnp.mean(lin * lin, axis=0, keepdims=True) + EPSILON)
    xhat = lin * inv
    d_gain = jnp.sum(y * xhat, axis=1, keepdims=True)
    y = y * gain
    return inv * (y - xhat * jnp.mean(y * xhat, axis=0, keepdims=True)), d_gain


def attn_bwd_kernel(blk, static, *refs):
    lin_refs = None
    if static:
        q_ref, k_ref, v_ref, do_ref, o_ref, lse_ref = refs[:6]
        lin_refs = refs[6:12]
        dq_ref, dk_ref, dv_ref, dgq_ref, dgk_ref, dk_acc, dv_acc = refs[12:]
        ql_ref, kl_ref, gq_ref, gk_ref, cos_ref, sin_ref = lin_refs
    else:
        (q_ref, k_ref, v_ref, do_ref, o_ref, lse_ref, sc_ref, sr_ref,
         dq_ref, dk_ref, dv_ref, dk_acc, dv_acc) = refs
    length = q_ref.shape[1]
    member = lax.rem(pl.program_id(0), GROUP)
    keys = k_ref[...].T
    values = v_ref[...].T

    @pl.when(member == 0)
    def _():
        dk_acc[...] = jnp.zeros_like(dk_acc)
        dv_acc[...] = jnp.zeros_like(dv_acc)

    def part(q, d_out, lse, delta, k_lo, k_n, q0, segs, mask):
        rows = pl.ds(k_lo, k_n)
        k_blk, v_blk = keys[k_lo : k_lo + k_n], values[k_lo : k_lo + k_n]
        s = dot(k_blk, q, 1, 0)
        if mask:
            s = masked(s, q0, k_lo, segs)
        p = jnp.exp(s - lse)
        dv_acc[rows, :] += dot(p.astype(BF), d_out, 1, 1)
        dp = dot(v_blk, d_out, 1, 0)
        ds = (p * (dp - delta)).astype(BF)
        dk_acc[rows, :] += dot(ds, q, 1, 1)
        return dot(k_ref[:, rows], ds, 1, 0)

    def prepare(q0):
        cols = pl.ds(q0, blk)
        d_out = do_ref[:, cols]
        delta = (d_out.astype(F32) * o_ref[:, cols].astype(F32)).sum(axis=0, keepdims=True)
        return cols, q_ref[:, cols], d_out, lse_ref[0, :, cols], delta

    scale = 1.0 / math.sqrt(HD)
    if static:
        for qb in range(length // blk):
            q0 = qb * blk
            cols, q, d_out, lse, delta = prepare(q0)
            dq = part(q, d_out, lse, delta, q0, blk, q0, None, True)
            if qb:
                dq = dq + part(q, d_out, lse, delta, 0, q0, q0, None, False)
            d_lin, d_gain = lin_back(
                dq * scale, ql_ref[:, cols], gq_ref[...], cos_ref[:, cols], sin_ref[:, cols]
            )
            dq_ref[:, cols] = d_lin.astype(BF)
            dgq_ref[0] = d_gain if qb == 0 else dgq_ref[0] + d_gain
    else:

        @pl.loop(0, length // blk)
        def _(qb):
            q0 = pl.multiple_of(qb * blk, blk)
            cols, q, d_out, lse, delta = prepare(q0)
            dq = part(q, d_out, lse, delta, 0, length, q0, (sc_ref[...], sr_ref[:, cols]), True)
            dq_ref[:, cols] = (dq * scale).astype(BF)

    @pl.when(member == GROUP - 1)
    def _():
        dk = dk_acc[...].T
        if static:
            dk, d_gain = lin_back(dk, kl_ref[...], gk_ref[...], cos_ref[...], sin_ref[...])
            dgk_ref[0] = d_gain
        dk_ref[...] = dk.astype(BF)
        dv_ref[...] = dv_acc[...].T.astype(BF)


def attn_specs(length):
    q_spec = pl.BlockSpec((HD, length), lambda h: (h, 0))
    kv_spec = pl.BlockSpec((HD, length), lambda h: (h // GROUP, 0))
    lse_spec = pl.BlockSpec((1, 1, length), lambda h: (h, 0, 0))
    seg_specs = [
        pl.BlockSpec((length, 1), lambda h: (0, 0)),
        pl.BlockSpec((1, length), lambda h: (0, 0)),
    ]
    return q_spec, kv_spec, lse_spec, seg_specs


def attn_fwd(q, k, v, segs):
    rows, length = q.shape
    heads = rows // HD
    static = segs is None
    q_spec, kv_spec, lse_spec, seg_specs = attn_specs(length)
    extra = () if static else (segs[:, None], segs[None, :])
    return pl.pallas_call(
        partial(attn_fwd_kernel, min(256, length), static),
        grid=(heads,),
        in_specs=[q_spec, kv_spec, kv_spec] + ([] if static else seg_specs),
        out_specs=[q_spec, lse_spec],
        out_shape=[
            jax.ShapeDtypeStruct((rows, length), BF),
            jax.ShapeDtypeStruct((heads, 1, length), F32),
        ],
        cost_estimate=SHORT,
        name="attn_fwd",
    )(q, k, v, *extra)


def attn_bwd(q, k, v, d_out, out, lse, segs, lins=()):
    rows, length = q.shape
    heads = rows // HD
    static = segs is None
    q_spec, kv_spec, lse_spec, seg_specs = attn_specs(length)
    extra = tuple(lins) if static else (segs[:, None], segs[None, :])
    whole = lambda arr: pl.BlockSpec(arr.shape, lambda h: (0, 0))
    lin_specs = [q_spec, pl.BlockSpec((HD, length), lambda h: (heads + h // GROUP, 0))]
    lin_specs += [whole(arr) for arr in lins[2:]]
    gain_specs = [
        pl.BlockSpec((1, HD, 1), lambda h: (h, 0, 0)),
        pl.BlockSpec((1, HD, 1), lambda h: (h // GROUP, 0, 0)),
    ]
    gain_shapes = [
        jax.ShapeDtypeStruct((heads, HD, 1), F32),
        jax.ShapeDtypeStruct((heads // GROUP, HD, 1), F32),
    ]
    return pl.pallas_call(
        partial(attn_bwd_kernel, min(256, length), static),
        grid=(heads,),
        in_specs=[q_spec, kv_spec, kv_spec, q_spec, q_spec, lse_spec]
        + (lin_specs if static else seg_specs),
        out_specs=[q_spec, kv_spec, kv_spec] + (gain_specs if static else []),
        out_shape=[
            jax.ShapeDtypeStruct((rows, length), BF),
            jax.ShapeDtypeStruct(k.shape, BF),
            jax.ShapeDtypeStruct(v.shape, BF),
        ]
        + (gain_shapes if static else []),
        scratch_shapes=[pltpu.VMEM((length, HD), F32), pltpu.VMEM((length, HD), F32)],
        cost_estimate=LONG,
        name="attn_bwd",
    )(q, k, v, d_out, out, lse, *extra)


def ff_prep_kernel(rank_ref, gate_ref, up_ref, down_ref, gain_ref, out_ref):
    first = rank_ref[0] == 0
    d_dp, ff_all = gate_ref.shape
    ff_w = down_ref.shape[0] // 2
    dp_n = ff_all // (2 * ff_w)
    gain = gain_ref[...]
    for half, ref in enumerate((gate_ref, up_ref)):
        for i in range(dp_n):
            lo = ref[:, 2 * i * ff_w : (2 * i + 1) * ff_w].astype(F32)
            hi = ref[:, (2 * i + 1) * ff_w : (2 * i + 2) * ff_w].astype(F32)
            at = (half * dp_n + hidden_place(i)) * ff_w
            out_ref[:d_dp, at : at + ff_w] = (jnp.where(first, lo, hi) * gain).astype(BF)
    for b in range(ff_w // 16):
        lo = down_ref[16 * b : 16 * b + 16, :]
        hi = down_ref[ff_w + 16 * b : ff_w + 16 * b + 16, :]
        rows = jnp.where(first, lo.astype(F32), hi.astype(F32)).astype(BF)
        for band, at, frm, to in down_places(b, rows.shape[1], ff_all):
            out_ref[d_dp + 16 * band : d_dp + 16 * band + 16, at : at + to - frm] = rows[:, frm:to]


def hidden_place(i):
    return (i % 2 * 2 + i // 2 % 2) * 4 + i // 4


def down_places(b, width, ff_all):
    places, start = [], b * width
    while start < (b + 1) * width:
        band = start // ff_all
        end = min((band + 1) * ff_all, (b + 1) * width)
        places.append((band, start - band * ff_all, start - b * width, end - b * width))
        start = end
    return places


def ff_prep(rank, w_gate, w_up, w_down, gain):
    d_dp, ff_all = w_gate.shape
    bands = w_down.shape[0] // 2 * w_down.shape[1] // ff_all
    whole = lambda arr: pl.BlockSpec(arr.shape, lambda i, r: (0, 0))
    return pl.pallas_call(
        ff_prep_kernel,
        grid_spec=pltpu.PrefetchScalarGridSpec(
            num_scalar_prefetch=1,
            grid=(1,),
            in_specs=[whole(w_gate), whole(w_up), whole(w_down), whole(gain)],
            out_specs=pl.BlockSpec((d_dp + bands, ff_all), lambda i, r: (0, 0)),
        ),
        out_shape=jax.ShapeDtypeStruct((d_dp + bands, ff_all), BF),
        name="ff_prep",
    )(rank[None], w_gate, w_up, w_down, gain)


def ffn_core_kernel(sub, fresh, *refs):
    x_ref, g_ref, wg_ref, wu_ref, wd_ref = refs[:5]
    hid_ref, dg_ref, du_ref, dx_out, out_out, down, dx_ref, out_ref = refs[5:] if fresh else refs[8:]
    dp_n, d_dp, blk = wg_ref.shape
    width = g_ref.shape[1]
    ff_all = wd_ref.shape[2]
    ff_w = down.shape[0] // dp_n
    step = pl.program_id(0)

    @pl.when(step == 0)
    def _():
        dx_ref[...] = jnp.zeros_like(dx_ref)
        out_ref[...] = jnp.zeros_like(out_ref)

        @pl.loop(0, dp_n)
        def _(i):
            for b in range(ff_w // 16):
                at_i = (lax.rem(i, 2) * 2 + lax.rem(lax.div(i, 2), 2)) * 4 + lax.div(i, 4)
                rows = pl.ds(pl.multiple_of(at_i * ff_w + 16 * b, 16), 16)
                for band, at, frm, to in down_places(b, width, ff_all):
                    down[rows, frm:to] = wd_ref[i, 16 * band : 16 * band + 16, at : at + to - frm]

    @pl.loop(0, blk // sub)
    def _(s):
        cols = pl.ds(pl.multiple_of(s * sub, 128), sub)
        rows = pl.ds(pl.multiple_of(step * blk + s * sub, 128), sub)
        x = x_ref[...]
        w_gate = wg_ref[:, :, cols].reshape(dp_n * d_dp, sub)
        w_up = wu_ref[:, :, cols].reshape(dp_n * d_dp, sub)
        w_down = down[rows, :]
        gate = dot(x, w_gate, 1, 0)
        up = dot(x, w_up, 1, 0)
        d_hid = dot(g_ref[...], w_down, 1, 1)
        sig = 1.0 / (1.0 + jnp.exp(-gate))
        silu = gate * sig
        hidden = (silu * up).astype(BF)
        d_gate = (d_hid * up * (sig * (1.0 + gate * (1.0 - sig)))).astype(BF)
        d_up = (d_hid * silu).astype(BF)
        hid_ref[:, cols] = hidden
        dg_ref[:, cols] = d_gate
        du_ref[:, cols] = d_up
        dx_ref[...] += dot(d_gate, w_gate, 1, 1) + dot(d_up, w_up, 1, 1)
        out_ref[...] += dot(hidden, w_down, 1, 0)

    @pl.when(step == pl.num_programs(0) - 1)
    def _():
        dx_out[...] = dx_ref[...].astype(dx_out.dtype)
        out_out[...] = out_ref[...].astype(out_out.dtype)


def ffn_core(x, g, packed, earlier, half, dp_n, d_dp, ff_w):
    rows, width = x.shape
    ff = dp_n * ff_w
    blk = ff // 2
    fresh = earlier is None
    whole = pl.BlockSpec((rows, width), lambda j: (0, 0))
    wide = pl.BlockSpec((rows, blk), lambda j: (half, j))
    bands = packed.shape[1] - d_dp
    keep = pl.BlockSpec(memory_space=pl.ANY)
    wide_shape = jax.ShapeDtypeStruct((2 * rows, ff), BF)
    return pl.pallas_call(
        partial(ffn_core_kernel, 384, fresh),
        grid=(2,),
        in_specs=[
            whole,
            whole,
            pl.BlockSpec((dp_n, d_dp, blk), lambda j: (0, 0, j)),
            pl.BlockSpec((dp_n, d_dp, blk), lambda j: (0, 0, 2 + j)),
            pl.BlockSpec(
                (dp_n, bands, 2 * ff), lambda j: (0, d_dp // bands, 0), pipeline_mode=pl.Buffered(1)
            ),
        ]
        + ([] if fresh else [keep] * 3),
        out_specs=[wide, wide, wide, whole, whole],
        out_shape=[wide_shape] * 3
        + [jax.ShapeDtypeStruct((rows, width), F32 if fresh else BF)] * 2,
        scratch_shapes=[pltpu.VMEM((ff, width), BF)] + [pltpu.VMEM((rows, width), F32)] * 2,
        input_output_aliases={} if fresh else {5: 0, 6: 1, 7: 2},
        compiler_params=pltpu.CompilerParams(vmem_limit_bytes=60 << 20),
        cost_estimate=SHORT,
        name="ffn_core",
    )(x, g, packed, packed, packed, *(() if fresh else earlier))


def mm_kernel(lc, rc, first_ref, a_ref, b_ref, *refs):
    total = dot(a_ref[...], b_ref[...], lc, rc)
    if len(refs) == 2:
        total = total + refs[0][...].astype(F32)
    refs[-1][...] = total.astype(refs[-1].dtype)


def mm(a, b, lc, rc, first, count, rows, dtype, add=None, add_first=0, cost=SHORT):
    cols = b.shape[1 - rc]
    a_spec = (
        pl.BlockSpec((rows, a.shape[1]), lambda i, f: (f[0] + i, 0))
        if lc
        else pl.BlockSpec((a.shape[0], rows), lambda i, f: (0, f[0] + i))
    )
    in_specs = [a_spec, pl.BlockSpec(b.shape, lambda i, f: (0, 0))]
    args = [a, b]
    if add is not None:
        in_specs.append(pl.BlockSpec((rows, cols), lambda i, f: (add_first + i, 0)))
        args.append(add)
    return pl.pallas_call(
        partial(mm_kernel, lc, rc),
        grid_spec=pltpu.PrefetchScalarGridSpec(
            num_scalar_prefetch=1,
            grid=(count,),
            in_specs=in_specs,
            out_specs=pl.BlockSpec((rows, cols), lambda i, f: (i, 0)),
        ),
        out_shape=jax.ShapeDtypeStruct((count * rows, cols), dtype),
        compiler_params=pltpu.CompilerParams(vmem_limit_bytes=48 << 20),
        cost_estimate=cost,
        name="mm",
    )(jnp.asarray(first, jnp.int32)[None], *args)


def resid_back_kernel(dx_ref, got_ref, cot_ref, xhat_ref, inv_ref, out_ref, low_ref):
    y = dx_ref[...] + got_ref[...].astype(F32)
    d_resid = cot_ref[...] + unit_rms_back(y, xhat_ref[...], inv_ref[...])
    out_ref[...] = d_resid
    low_ref[...] = d_resid.astype(BF)


def resid_back(dx_own, dx_got, cotangent, xhat, inv):
    rows, width = dx_own.shape
    wide = pl.BlockSpec((rows // 4, width), lambda i: (i, 0))
    return pl.pallas_call(
        resid_back_kernel,
        grid=(4,),
        in_specs=[wide, wide, wide, wide, pl.BlockSpec((rows // 4, 1), lambda i: (i, 0))],
        out_specs=[wide, wide],
        out_shape=[
            jax.ShapeDtypeStruct((rows, width), F32),
            jax.ShapeDtypeStruct((rows, width), BF),
        ],
        cost_estimate=LONG,
        name="resid_back",
    )(dx_own, dx_got, cotangent, xhat, inv)


def ff_finish_kernel(rank_ref, mine_ref, theirs_ref, w_ref, gain_ref, out_ref, d_gain_ref):
    first = rank_ref[0] == 0
    mine, theirs = mine_ref[...].astype(F32), theirs_ref[...].astype(F32)
    low_ = jnp.where(first, mine, theirs)
    high = jnp.where(first, theirs, mine)
    gain = gain_ref[...]
    dp_n = gain_ref.shape[1]
    n = mine.shape[1] // dp_n
    total = jnp.zeros((mine.shape[0], 2 * n), F32)
    for i in range(dp_n):
        cols = slice(2 * i * n, 2 * (i + 1) * n)
        at = hidden_place(i) * n
        pair = jnp.concatenate([low_[:, at : at + n], high[:, at : at + n]], axis=1)
        total = total + pair * w_ref[:, cols].astype(F32)
        out_ref[:, cols] = pair * gain[:, :1]
    d_gain_ref[...] = total.sum(axis=1, keepdims=True)


def ff_finish(rank, mine, theirs, weight, gain, dp_n):
    gain = jnp.broadcast_to(gain, (gain.shape[0], dp_n))
    whole = lambda arr: pl.BlockSpec(arr.shape, lambda i, r: (0, 0))
    return pl.pallas_call(
        ff_finish_kernel,
        grid_spec=pltpu.PrefetchScalarGridSpec(
            num_scalar_prefetch=1,
            grid=(1,),
            in_specs=[whole(mine), whole(theirs), whole(weight), whole(gain)],
            out_specs=[
                pl.BlockSpec(weight.shape, lambda i, r: (0, 0)),
                pl.BlockSpec((weight.shape[0], 1), lambda i, r: (0, 0)),
            ],
        ),
        out_shape=[
            jax.ShapeDtypeStruct(weight.shape, F32),
            jax.ShapeDtypeStruct((weight.shape[0], 1), F32),
        ],
        name="ff_finish",
    )(rank[None], mine, theirs, weight, gain)


def assemble_kernel(place_ref, *refs):
    out_ref = refs[-1]
    rows = refs[0].shape[0]
    z, x, core = place_ref[0], place_ref[1], place_ref[2]
    for n, ref in enumerate(refs[:-1]):
        b, a, s = n // 8, n // 4 % 2, n % 4
        at = (lax.rem(z + s, 4) * 2 + (a + x - 2 * a * x)) * 2 + (b + core - 2 * b * core)
        out_ref[at] = ref[...]


def assemble(place, pieces):
    shape = pieces[0].shape
    return pl.pallas_call(
        assemble_kernel,
        grid_spec=pltpu.PrefetchScalarGridSpec(
            num_scalar_prefetch=1,
            grid=(1,),
            in_specs=[pl.BlockSpec(shape, lambda i, p: (0, 0))] * 16,
            out_specs=pl.BlockSpec((16,) + shape, lambda i, p: (0, 0, 0)),
        ),
        out_shape=jax.ShapeDtypeStruct((16,) + shape, BF),
        name="assemble",
    )(place, *pieces)


def pick(arr, index, axis):
    return lax.dynamic_index_in_dim(arr, index, axis, keepdims=False)


def ordered(mine, other, rank, axis):
    low_ = jnp.where(rank == 0, mine, other)
    high = jnp.where(rank == 0, other, mine)
    return jnp.stack([low_, high], axis=axis)


def dp_gather(shard):
    return lax.all_gather(shard, "dp", axis=0, tiled=False)


def dp_scatter(parts):
    flat = parts.reshape((-1,) + parts.shape[2:])
    return lax.psum_scatter(flat, "dp", scatter_dimension=0, tiled=True).astype(F32)


def dp_place():
    index = lax.axis_index("dp")
    return index // 4, (index // 2) % 2, index % 2


def to_core(arr):
    return lax.ppermute(arr, "dp", [(j, j ^ 1) for j in range(16)])


def to_x(arr):
    return lax.ppermute(arr, "dp", [(j, j ^ 2) for j in range(16)])


def to_z(arr, s):
    return lax.ppermute(arr, "dp", [(j, (j + 4 * s) % 16) for j in range(16)])


def gather_z(shard):
    return [shard] + [to_z(shard, 4 - s) for s in (1, 2, 3)]


def gather_rest(line):
    plane = line + [to_x(piece) for piece in line]
    return plane + [to_core(piece) for piece in plane]


def place_matrix(width):
    z, x, core = dp_place()
    n = jnp.arange(width, dtype=jnp.int32)
    part = width // 16
    block = (
        (z + n // part % 4) % 4 * 4
        + jnp.bitwise_xor(x, n // (4 * part) % 2) * 2
        + jnp.bitwise_xor(core, n // (8 * part))
    )
    source = block * part + n % part
    return (n[:, None] == source[None, :]).astype(BF)


def phase(*values):
    return lax.optimization_barrier(values)


def z_parts(kept, got):
    r = kept.shape[0] // 4
    sums = [kept[s * r : s * r + r] + got[s * r : s * r + r].astype(F32) for s in range(4)]
    return sums[0], [part.astype(BF) for part in sums[1:]]


def z_send(parts):
    return [to_z(part, s + 1) for s, part in enumerate(parts)]


def z_total(kept, got):
    total = kept
    for term in got:
        total = total + term.astype(F32)
    return total


def after(value, *others):
    return lax.optimization_barrier((value,) + tuple(others))[0]


def seq_swap(arr):
    return lax.ppermute(arr, "seq", [(0, 1), (1, 0)])


def seq_tokens(rows):
    if lax.axis_size("seq") == 2:
        return jnp.concatenate([rows, seq_swap(rows)], axis=0)
    return lax.all_gather(rows, "seq", axis=0, tiled=True)


def seq_tokens_sum(parts):
    if lax.axis_size("seq") == 2:
        own = parts.shape[0] // 2
        return parts[:own] + seq_swap(parts[own:].astype(BF)).astype(F32)
    return lax.psum_scatter(parts.astype(BF), "seq", scatter_dimension=0, tiled=True).astype(F32)


def seq_stack(arr):
    if lax.axis_size("seq") == 2:
        return ordered(arr, seq_swap(arr), lax.axis_index("seq"), 0)
    return lax.all_gather(arr, "seq", axis=0, tiled=False)


def heads_to_tokens(arr):
    count = lax.axis_size("seq")
    rows, length = arr.shape
    if count == 2:
        rank = lax.axis_index("seq")
        own = length // 2
        mine = lax.dynamic_slice_in_dim(arr, rank * own, own, 1)
        theirs = seq_swap(lax.dynamic_slice_in_dim(arr, (1 - rank) * own, own, 1))
        return ordered(mine, theirs, rank, 0).reshape(2 * rows, own)
    return lax.all_to_all(arr, "seq", split_axis=1, concat_axis=0, tiled=True)


def tokens_to_heads(arr):
    count = lax.axis_size("seq")
    rows, own = arr.shape
    if count == 2:
        rank = lax.axis_index("seq")
        half = rows // 2
        mine = lax.dynamic_slice_in_dim(arr, rank * half, half, 0)
        theirs = seq_swap(lax.dynamic_slice_in_dim(arr, (1 - rank) * half, half, 0))
        first = jnp.where(rank == 0, mine, theirs)
        second = jnp.where(rank == 0, theirs, mine)
        return jnp.concatenate([first, second], axis=1)
    return lax.all_to_all(arr, "seq", split_axis=0, concat_axis=1, tiled=True)


def pack_layout(seq_lens, total):
    places = jnp.arange(total, dtype=jnp.int32)
    ends = jnp.cumsum(seq_lens)
    starts = ends - seq_lens
    segment = jnp.sum((places[:, None] >= ends[None, :]).astype(jnp.int32), axis=1)
    starts_ext = jnp.concatenate([starts, ends[-1:]])
    labels = jnp.arange(seq_lens.shape[0] + 1, dtype=jnp.int32)
    offset = jnp.sum(jnp.where(segment[:, None] == labels[None, :], starts_ext[None, :], 0), axis=1)
    return segment, places - offset, segment < seq_lens.shape[0]


def unit_rms(values):
    inv = lax.rsqrt(jnp.mean(values * values, axis=-1, keepdims=True) + EPSILON)
    return values * inv, inv


def unit_rms_back(y, xhat, inv):
    return inv * (y - xhat * jnp.mean(y * xhat, axis=-1, keepdims=True))


def head_prep(lin, gain, cos_tab, sin_tab, scale):
    u = lin.reshape(-1, HD, lin.shape[1])
    inv = lax.rsqrt(jnp.mean(u * u, axis=1, keepdims=True) + EPSILON)
    u = u * inv * gain[None, :, None]
    first, second = u[:, : HD // 2], u[:, HD // 2 :]
    out = jnp.concatenate(
        [first * cos_tab - second * sin_tab, second * cos_tab + first * sin_tab], axis=1
    )
    return (out * scale).astype(BF).reshape(lin.shape)


def head_prep_back(grad, lin, gain, cos_tab, sin_tab):
    y = grad.astype(F32).reshape(-1, HD, lin.shape[1])
    first, second = y[:, : HD // 2], y[:, HD // 2 :]
    y = jnp.concatenate(
        [first * cos_tab + second * sin_tab, second * cos_tab - first * sin_tab], axis=1
    )
    u = lin.reshape(y.shape)
    inv = lax.rsqrt(jnp.mean(u * u, axis=1, keepdims=True) + EPSILON)
    xhat = u * inv
    d_gain = jnp.sum(y * xhat, axis=(0, 2))
    y = y * gain[None, :, None]
    d_lin = inv * (y - xhat * jnp.mean(y * xhat, axis=1, keepdims=True))
    return d_lin.astype(BF).reshape(lin.shape), d_gain


def body(
    tokens, lengths, attn_gain, w_query, w_key, w_value, query_gain, key_gain, w_out,
    ffn_gain, w_gate, w_up, w_down, cotangent,
):
    seq_n = lax.axis_size("seq")
    dp_n = lax.axis_size("dp")
    rank = lax.axis_index("seq")
    dp_rank = lax.axis_index("dp")
    own, width = tokens.shape
    length = own * seq_n
    q_w, kv_w = H * HD // seq_n, KV * HD // seq_n
    ff_dp = w_down.shape[0]
    ff_w = ff_dp // seq_n
    ff = ff_w * dp_n
    d_dp = w_query.shape[0]

    full = length == MINLEN * lengths.shape[1]
    segment, positions, valid = pack_layout(lengths[0], length)
    segs = None if full and lengths.shape[1] == 1 else segment
    my_valid = lax.dynamic_slice_in_dim(valid, rank * own, own).astype(F32)[:, None]

    def keep_valid(arr):
        return arr if full else arr * my_valid

    gain_a = attn_gain.astype(F32)[:, None]
    gain_f = ffn_gain.astype(F32)[:, None]

    def my_cols(w, n):
        return lax.dynamic_slice_in_dim(w, rank * n, n, 1)

    qkv_part = jnp.concatenate(
        [my_cols(w_query, q_w), my_cols(w_key, kv_w), my_cols(w_value, kv_w)], axis=1
    )
    qkv_part = (qkv_part.astype(F32) * gain_a).astype(BF)
    gains = jnp.concatenate([query_gain, key_gain])
    gains = jnp.pad(gains[None, :], ((0, 7), (0, qkv_part.shape[1] - gains.shape[0])))
    pick_ff = lambda w: pick(w.reshape(d_dp, dp_n, seq_n, ff_w), rank, 2).reshape(d_dp, ff)
    gu_part = jnp.concatenate([pick_ff(w_gate), pick_ff(w_up)], axis=1)
    gu_part = (gu_part.astype(F32) * gain_f).astype(BF)
    down_part = pick(w_down.reshape(seq_n, ff_w, width), rank, 0)

    gu_full = lax.all_gather(gu_part, "dp", axis=0, tiled=True)
    down_full = lax.all_gather(down_part, "dp", axis=0, tiled=True)
    got = dp_gather(jnp.concatenate([qkv_part, gains], axis=0))
    qkv_full = got[:, :d_dp].reshape(width, -1)
    per = query_gain.shape[0]
    gain_q = got[:, d_dp, :per].reshape(-1).astype(F32)
    gain_k = got[:, d_dp, per : 2 * per].reshape(-1).astype(F32)
    out_full = dp_gather(w_out).reshape(H * HD, width)

    xhat_a, inv_a = unit_rms(tokens)
    low_own = xhat_a.astype(BF)
    if seq_n == 2:
        low_a = ordered(low_own, seq_swap(low_own), rank, 0).reshape(length, width)
    else:
        low_a = lax.all_gather(low_own, "seq", axis=0, tiled=True)
    lin = dot(qkv_full, low_a, 0, 1)
    q_lin, k_lin = lin[:q_w], lin[q_w : q_w + kv_w]
    values = lin[q_w + kv_w :].astype(BF)
    freqs = ROPE_BASE ** (-(jnp.arange(HD // 2, dtype=F32) * (2.0 / HD)))
    angles = freqs[:, None] * positions.astype(F32)[None, :]
    cos_tab, sin_tab = jnp.cos(angles), jnp.sin(angles)
    queries = head_prep(q_lin, gain_q, cos_tab, sin_tab, 1.0 / math.sqrt(HD))
    keys = head_prep(k_lin, gain_k, cos_tab, sin_tab, 1.0)
    att_heads, lse = attn_fwd(queries, keys, values, segs)
    attended = heads_to_tokens(att_heads)
    resid = tokens + dot(attended, out_full, 0, 0)

    xhat_f, inv_f = unit_rms(resid)
    grad = keep_valid(cotangent)
    x_all = seq_tokens(xhat_f.astype(BF))
    g_all = seq_tokens(grad.astype(BF))
    gate = dot(x_all, gu_full[:, :ff], 1, 0)
    up = dot(x_all, gu_full[:, ff:], 1, 0)
    d_hidden = dot(g_all, down_full, 1, 1)
    sig = jax.nn.sigmoid(gate)
    silu = gate * sig
    hidden = (silu * up).astype(BF)
    d_gate = (d_hidden * up * sig * (1.0 + gate * (1.0 - sig))).astype(BF)
    d_up = (d_hidden * silu).astype(BF)
    d_ffn = dot(d_gate, gu_full[:, :ff], 1, 1) + dot(d_up, gu_full[:, ff:], 1, 1)
    d_ffn = seq_tokens_sum(d_ffn)
    d_resid = grad + unit_rms_back(d_ffn, xhat_f, inv_f)

    block_out = keep_valid(resid + seq_tokens_sum(dot(hidden, down_full, 1, 0)))
    d_w_g = dp_scatter(dot(x_all, d_gate, 0, 0).astype(BF).reshape(dp_n, d_dp, ff))
    d_w_u = dp_scatter(dot(x_all, d_up, 0, 0).astype(BF).reshape(dp_n, d_dp, ff))
    d_w_d = dp_scatter(dot(hidden, g_all, 0, 0).astype(BF).reshape(dp_n, ff_w, width))

    def full_ff(shard):
        both = seq_stack(shard.astype(BF)).reshape(seq_n, d_dp, dp_n, ff_w)
        return both.transpose(1, 2, 0, 3).reshape(d_dp, dp_n * seq_n * ff_w).astype(F32)

    d_w_g, d_w_u = full_ff(d_w_g), full_ff(d_w_u)
    d_w_d = seq_stack(d_w_d.astype(BF)).reshape(ff_dp, width).astype(F32)
    d_ffn_gain = jnp.sum(w_gate.astype(F32) * d_w_g + w_up.astype(F32) * d_w_u, axis=1)

    r_low = d_resid.astype(BF)
    d_att = tokens_to_heads(dot(out_full, r_low, 1, 1).astype(BF))
    d_w_o = dp_scatter(dot(attended, r_low, 1, 0).astype(BF).reshape(dp_n, d_dp, width))
    if segs is None:
        lins = (lin, lin, gain_q[:, None], gain_k[:, None], cos_tab, sin_tab)
        d_q, d_k, d_v, d_gq, d_gk = attn_bwd(queries, keys, values, d_att, att_heads, lse, None, lins)
        d_gq, d_gk = d_gq.sum(axis=(0, 2)), d_gk.sum(axis=(0, 2))
    else:
        d_q, d_k, d_v = attn_bwd(queries, keys, values, d_att, att_heads, lse, segs)
        d_q, d_gq = head_prep_back(d_q, q_lin, gain_q, cos_tab, sin_tab)
        d_k, d_gk = head_prep_back(d_k, k_lin, gain_k, cos_tab, sin_tab)
    d_lin = jnp.concatenate([d_q, d_k, d_v], axis=0)
    d_norm = dot(d_lin, qkv_full, 0, 1)
    if seq_n == 2:
        other = lax.dynamic_slice_in_dim(d_norm, (1 - rank) * own, own, 0)
        d_norm = lax.dynamic_slice_in_dim(d_norm, rank * own, own, 0)
        d_norm = d_norm + seq_swap(other.astype(BF)).astype(F32)
    else:
        d_norm = seq_tokens_sum(d_norm)
    d_tokens = d_resid + unit_rms_back(d_norm, xhat_a, inv_a)

    d_w_x = dot(low_a, d_lin, 0, 1).astype(BF).reshape(dp_n, d_dp, -1)
    d_g = jnp.concatenate([d_gq, d_gk]).astype(BF)
    d_g = jnp.pad(d_g[None, :], ((0, 7), (0, d_w_x.shape[2] - d_g.shape[0])))
    d_g = jnp.broadcast_to(d_g[None], (dp_n,) + d_g.shape)
    d_w_x = dp_scatter(jnp.concatenate([d_w_x, d_g], axis=1))
    d_w_x = seq_stack(d_w_x.astype(BF)).astype(F32)
    both = d_w_x[:, :d_dp]
    join = lambda lo, n: both[:, :, lo : lo + n].transpose(1, 0, 2).reshape(d_dp, seq_n * n)
    d_w_q, d_w_k, d_w_v = join(0, q_w), join(q_w, kv_w), join(q_w + kv_w, kv_w)
    d_gains = jnp.sum(d_w_x[:, d_dp, : 2 * HD], axis=0)
    d_gq = lax.dynamic_slice_in_dim(d_gains, dp_rank * per, per)
    d_gk = lax.dynamic_slice_in_dim(d_gains, HD + dp_rank * per, per)
    d_attn_gain = jnp.sum(w_query.astype(F32) * d_w_q, axis=1) + jnp.sum(
        w_key.astype(F32) * d_w_k + w_value.astype(F32) * d_w_v, axis=1
    )
    d_w_o = jnp.sum(seq_stack(d_w_o.astype(BF)).astype(F32), axis=0)
    return (
        block_out,
        d_tokens,
        d_attn_gain,
        d_w_q * gain_a,
        d_w_k * gain_a,
        d_w_v * gain_a,
        d_gq,
        d_gk,
        d_w_o,
        d_ffn_gain,
        d_w_g * gain_f,
        d_w_u * gain_f,
        d_w_d,
    )


def body_fast(
    tokens, lengths, attn_gain, w_query, w_key, w_value, query_gain, key_gain, w_out,
    ffn_gain, w_gate, w_up, w_down, cotangent,
):
    seq_n, dp_n = 2, 16
    rank = lax.axis_index("seq")
    dp_rank = lax.axis_index("dp")
    place = jnp.stack(dp_place()).astype(jnp.int32)
    own, width = tokens.shape
    length = own * seq_n
    q_w, kv_w = H * HD // seq_n, KV * HD // seq_n
    ff_dp = w_down.shape[0]
    ff_w = ff_dp // seq_n
    ff = ff_w * dp_n
    d_dp = w_query.shape[0]
    gain_a = attn_gain.astype(F32)[:, None]
    gain_f = ffn_gain.astype(F32)[:, None]
    per = query_gain.shape[0]

    packed = ff_prep(rank, w_gate, w_up, w_down, gain_f)
    ff_full = lax.all_gather(packed, "dp", axis=0, tiled=False)

    def my_cols(w, n):
        return lax.dynamic_slice_in_dim(w, rank * n, n, 1)

    qkv_part = jnp.concatenate(
        [my_cols(w_query, q_w), my_cols(w_key, kv_w), my_cols(w_value, kv_w)], axis=1
    )
    qkv_part = (qkv_part.astype(F32) * gain_a).astype(BF)
    gains = jnp.concatenate([query_gain, key_gain])
    gains = jnp.pad(gains[None, :], ((0, 7), (0, qkv_part.shape[1] - gains.shape[0])))
    qkv_line = gather_z(jnp.concatenate([qkv_part, gains], axis=0))
    xhat_a, inv_a = unit_rms(tokens)
    low_own = xhat_a.astype(BF)
    low_other = seq_swap(low_own)
    qkv_pieces = gather_rest(qkv_line)
    g_own = cotangent.astype(BF)
    g_other = seq_swap(g_own)
    got = assemble(place, qkv_pieces)
    qkv_full = got[:, :d_dp].reshape(width, -1)
    gain_q = got[:, d_dp, :per].reshape(-1).astype(F32)
    gain_k = got[:, d_dp, per : 2 * per].reshape(-1).astype(F32)
    out_line = gather_z(after(w_out, *qkv_line))

    low_a = ordered(low_own, low_other, rank, 0).reshape(length, width)
    lin = dot(qkv_full, low_a, 0, 1)
    q_lin, k_lin = lin[:q_w], lin[q_w : q_w + kv_w]
    values = lin[q_w + kv_w :].astype(BF)
    freqs = ROPE_BASE ** (-(jnp.arange(HD // 2, dtype=F32) * (2.0 / HD)))
    angles = freqs[:, None] * jnp.arange(length, dtype=jnp.int32).astype(F32)[None, :]
    cos_tab, sin_tab = jnp.cos(angles), jnp.sin(angles)
    queries = head_prep(q_lin, gain_q, cos_tab, sin_tab, 1.0 / math.sqrt(HD))
    keys = head_prep(k_lin, gain_k, cos_tab, sin_tab, 1.0)
    place_mat = place_matrix(width)
    low_placed = dot(place_mat, low_a, 0, 1).astype(BF)
    queries, low_placed, g_other, *out_line = phase(queries, low_placed, g_other, *out_line)
    out_pieces = gather_rest(out_line)
    att_heads, lse = attn_fwd(queries, keys, values, None)
    attended = heads_to_tokens(att_heads)
    out_full = assemble(place, out_pieces).reshape(H * HD, width)
    resid = tokens + dot(attended, out_full, 0, 0)

    z, x, core = dp_place()
    half, quarter = width // 2, width // 4
    xhat_f, inv_f = unit_rms(resid)
    x_own = xhat_f.astype(BF)
    x_other = seq_swap(x_own)
    sizes = (dp_n, d_dp, ff_w)
    *wide, dx_own, out_own = ffn_core(x_own, g_own, ff_full, None, 0, *sizes)
    x_other, g_both, wide[0] = phase(x_other, g_other, wide[0])
    x_placed = dot(place_mat, jnp.concatenate([x_own, x_other], axis=0), 0, 1).astype(BF)
    g_all = jnp.concatenate([g_own, g_both], axis=0)
    x_placed, x_other, g_all = phase(x_placed, x_other, g_all)
    *wide, dx_other, out_other = ffn_core(x_other, g_other, ff_full, wide, 1, *sizes)
    hidden, d_gate, d_up = wide

    dx_send, d_gate = phase(dx_other, d_gate)
    dx_got = seq_swap(dx_send)
    g_far = mm(x_placed, d_gate, 1, 0, 2, 2, quarter, BF)
    g_far, d_up = phase(g_far, d_up)
    g_got = to_core(g_far)
    u_far = mm(x_placed, d_up, 1, 0, 2, 2, quarter, BF)
    u_far, g_got, d_gate = phase(u_far, g_got, d_gate)
    u_got = to_core(u_far)
    g_xs = mm(x_placed, d_gate, 1, 0, 1, 1, quarter, BF, g_got, 1)
    g_xs, d_up, u_got = phase(g_xs, d_up, u_got)
    g_xgot = to_x(g_xs)
    u_xs = mm(x_placed, d_up, 1, 0, 1, 1, quarter, BF, u_got, 1)
    u_xs, d_gate, d_up = phase(u_xs, d_gate, d_up)
    g_kept = mm(x_placed, d_gate, 1, 0, 0, 1, quarter, F32, g_got)
    u_kept = mm(x_placed, d_up, 1, 0, 0, 1, quarter, F32, u_got)
    u_xs, dx_got, g_xgot, g_kept, u_kept = phase(u_xs, dx_got, g_xgot, g_kept, u_kept)
    u_xgot = to_x(u_xs)

    d_resid, r_low = resid_back(dx_own, dx_got, cotangent, xhat_f, inv_f)
    d_att_all = dot(out_full, r_low, 1, 1).astype(BF)
    d_att_send = lax.dynamic_slice_in_dim(d_att_all, (1 - rank) * q_w, q_w, 0)
    g_own_part, g_zs = z_parts(g_kept, g_xgot)
    d_att_send, hidden, g_own_part, *g_zs = phase(d_att_send, hidden, g_own_part, *g_zs)
    d_att_got = seq_swap(d_att_send)
    g_zgot = z_send(g_zs)
    third = ff // 6
    d_far = mm(hidden, g_all, 0, 0, (1 - core) * 3, 3, third, BF, cost=LONG)
    d_far, attended = phase(d_far, attended)
    d_got = to_core(d_far)
    att_placed = dot(place_mat, attended, 0, 0).astype(BF)
    o_far = mm(att_placed, r_low, 1, 0, 2, 2, quarter, BF)
    o_far, d_got, hidden = phase(o_far, d_got, hidden)
    o_got = to_core(o_far)
    d_sum = mm(hidden, g_all, 0, 0, core * 3, 3, third, BF, d_got).reshape(2, ff // 4, width)
    d_xs = pick(d_sum, 1 - x, 0)
    d_att_mine = lax.dynamic_slice_in_dim(d_att_all, rank * q_w, q_w, 0)
    d_att = jnp.concatenate(
        [jnp.where(rank == 0, d_att_mine, d_att_got), jnp.where(rank == 0, d_att_got, d_att_mine)],
        axis=1,
    )
    d_xs, o_got, d_att = phase(d_xs, o_got, d_att)
    o_sum = mm(att_placed, r_low, 1, 0, 0, 2, quarter, F32, o_got)
    o_xs = o_sum[quarter:].astype(BF)
    o_xs, o_sum, u_xgot = phase(o_xs, o_sum, u_xgot)

    u_own_part, u_zs = z_parts(u_kept, u_xgot)
    vals = phase(d_att, o_xs, d_xs, out_other, *u_zs, *g_zgot)
    d_att, o_xs, d_xs, out_send = vals[:4]
    d_xgot = to_x(d_xs)
    u_zgot, g_zgot = z_send(vals[4:7]), vals[7:]
    out_got = seq_swap(out_send)
    lins = (lin, lin, gain_q[:, None], gain_k[:, None], cos_tab, sin_tab)
    d_q, d_k, d_v, d_gq, d_gk = attn_bwd(queries, keys, values, d_att, att_heads, lse, None, lins)
    vals = phase(d_q, d_k, d_v, d_gq, d_gk, d_xgot, out_got, o_xs, *u_zgot)
    d_q, d_k, d_v, d_gq, d_gk, d_xgot, out_got, o_xs = vals[:8]
    o_xgot = to_x(o_xs)
    u_zgot = vals[8:]

    d_lin = jnp.concatenate([d_q, d_k, d_v], axis=0)
    d_g = jnp.concatenate([d_gq.sum(axis=(0, 2)), d_gk.sum(axis=(0, 2))])

    def with_gains(arr, gains):
        high = gains.astype(BF)
        row = jnp.concatenate([high, (gains - high.astype(F32)).astype(BF)])[None]
        return jnp.concatenate([arr, jnp.pad(row, ((0, 7), (0, arr.shape[1] - row.shape[1])))], axis=0)

    def gains_of(arr):
        row = arr[-8].astype(F32)
        return row[: 2 * HD] + row[2 * HD : 4 * HD]

    d_norm_send = mm(d_lin, qkv_full, 0, 1, (1 - rank) * 2, 2, own // 2, BF)
    d_sum_kept = pick(d_sum, x, 0).astype(F32) + d_xgot.astype(F32)
    d_line = d_sum_kept.reshape(4, ff_w, width)
    d_own_part = pick(d_line, z, 0)
    d_zs = [pick(d_line, (z + s) % 4, 0).astype(BF) for s in (1, 2, 3)]
    d_norm_send, d_lin, d_own_part, *d_zs = phase(d_norm_send, d_lin, d_own_part, *d_zs)
    d_norm_got = seq_swap(d_norm_send)
    d_zgot = z_send(d_zs)
    x_far = with_gains(mm(low_placed, d_lin, 1, 1, 2, 2, quarter, BF), d_g)
    x_got = to_core(x_far)
    x_sum = mm(low_placed, d_lin, 1, 1, 0, 2, quarter, F32, x_got)
    d_g = d_g + gains_of(x_got)
    x_xs = with_gains(x_sum[quarter:].astype(BF), d_g)
    x_xs, o_xgot = phase(x_xs, o_xgot)
    x_xgot = to_x(x_xs)
    o_own_part, o_zs = z_parts(o_sum[:quarter], o_xgot)
    gu_end = jnp.concatenate([z_total(g_own_part, g_zgot), z_total(u_own_part, u_zgot)], axis=0)
    gu_end = gu_end.astype(BF)
    block_out = resid + out_own + out_got.astype(F32)
    vals = phase(o_own_part, *o_zs, *d_zgot)
    o_own_part, o_zgot, d_zgot = vals[0], z_send(vals[1:4]), vals[4:]
    d_norm_got, gu_end, x_xgot, block_out, *o_zgot = phase(
        d_norm_got, gu_end, x_xgot, block_out, *o_zgot
    )
    x_own_part, x_zs = z_parts(x_sum[:quarter], x_xgot[:quarter])
    d_g = d_g + gains_of(x_xgot)
    x_own_part, gu_end, *x_zs = phase(x_own_part, gu_end, *[with_gains(part, d_g) for part in x_zs])
    x_zgot = z_send(x_zs)
    gu_swap = seq_swap(gu_end)
    d_norm = mm(d_lin, qkv_full, 0, 1, rank * 2, 2, own // 2, F32, d_norm_got)
    d_tokens = d_resid + unit_rms_back(d_norm, xhat_a, inv_a)
    d_end = z_total(d_own_part, d_zgot).astype(BF)
    o_end = z_total(o_own_part, o_zgot).astype(BF)
    d_tokens, d_end, o_end, *x_zgot = phase(d_tokens, d_end, o_end, *x_zgot)
    for got_s in x_zgot:
        d_g = d_g + gains_of(got_s)
    x_end = z_total(x_own_part, [got_s[:d_dp] for got_s in x_zgot]).astype(BF)
    ends = jnp.concatenate([d_end, o_end, with_gains(x_end, d_g)], axis=0)
    ends, gu_swap = phase(ends, gu_swap)
    swaps = seq_swap(ends)
    d_w_g, dg_g = ff_finish(rank, gu_end[:d_dp], gu_swap[:d_dp], w_gate, gain_f, dp_n)
    d_w_u, dg_u = ff_finish(rank, gu_end[d_dp:], gu_swap[d_dp:], w_up, gain_f, dp_n)
    d_ffn_gain = (dg_g + dg_u)[:, 0]
    d_w_d = ordered(d_end, swaps[:ff_w], rank, 0).reshape(ff_dp, width).astype(F32)
    d_w_o = o_end.astype(F32) + swaps[ff_w : ff_w + d_dp].astype(F32)
    d_gains = d_g + gains_of(swaps)
    both = ordered(x_end, swaps[ff_w + d_dp : -8], rank, 0).astype(F32)
    join = lambda lo, n: both[:, :, lo : lo + n].transpose(1, 0, 2).reshape(d_dp, seq_n * n)
    d_w_q, d_w_k, d_w_v = join(0, q_w), join(q_w, kv_w), join(q_w + kv_w, kv_w)
    d_gq = lax.dynamic_slice_in_dim(d_gains, dp_rank * per, per)
    d_gk = lax.dynamic_slice_in_dim(d_gains, HD + dp_rank * per, per)
    d_attn_gain = jnp.sum(w_query.astype(F32) * d_w_q, axis=1) + jnp.sum(
        w_key.astype(F32) * d_w_k + w_value.astype(F32) * d_w_v, axis=1
    )
    return (
        block_out,
        d_tokens,
        d_attn_gain,
        d_w_q * gain_a,
        d_w_k * gain_a,
        d_w_v * gain_a,
        d_gq,
        d_gk,
        d_w_o,
        d_ffn_gain,
        d_w_g,
        d_w_u,
        d_w_d,
    )


def body_for(*args):
    tokens, lengths = args[:2]
    sizes = (lax.axis_size("dp"), lax.axis_size("seq"))
    exact = lengths.shape[1] == 1 and tokens.shape[0] * sizes[1] == MINLEN
    return (body_fast if sizes == (16, 2) and exact else body)(*args)


def solution(mesh):
    rows, shard, vec = P(("dp", "seq"), None), P("dp", None), P("dp")
    return jax.shard_map(
        body_for,
        mesh=mesh,
        in_specs=(
            rows, shard, vec, shard, shard, shard, vec, vec, shard, vec, shard, shard, shard, rows,
        ),
        out_specs=(
            rows, rows, vec, shard, shard, shard, vec, vec, shard, vec, shard, shard, shard,
        ),
        check_vma=False,
    )
```

```python
from functools import partial
import math

import jax
import jax.numpy as jnp
from jax import lax
from jax.experimental import pallas as pl
from jax.experimental.pallas import tpu as pltpu
from jax.sharding import PartitionSpec as P

H = 16
KV = 8
HD = 64
GROUP = H // KV
MINLEN = 1024

EPSILON = 1e-05
ROPE_BASE = 1000000.0
MASKED_SCORE = -1e30
BF = jnp.bfloat16
F32 = jnp.float32


LONG = pl.CostEstimate(flops=40 << 30, transcendentals=0, bytes_accessed=96 << 20)
SHORT = pl.CostEstimate(flops=1 << 20, transcendentals=0, bytes_accessed=1 << 14)


def dot(left, right, lc, rc):
    return lax.dot_general(left, right, (((lc,), (rc,)), ((), ())), preferred_element_type=F32)


def masked(scores, q0, k0, segs):
    row = lax.broadcasted_iota(jnp.int32, scores.shape, 0) + k0
    col = lax.broadcasted_iota(jnp.int32, scores.shape, 1) + q0
    allowed = row <= col
    if segs is not None:
        allowed = allowed & (segs[0] == segs[1])
    return jnp.where(allowed, scores, MASKED_SCORE)


def attn_fwd_kernel(blk, static, *refs):
    if static:
        q_ref, k_ref, v_ref, o_ref, lse_ref = refs
    else:
        q_ref, k_ref, v_ref, sc_ref, sr_ref, o_ref, lse_ref = refs
    length = q_ref.shape[1]
    keys = k_ref[...].T

    def finish(q0, parts):
        top = parts[0][0].max(axis=0, keepdims=True)
        for s, _ in parts[1:]:
            top = jnp.maximum(top, s.max(axis=0, keepdims=True))
        total, out = 0.0, 0.0
        for s, v in parts:
            p = jnp.exp(s - top)
            total = total + p.sum(axis=0, keepdims=True)
            out = out + dot(v, p.astype(BF), 1, 0)
        o_ref[:, pl.ds(q0, blk)] = (out / total).astype(BF)
        lse_ref[0, :, pl.ds(q0, blk)] = top + jnp.log(total)

    if static:
        for qb in range(length // blk):
            q0 = qb * blk
            q = q_ref[:, q0 : q0 + blk]
            parts = []
            if qb:
                parts.append((dot(keys[:q0], q, 1, 0), v_ref[:, :q0]))
            diag = masked(dot(keys[q0 : q0 + blk], q, 1, 0), 0, 0, None)
            parts.append((diag, v_ref[:, q0 : q0 + blk]))
            finish(q0, parts)
    else:

        @pl.loop(0, length // blk)
        def _(qb):
            q0 = pl.multiple_of(qb * blk, blk)
            s = dot(keys, q_ref[:, pl.ds(q0, blk)], 1, 0)
            s = masked(s, q0, 0, (sc_ref[...], sr_ref[:, pl.ds(q0, blk)]))
            finish(q0, [(s, v_ref[...])])


def lin_back(y, lin, gain, cos_tab, sin_tab):
    first, second = y[: HD // 2], y[HD // 2 :]
    y = jnp.concatenate(
        [first * cos_tab + second * sin_tab, second * cos_tab - first * sin_tab], axis=0
    )
    inv = lax.rsqrt(jnp.mean(lin * lin, axis=0, keepdims=True) + EPSILON)
    xhat = lin * inv
    d_gain = jnp.sum(y * xhat, axis=1, keepdims=True)
    y = y * gain
    return inv * (y - xhat * jnp.mean(y * xhat, axis=0, keepdims=True)), d_gain


def attn_bwd_kernel(blk, static, *refs):
    lin_refs = None
    if static:
        q_ref, k_ref, v_ref, do_ref, o_ref, lse_ref = refs[:6]
        lin_refs = refs[6:12]
        dq_ref, dk_ref, dv_ref, dgq_ref, dgk_ref, dk_acc, dv_acc = refs[12:]
        ql_ref, kl_ref, gq_ref, gk_ref, cos_ref, sin_ref = lin_refs
    else:
        (q_ref, k_ref, v_ref, do_ref, o_ref, lse_ref, sc_ref, sr_ref,
         dq_ref, dk_ref, dv_ref, dk_acc, dv_acc) = refs
    length = q_ref.shape[1]
    member = lax.rem(pl.program_id(0), GROUP)
    keys = k_ref[...].T
    values = v_ref[...].T

    @pl.when(member == 0)
    def _():
        dk_acc[...] = jnp.zeros_like(dk_acc)
        dv_acc[...] = jnp.zeros_like(dv_acc)

    def part(q, d_out, lse, delta, k_lo, k_n, q0, segs, mask):
        rows = pl.ds(k_lo, k_n)
        k_blk, v_blk = keys[k_lo : k_lo + k_n], values[k_lo : k_lo + k_n]
        s = dot(k_blk, q, 1, 0)
        if mask:
            s = masked(s, q0, k_lo, segs)
        p = jnp.exp(s - lse)
        dv_acc[rows, :] += dot(p.astype(BF), d_out, 1, 1)
        dp = dot(v_blk, d_out, 1, 0)
        ds = (p * (dp - delta)).astype(BF)
        dk_acc[rows, :] += dot(ds, q, 1, 1)
        return dot(k_ref[:, rows], ds, 1, 0)

    def prepare(q0):
        cols = pl.ds(q0, blk)
        d_out = do_ref[:, cols]
        delta = (d_out.astype(F32) * o_ref[:, cols].astype(F32)).sum(axis=0, keepdims=True)
        return cols, q_ref[:, cols], d_out, lse_ref[0, :, cols], delta

    scale = 1.0 / math.sqrt(HD)
    if static:
        for qb in range(length // blk):
            q0 = qb * blk
            cols, q, d_out, lse, delta = prepare(q0)
            dq = part(q, d_out, lse, delta, q0, blk, q0, None, True)
            if qb:
                dq = dq + part(q, d_out, lse, delta, 0, q0, q0, None, False)
            d_lin, d_gain = lin_back(
                dq * scale, ql_ref[:, cols], gq_ref[...], cos_ref[:, cols], sin_ref[:, cols]
            )
            dq_ref[:, cols] = d_lin.astype(BF)
            dgq_ref[0] = d_gain if qb == 0 else dgq_ref[0] + d_gain
    else:

        @pl.loop(0, length // blk)
        def _(qb):
            q0 = pl.multiple_of(qb * blk, blk)
            cols, q, d_out, lse, delta = prepare(q0)
            dq = part(q, d_out, lse, delta, 0, length, q0, (sc_ref[...], sr_ref[:, cols]), True)
            dq_ref[:, cols] = (dq * scale).astype(BF)

    @pl.when(member == GROUP - 1)
    def _():
        dk = dk_acc[...].T
        if static:
            dk, d_gain = lin_back(dk, kl_ref[...], gk_ref[...], cos_ref[...], sin_ref[...])
            dgk_ref[0] = d_gain
        dk_ref[...] = dk.astype(BF)
        dv_ref[...] = dv_acc[...].T.astype(BF)


def attn_specs(length):
    q_spec = pl.BlockSpec((HD, length), lambda h: (h, 0))
    kv_spec = pl.BlockSpec((HD, length), lambda h: (h // GROUP, 0))
    lse_spec = pl.BlockSpec((1, 1, length), lambda h: (h, 0, 0))
    seg_specs = [
        pl.BlockSpec((length, 1), lambda h: (0, 0)),
        pl.BlockSpec((1, length), lambda h: (0, 0)),
    ]
    return q_spec, kv_spec, lse_spec, seg_specs


def attn_fwd(q, k, v, segs):
    rows, length = q.shape
    heads = rows // HD
    static = segs is None
    q_spec, kv_spec, lse_spec, seg_specs = attn_specs(length)
    extra = () if static else (segs[:, None], segs[None, :])
    return pl.pallas_call(
        partial(attn_fwd_kernel, min(256, length), static),
        grid=(heads,),
        in_specs=[q_spec, kv_spec, kv_spec] + ([] if static else seg_specs),
        out_specs=[q_spec, lse_spec],
        out_shape=[
            jax.ShapeDtypeStruct((rows, length), BF),
            jax.ShapeDtypeStruct((heads, 1, length), F32),
        ],
        cost_estimate=SHORT,
        name="attn_fwd",
    )(q, k, v, *extra)


def attn_bwd(q, k, v, d_out, out, lse, segs, lins=()):
    rows, length = q.shape
    heads = rows // HD
    static = segs is None
    q_spec, kv_spec, lse_spec, seg_specs = attn_specs(length)
    extra = tuple(lins) if static else (segs[:, None], segs[None, :])
    whole = lambda arr: pl.BlockSpec(arr.shape, lambda h: (0, 0))
    lin_specs = [q_spec, pl.BlockSpec((HD, length), lambda h: (heads + h // GROUP, 0))]
    lin_specs += [whole(arr) for arr in lins[2:]]
    gain_specs = [
        pl.BlockSpec((1, HD, 1), lambda h: (h, 0, 0)),
        pl.BlockSpec((1, HD, 1), lambda h: (h // GROUP, 0, 0)),
    ]
    gain_shapes = [
        jax.ShapeDtypeStruct((heads, HD, 1), F32),
        jax.ShapeDtypeStruct((heads // GROUP, HD, 1), F32),
    ]
    return pl.pallas_call(
        partial(attn_bwd_kernel, min(256, length), static),
        grid=(heads,),
        in_specs=[q_spec, kv_spec, kv_spec, q_spec, q_spec, lse_spec]
        + (lin_specs if static else seg_specs),
        out_specs=[q_spec, kv_spec, kv_spec] + (gain_specs if static else []),
        out_shape=[
            jax.ShapeDtypeStruct((rows, length), BF),
            jax.ShapeDtypeStruct(k.shape, BF),
            jax.ShapeDtypeStruct(v.shape, BF),
        ]
        + (gain_shapes if static else []),
        scratch_shapes=[pltpu.VMEM((length, HD), F32), pltpu.VMEM((length, HD), F32)],
        cost_estimate=LONG,
        name="attn_bwd",
    )(q, k, v, d_out, out, lse, *extra)


def ff_prep_kernel(rank_ref, gate_ref, up_ref, down_ref, gain_ref, out_ref):
    first = rank_ref[0] == 0
    d_dp, ff_all = gate_ref.shape
    ff_w = down_ref.shape[0] // 2
    dp_n = ff_all // (2 * ff_w)
    gain = gain_ref[...]
    for half, ref in enumerate((gate_ref, up_ref)):
        for i in range(dp_n):
            lo = ref[:, 2 * i * ff_w : (2 * i + 1) * ff_w].astype(F32)
            hi = ref[:, (2 * i + 1) * ff_w : (2 * i + 2) * ff_w].astype(F32)
            at = (half * dp_n + hidden_place(i)) * ff_w
            out_ref[:d_dp, at : at + ff_w] = (jnp.where(first, lo, hi) * gain).astype(BF)
    for b in range(ff_w // 16):
        lo = down_ref[16 * b : 16 * b + 16, :]
        hi = down_ref[ff_w + 16 * b : ff_w + 16 * b + 16, :]
        rows = jnp.where(first, lo.astype(F32), hi.astype(F32)).astype(BF)
        for band, at, frm, to in down_places(b, rows.shape[1], ff_all):
            out_ref[d_dp + 16 * band : d_dp + 16 * band + 16, at : at + to - frm] = rows[:, frm:to]


def hidden_place(i):
    return (i % 2 * 2 + i // 2 % 2) * 4 + i // 4


def down_places(b, width, ff_all):
    places, start = [], b * width
    while start < (b + 1) * width:
        band = start // ff_all
        end = min((band + 1) * ff_all, (b + 1) * width)
        places.append((band, start - band * ff_all, start - b * width, end - b * width))
        start = end
    return places


def ff_prep(rank, w_gate, w_up, w_down, gain):
    d_dp, ff_all = w_gate.shape
    bands = w_down.shape[0] // 2 * w_down.shape[1] // ff_all
    whole = lambda arr: pl.BlockSpec(arr.shape, lambda i, r: (0, 0))
    return pl.pallas_call(
        ff_prep_kernel,
        grid_spec=pltpu.PrefetchScalarGridSpec(
            num_scalar_prefetch=1,
            grid=(1,),
            in_specs=[whole(w_gate), whole(w_up), whole(w_down), whole(gain)],
            out_specs=pl.BlockSpec((d_dp + bands, ff_all), lambda i, r: (0, 0)),
        ),
        out_shape=jax.ShapeDtypeStruct((d_dp + bands, ff_all), BF),
        name="ff_prep",
    )(rank[None], w_gate, w_up, w_down, gain)


def ffn_core_kernel(sub, fresh, *refs):
    x_ref, g_ref, wg_ref, wu_ref, wd_ref = refs[:5]
    hid_ref, dg_ref, du_ref, dx_out, out_out, down, dx_ref, out_ref = refs[5:] if fresh else refs[8:]
    dp_n, d_dp, blk = wg_ref.shape
    width = g_ref.shape[1]
    ff_all = wd_ref.shape[2]
    ff_w = down.shape[0] // dp_n
    step = pl.program_id(0)

    @pl.when(step == 0)
    def _():
        dx_ref[...] = jnp.zeros_like(dx_ref)
        out_ref[...] = jnp.zeros_like(out_ref)

        @pl.loop(0, dp_n)
        def _(i):
            for b in range(ff_w // 16):
                at_i = (lax.rem(i, 2) * 2 + lax.rem(lax.div(i, 2), 2)) * 4 + lax.div(i, 4)
                rows = pl.ds(pl.multiple_of(at_i * ff_w + 16 * b, 16), 16)
                for band, at, frm, to in down_places(b, width, ff_all):
                    down[rows, frm:to] = wd_ref[i, 16 * band : 16 * band + 16, at : at + to - frm]

    @pl.loop(0, blk // sub)
    def _(s):
        cols = pl.ds(pl.multiple_of(s * sub, 128), sub)
        rows = pl.ds(pl.multiple_of(step * blk + s * sub, 128), sub)
        x = x_ref[...]
        w_gate = wg_ref[:, :, cols].reshape(dp_n * d_dp, sub)
        w_up = wu_ref[:, :, cols].reshape(dp_n * d_dp, sub)
        w_down = down[rows, :]
        gate = dot(x, w_gate, 1, 0)
        up = dot(x, w_up, 1, 0)
        d_hid = dot(g_ref[...], w_down, 1, 1)
        sig = 1.0 / (1.0 + jnp.exp(-gate))
        silu = gate * sig
        hidden = (silu * up).astype(BF)
        d_gate = (d_hid * up * (sig * (1.0 + gate * (1.0 - sig)))).astype(BF)
        d_up = (d_hid * silu).astype(BF)
        hid_ref[:, cols] = hidden
        dg_ref[:, cols] = d_gate
        du_ref[:, cols] = d_up
        dx_ref[...] += dot(d_gate, w_gate, 1, 1) + dot(d_up, w_up, 1, 1)
        out_ref[...] += dot(hidden, w_down, 1, 0)

    @pl.when(step == pl.num_programs(0) - 1)
    def _():
        dx_out[...] = dx_ref[...].astype(dx_out.dtype)
        out_out[...] = out_ref[...].astype(out_out.dtype)


def ffn_core(x, g, packed, earlier, half, dp_n, d_dp, ff_w):
    rows, width = x.shape
    ff = dp_n * ff_w
    blk = ff // 2
    fresh = earlier is None
    whole = pl.BlockSpec((rows, width), lambda j: (0, 0))
    wide = pl.BlockSpec((rows, blk), lambda j: (half, j))
    bands = packed.shape[1] - d_dp
    keep = pl.BlockSpec(memory_space=pl.ANY)
    wide_shape = jax.ShapeDtypeStruct((2 * rows, ff), BF)
    return pl.pallas_call(
        partial(ffn_core_kernel, 384, fresh),
        grid=(2,),
        in_specs=[
            whole,
            whole,
            pl.BlockSpec((dp_n, d_dp, blk), lambda j: (0, 0, j)),
            pl.BlockSpec((dp_n, d_dp, blk), lambda j: (0, 0, 2 + j)),
            pl.BlockSpec(
                (dp_n, bands, 2 * ff), lambda j: (0, d_dp // bands, 0), pipeline_mode=pl.Buffered(1)
            ),
        ]
        + ([] if fresh else [keep] * 3),
        out_specs=[wide, wide, wide, whole, whole],
        out_shape=[wide_shape] * 3
        + [jax.ShapeDtypeStruct((rows, width), F32 if fresh else BF)] * 2,
        scratch_shapes=[pltpu.VMEM((ff, width), BF)] + [pltpu.VMEM((rows, width), F32)] * 2,
        input_output_aliases={} if fresh else {5: 0, 6: 1, 7: 2},
        compiler_params=pltpu.CompilerParams(vmem_limit_bytes=60 << 20),
        cost_estimate=SHORT,
        name="ffn_core",
    )(x, g, packed, packed, packed, *(() if fresh else earlier))


def mm_kernel(lc, rc, first_ref, a_ref, b_ref, *refs):
    total = dot(a_ref[...], b_ref[...], lc, rc)
    if len(refs) == 2:
        total = total + refs[0][...].astype(F32)
    refs[-1][...] = total.astype(refs[-1].dtype)


def mm(a, b, lc, rc, first, count, rows, dtype, add=None, add_first=0, cost=SHORT):
    cols = b.shape[1 - rc]
    a_spec = (
        pl.BlockSpec((rows, a.shape[1]), lambda i, f: (f[0] + i, 0))
        if lc
        else pl.BlockSpec((a.shape[0], rows), lambda i, f: (0, f[0] + i))
    )
    in_specs = [a_spec, pl.BlockSpec(b.shape, lambda i, f: (0, 0))]
    args = [a, b]
    if add is not None:
        in_specs.append(pl.BlockSpec((rows, cols), lambda i, f: (add_first + i, 0)))
        args.append(add)
    return pl.pallas_call(
        partial(mm_kernel, lc, rc),
        grid_spec=pltpu.PrefetchScalarGridSpec(
            num_scalar_prefetch=1,
            grid=(count,),
            in_specs=in_specs,
            out_specs=pl.BlockSpec((rows, cols), lambda i, f: (i, 0)),
        ),
        out_shape=jax.ShapeDtypeStruct((count * rows, cols), dtype),
        compiler_params=pltpu.CompilerParams(vmem_limit_bytes=48 << 20),
        cost_estimate=cost,
        name="mm",
    )(jnp.asarray(first, jnp.int32)[None], *args)


def resid_back_kernel(dx_ref, got_ref, cot_ref, xhat_ref, inv_ref, out_ref, low_ref):
    y = dx_ref[...] + got_ref[...].astype(F32)
    d_resid = cot_ref[...] + unit_rms_back(y, xhat_ref[...], inv_ref[...])
    out_ref[...] = d_resid
    low_ref[...] = d_resid.astype(BF)


def resid_back(dx_own, dx_got, cotangent, xhat, inv):
    rows, width = dx_own.shape
    wide = pl.BlockSpec((rows // 4, width), lambda i: (i, 0))
    return pl.pallas_call(
        resid_back_kernel,
        grid=(4,),
        in_specs=[wide, wide, wide, wide, pl.BlockSpec((rows // 4, 1), lambda i: (i, 0))],
        out_specs=[wide, wide],
        out_shape=[
            jax.ShapeDtypeStruct((rows, width), F32),
            jax.ShapeDtypeStruct((rows, width), BF),
        ],
        cost_estimate=LONG,
        name="resid_back",
    )(dx_own, dx_got, cotangent, xhat, inv)


def ff_finish_kernel(rank_ref, mine_ref, theirs_ref, w_ref, gain_ref, out_ref, d_gain_ref):
    first = rank_ref[0] == 0
    mine, theirs = mine_ref[...].astype(F32), theirs_ref[...].astype(F32)
    low_ = jnp.where(first, mine, theirs)
    high = jnp.where(first, theirs, mine)
    gain = gain_ref[...]
    dp_n = gain_ref.shape[1]
    n = mine.shape[1] // dp_n
    total = jnp.zeros((mine.shape[0], 2 * n), F32)
    for i in range(dp_n):
        cols = slice(2 * i * n, 2 * (i + 1) * n)
        at = hidden_place(i) * n
        pair = jnp.concatenate([low_[:, at : at + n], high[:, at : at + n]], axis=1)
        total = total + pair * w_ref[:, cols].astype(F32)
        out_ref[:, cols] = pair * gain[:, :1]
    d_gain_ref[...] = total.sum(axis=1, keepdims=True)


def ff_finish(rank, mine, theirs, weight, gain, dp_n):
    gain = jnp.broadcast_to(gain, (gain.shape[0], dp_n))
    whole = lambda arr: pl.BlockSpec(arr.shape, lambda i, r: (0, 0))
    return pl.pallas_call(
        ff_finish_kernel,
        grid_spec=pltpu.PrefetchScalarGridSpec(
            num_scalar_prefetch=1,
            grid=(1,),
            in_specs=[whole(mine), whole(theirs), whole(weight), whole(gain)],
            out_specs=[
                pl.BlockSpec(weight.shape, lambda i, r: (0, 0)),
                pl.BlockSpec((weight.shape[0], 1), lambda i, r: (0, 0)),
            ],
        ),
        out_shape=[
            jax.ShapeDtypeStruct(weight.shape, F32),
            jax.ShapeDtypeStruct((weight.shape[0], 1), F32),
        ],
        name="ff_finish",
    )(rank[None], mine, theirs, weight, gain)


def assemble_kernel(place_ref, *refs):
    out_ref = refs[-1]
    rows = refs[0].shape[0]
    z, x, core = place_ref[0], place_ref[1], place_ref[2]
    for n, ref in enumerate(refs[:-1]):
        b, a, s = n // 8, n // 4 % 2, n % 4
        at = (lax.rem(z + s, 4) * 2 + (a + x - 2 * a * x)) * 2 + (b + core - 2 * b * core)
        out_ref[at] = ref[...]


def assemble(place, pieces):
    shape = pieces[0].shape
    return pl.pallas_call(
        assemble_kernel,
        grid_spec=pltpu.PrefetchScalarGridSpec(
            num_scalar_prefetch=1,
            grid=(1,),
            in_specs=[pl.BlockSpec(shape, lambda i, p: (0, 0))] * 16,
            out_specs=pl.BlockSpec((16,) + shape, lambda i, p: (0, 0, 0)),
        ),
        out_shape=jax.ShapeDtypeStruct((16,) + shape, BF),
        name="assemble",
    )(place, *pieces)


def pick(arr, index, axis):
    return lax.dynamic_index_in_dim(arr, index, axis, keepdims=False)


def ordered(mine, other, rank, axis):
    low_ = jnp.where(rank == 0, mine, other)
    high = jnp.where(rank == 0, other, mine)
    return jnp.stack([low_, high], axis=axis)


def dp_gather(shard):
    return lax.all_gather(shard, "dp", axis=0, tiled=False)


def dp_scatter(parts):
    flat = parts.reshape((-1,) + parts.shape[2:])
    return lax.psum_scatter(flat, "dp", scatter_dimension=0, tiled=True).astype(F32)


def dp_place():
    index = lax.axis_index("dp")
    return index // 4, (index // 2) % 2, index % 2


def to_core(arr):
    return lax.ppermute(arr, "dp", [(j, j ^ 1) for j in range(16)])


def to_x(arr):
    return lax.ppermute(arr, "dp", [(j, j ^ 2) for j in range(16)])


def to_z(arr, s):
    return lax.ppermute(arr, "dp", [(j, (j + 4 * s) % 16) for j in range(16)])


def gather_z(shard):
    return [shard] + [to_z(shard, 4 - s) for s in (1, 2, 3)]


def gather_rest(line):
    plane = line + [to_x(piece) for piece in line]
    return plane + [to_core(piece) for piece in plane]


def place_matrix(width):
    z, x, core = dp_place()
    n = jnp.arange(width, dtype=jnp.int32)
    part = width // 16
    block = (
        (z + n // part % 4) % 4 * 4
        + jnp.bitwise_xor(x, n // (4 * part) % 2) * 2
        + jnp.bitwise_xor(core, n // (8 * part))
    )
    source = block * part + n % part
    return (n[:, None] == source[None, :]).astype(BF)


def phase(*values):
    return lax.optimization_barrier(values)


def z_parts(kept, got):
    r = kept.shape[0] // 4
    sums = [kept[s * r : s * r + r] + got[s * r : s * r + r].astype(F32) for s in range(4)]
    return sums[0], [part.astype(BF) for part in sums[1:]]


def z_send(parts):
    return [to_z(part, s + 1) for s, part in enumerate(parts)]


def z_total(kept, got):
    total = kept
    for term in got:
        total = total + term.astype(F32)
    return total


def after(value, *others):
    return lax.optimization_barrier((value,) + tuple(others))[0]


def seq_swap(arr):
    return lax.ppermute(arr, "seq", [(0, 1), (1, 0)])


def seq_tokens(rows):
    if lax.axis_size("seq") == 2:
        return jnp.concatenate([rows, seq_swap(rows)], axis=0)
    return lax.all_gather(rows, "seq", axis=0, tiled=True)


def seq_tokens_sum(parts):
    if lax.axis_size("seq") == 2:
        own = parts.shape[0] // 2
        return parts[:own] + seq_swap(parts[own:].astype(BF)).astype(F32)
    return lax.psum_scatter(parts.astype(BF), "seq", scatter_dimension=0, tiled=True).astype(F32)


def seq_stack(arr):
    if lax.axis_size("seq") == 2:
        return ordered(arr, seq_swap(arr), lax.axis_index("seq"), 0)
    return lax.all_gather(arr, "seq", axis=0, tiled=False)


def heads_to_tokens(arr):
    count = lax.axis_size("seq")
    rows, length = arr.shape
    if count == 2:
        rank = lax.axis_index("seq")
        own = length // 2
        mine = lax.dynamic_slice_in_dim(arr, rank * own, own, 1)
        theirs = seq_swap(lax.dynamic_slice_in_dim(arr, (1 - rank) * own, own, 1))
        return ordered(mine, theirs, rank, 0).reshape(2 * rows, own)
    return lax.all_to_all(arr, "seq", split_axis=1, concat_axis=0, tiled=True)


def tokens_to_heads(arr):
    count = lax.axis_size("seq")
    rows, own = arr.shape
    if count == 2:
        rank = lax.axis_index("seq")
        half = rows // 2
        mine = lax.dynamic_slice_in_dim(arr, rank * half, half, 0)
        theirs = seq_swap(lax.dynamic_slice_in_dim(arr, (1 - rank) * half, half, 0))
        first = jnp.where(rank == 0, mine, theirs)
        second = jnp.where(rank == 0, theirs, mine)
        return jnp.concatenate([first, second], axis=1)
    return lax.all_to_all(arr, "seq", split_axis=0, concat_axis=1, tiled=True)


def pack_layout(seq_lens, total):
    places = jnp.arange(total, dtype=jnp.int32)
    ends = jnp.cumsum(seq_lens)
    starts = ends - seq_lens
    segment = jnp.sum((places[:, None] >= ends[None, :]).astype(jnp.int32), axis=1)
    starts_ext = jnp.concatenate([starts, ends[-1:]])
    labels = jnp.arange(seq_lens.shape[0] + 1, dtype=jnp.int32)
    offset = jnp.sum(jnp.where(segment[:, None] == labels[None, :], starts_ext[None, :], 0), axis=1)
    return segment, places - offset, segment < seq_lens.shape[0]


def unit_rms(values):
    inv = lax.rsqrt(jnp.mean(values * values, axis=-1, keepdims=True) + EPSILON)
    return values * inv, inv


def unit_rms_back(y, xhat, inv):
    return inv * (y - xhat * jnp.mean(y * xhat, axis=-1, keepdims=True))


def head_prep(lin, gain, cos_tab, sin_tab, scale):
    u = lin.reshape(-1, HD, lin.shape[1])
    inv = lax.rsqrt(jnp.mean(u * u, axis=1, keepdims=True) + EPSILON)
    u = u * inv * gain[None, :, None]
    first, second = u[:, : HD // 2], u[:, HD // 2 :]
    out = jnp.concatenate(
        [first * cos_tab - second * sin_tab, second * cos_tab + first * sin_tab], axis=1
    )
    return (out * scale).astype(BF).reshape(lin.shape)


def head_prep_back(grad, lin, gain, cos_tab, sin_tab):
    y = grad.astype(F32).reshape(-1, HD, lin.shape[1])
    first, second = y[:, : HD // 2], y[:, HD // 2 :]
    y = jnp.concatenate(
        [first * cos_tab + second * sin_tab, second * cos_tab - first * sin_tab], axis=1
    )
    u = lin.reshape(y.shape)
    inv = lax.rsqrt(jnp.mean(u * u, axis=1, keepdims=True) + EPSILON)
    xhat = u * inv
    d_gain = jnp.sum(y * xhat, axis=(0, 2))
    y = y * gain[None, :, None]
    d_lin = inv * (y - xhat * jnp.mean(y * xhat, axis=1, keepdims=True))
    return d_lin.astype(BF).reshape(lin.shape), d_gain


def body(
    tokens, lengths, attn_gain, w_query, w_key, w_value, query_gain, key_gain, w_out,
    ffn_gain, w_gate, w_up, w_down, cotangent,
):
    seq_n = lax.axis_size("seq")
    dp_n = lax.axis_size("dp")
    rank = lax.axis_index("seq")
    dp_rank = lax.axis_index("dp")
    own, width = tokens.shape
    length = own * seq_n
    q_w, kv_w = H * HD // seq_n, KV * HD // seq_n
    ff_dp = w_down.shape[0]
    ff_w = ff_dp // seq_n
    ff = ff_w * dp_n
    d_dp = w_query.shape[0]

    full = length == MINLEN * lengths.shape[1]
    segment, positions, valid = pack_layout(lengths[0], length)
    segs = None if full and lengths.shape[1] == 1 else segment
    my_valid = lax.dynamic_slice_in_dim(valid, rank * own, own).astype(F32)[:, None]

    def keep_valid(arr):
        return arr if full else arr * my_valid

    gain_a = attn_gain.astype(F32)[:, None]
    gain_f = ffn_gain.astype(F32)[:, None]

    def my_cols(w, n):
        return lax.dynamic_slice_in_dim(w, rank * n, n, 1)

    qkv_part = jnp.concatenate(
        [my_cols(w_query, q_w), my_cols(w_key, kv_w), my_cols(w_value, kv_w)], axis=1
    )
    qkv_part = (qkv_part.astype(F32) * gain_a).astype(BF)
    gains = jnp.concatenate([query_gain, key_gain])
    gains = jnp.pad(gains[None, :], ((0, 7), (0, qkv_part.shape[1] - gains.shape[0])))
    pick_ff = lambda w: pick(w.reshape(d_dp, dp_n, seq_n, ff_w), rank, 2).reshape(d_dp, ff)
    gu_part = jnp.concatenate([pick_ff(w_gate), pick_ff(w_up)], axis=1)
    gu_part = (gu_part.astype(F32) * gain_f).astype(BF)
    down_part = pick(w_down.reshape(seq_n, ff_w, width), rank, 0)

    gu_full = lax.all_gather(gu_part, "dp", axis=0, tiled=True)
    down_full = lax.all_gather(down_part, "dp", axis=0, tiled=True)
    got = dp_gather(jnp.concatenate([qkv_part, gains], axis=0))
    qkv_full = got[:, :d_dp].reshape(width, -1)
    per = query_gain.shape[0]
    gain_q = got[:, d_dp, :per].reshape(-1).astype(F32)
    gain_k = got[:, d_dp, per : 2 * per].reshape(-1).astype(F32)
    out_full = dp_gather(w_out).reshape(H * HD, width)

    xhat_a, inv_a = unit_rms(tokens)
    low_own = xhat_a.astype(BF)
    if seq_n == 2:
        low_a = ordered(low_own, seq_swap(low_own), rank, 0).reshape(length, width)
    else:
        low_a = lax.all_gather(low_own, "seq", axis=0, tiled=True)
    lin = dot(qkv_full, low_a, 0, 1)
    q_lin, k_lin = lin[:q_w], lin[q_w : q_w + kv_w]
    values = lin[q_w + kv_w :].astype(BF)
    freqs = ROPE_BASE ** (-(jnp.arange(HD // 2, dtype=F32) * (2.0 / HD)))
    angles = freqs[:, None] * positions.astype(F32)[None, :]
    cos_tab, sin_tab = jnp.cos(angles), jnp.sin(angles)
    queries = head_prep(q_lin, gain_q, cos_tab, sin_tab, 1.0 / math.sqrt(HD))
    keys = head_prep(k_lin, gain_k, cos_tab, sin_tab, 1.0)
    att_heads, lse = attn_fwd(queries, keys, values, segs)
    attended = heads_to_tokens(att_heads)
    resid = tokens + dot(attended, out_full, 0, 0)

    xhat_f, inv_f = unit_rms(resid)
    grad = keep_valid(cotangent)
    x_all = seq_tokens(xhat_f.astype(BF))
    g_all = seq_tokens(grad.astype(BF))
    gate = dot(x_all, gu_full[:, :ff], 1, 0)
    up = dot(x_all, gu_full[:, ff:], 1, 0)
    d_hidden = dot(g_all, down_full, 1, 1)
    sig = jax.nn.sigmoid(gate)
    silu = gate * sig
    hidden = (silu * up).astype(BF)
    d_gate = (d_hidden * up * sig * (1.0 + gate * (1.0 - sig))).astype(BF)
    d_up = (d_hidden * silu).astype(BF)
    d_ffn = dot(d_gate, gu_full[:, :ff], 1, 1) + dot(d_up, gu_full[:, ff:], 1, 1)
    d_ffn = seq_tokens_sum(d_ffn)
    d_resid = grad + unit_rms_back(d_ffn, xhat_f, inv_f)

    block_out = keep_valid(resid + seq_tokens_sum(dot(hidden, down_full, 1, 0)))
    d_w_g = dp_scatter(dot(x_all, d_gate, 0, 0).astype(BF).reshape(dp_n, d_dp, ff))
    d_w_u = dp_scatter(dot(x_all, d_up, 0, 0).astype(BF).reshape(dp_n, d_dp, ff))
    d_w_d = dp_scatter(dot(hidden, g_all, 0, 0).astype(BF).reshape(dp_n, ff_w, width))

    def full_ff(shard):
        both = seq_stack(shard.astype(BF)).reshape(seq_n, d_dp, dp_n, ff_w)
        return both.transpose(1, 2, 0, 3).reshape(d_dp, dp_n * seq_n * ff_w).astype(F32)

    d_w_g, d_w_u = full_ff(d_w_g), full_ff(d_w_u)
    d_w_d = seq_stack(d_w_d.astype(BF)).reshape(ff_dp, width).astype(F32)
    d_ffn_gain = jnp.sum(w_gate.astype(F32) * d_w_g + w_up.astype(F32) * d_w_u, axis=1)

    r_low = d_resid.astype(BF)
    d_att = tokens_to_heads(dot(out_full, r_low, 1, 1).astype(BF))
    d_w_o = dp_scatter(dot(attended, r_low, 1, 0).astype(BF).reshape(dp_n, d_dp, width))
    if segs is None:
        lins = (lin, lin, gain_q[:, None], gain_k[:, None], cos_tab, sin_tab)
        d_q, d_k, d_v, d_gq, d_gk = attn_bwd(queries, keys, values, d_att, att_heads, lse, None, lins)
        d_gq, d_gk = d_gq.sum(axis=(0, 2)), d_gk.sum(axis=(0, 2))
    else:
        d_q, d_k, d_v = attn_bwd(queries, keys, values, d_att, att_heads, lse, segs)
        d_q, d_gq = head_prep_back(d_q, q_lin, gain_q, cos_tab, sin_tab)
        d_k, d_gk = head_prep_back(d_k, k_lin, gain_k, cos_tab, sin_tab)
    d_lin = jnp.concatenate([d_q, d_k, d_v], axis=0)
    d_norm = dot(d_lin, qkv_full, 0, 1)
    if seq_n == 2:
        other = lax.dynamic_slice_in_dim(d_norm, (1 - rank) * own, own, 0)
        d_norm = lax.dynamic_slice_in_dim(d_norm, rank * own, own, 0)
        d_norm = d_norm + seq_swap(other.astype(BF)).astype(F32)
    else:
        d_norm = seq_tokens_sum(d_norm)
    d_tokens = d_resid + unit_rms_back(d_norm, xhat_a, inv_a)

    d_w_x = dot(low_a, d_lin, 0, 1).astype(BF).reshape(dp_n, d_dp, -1)
    d_g = jnp.concatenate([d_gq, d_gk]).astype(BF)
    d_g = jnp.pad(d_g[None, :], ((0, 7), (0, d_w_x.shape[2] - d_g.shape[0])))
    d_g = jnp.broadcast_to(d_g[None], (dp_n,) + d_g.shape)
    d_w_x = dp_scatter(jnp.concatenate([d_w_x, d_g], axis=1))
    d_w_x = seq_stack(d_w_x.astype(BF)).astype(F32)
    both = d_w_x[:, :d_dp]
    join = lambda lo, n: both[:, :, lo : lo + n].transpose(1, 0, 2).reshape(d_dp, seq_n * n)
    d_w_q, d_w_k, d_w_v = join(0, q_w), join(q_w, kv_w), join(q_w + kv_w, kv_w)
    d_gains = jnp.sum(d_w_x[:, d_dp, : 2 * HD], axis=0)
    d_gq = lax.dynamic_slice_in_dim(d_gains, dp_rank * per, per)
    d_gk = lax.dynamic_slice_in_dim(d_gains, HD + dp_rank * per, per)
    d_attn_gain = jnp.sum(w_query.astype(F32) * d_w_q, axis=1) + jnp.sum(
        w_key.astype(F32) * d_w_k + w_value.astype(F32) * d_w_v, axis=1
    )
    d_w_o = jnp.sum(seq_stack(d_w_o.astype(BF)).astype(F32), axis=0)
    return (
        block_out,
        d_tokens,
        d_attn_gain,
        d_w_q * gain_a,
        d_w_k * gain_a,
        d_w_v * gain_a,
        d_gq,
        d_gk,
        d_w_o,
        d_ffn_gain,
        d_w_g * gain_f,
        d_w_u * gain_f,
        d_w_d,
    )


def body_fast(
    tokens, lengths, attn_gain, w_query, w_key, w_value, query_gain, key_gain, w_out,
    ffn_gain, w_gate, w_up, w_down, cotangent,
):
    seq_n, dp_n = 2, 16
    rank = lax.axis_index("seq")
    dp_rank = lax.axis_index("dp")
    place = jnp.stack(dp_place()).astype(jnp.int32)
    own, width = tokens.shape
    length = own * seq_n
    q_w, kv_w = H * HD // seq_n, KV * HD // seq_n
    ff_dp = w_down.shape[0]
    ff_w = ff_dp // seq_n
    ff = ff_w * dp_n
    d_dp = w_query.shape[0]
    gain_a = attn_gain.astype(F32)[:, None]
    gain_f = ffn_gain.astype(F32)[:, None]
    per = query_gain.shape[0]

    packed = ff_prep(rank, w_gate, w_up, w_down, gain_f)
    ff_full = lax.all_gather(packed, "dp", axis=0, tiled=False)

    def my_cols(w, n):
        return lax.dynamic_slice_in_dim(w, rank * n, n, 1)

    qkv_part = jnp.concatenate(
        [my_cols(w_query, q_w), my_cols(w_key, kv_w), my_cols(w_value, kv_w)], axis=1
    )
    qkv_part = (qkv_part.astype(F32) * gain_a).astype(BF)
    gains = jnp.concatenate([query_gain, key_gain])
    gains = jnp.pad(gains[None, :], ((0, 7), (0, qkv_part.shape[1] - gains.shape[0])))
    qkv_line = gather_z(jnp.concatenate([qkv_part, gains], axis=0))
    xhat_a, inv_a = unit_rms(tokens)
    low_own = xhat_a.astype(BF)
    low_other = seq_swap(low_own)
    qkv_pieces = gather_rest(qkv_line)
    g_own = cotangent.astype(BF)
    g_other = seq_swap(g_own)
    got = assemble(place, qkv_pieces)
    qkv_full = got[:, :d_dp].reshape(width, -1)
    gain_q = got[:, d_dp, :per].reshape(-1).astype(F32)
    gain_k = got[:, d_dp, per : 2 * per].reshape(-1).astype(F32)
    out_line = gather_z(after(w_out, *qkv_line))

    low_a = ordered(low_own, low_other, rank, 0).reshape(length, width)
    lin = dot(qkv_full, low_a, 0, 1)
    q_lin, k_lin = lin[:q_w], lin[q_w : q_w + kv_w]
    values = lin[q_w + kv_w :].astype(BF)
    freqs = ROPE_BASE ** (-(jnp.arange(HD // 2, dtype=F32) * (2.0 / HD)))
    angles = freqs[:, None] * jnp.arange(length, dtype=jnp.int32).astype(F32)[None, :]
    cos_tab, sin_tab = jnp.cos(angles), jnp.sin(angles)
    queries = head_prep(q_lin, gain_q, cos_tab, sin_tab, 1.0 / math.sqrt(HD))
    keys = head_prep(k_lin, gain_k, cos_tab, sin_tab, 1.0)
    place_mat = place_matrix(width)
    low_placed = dot(place_mat, low_a, 0, 1).astype(BF)
    queries, low_placed, g_other, *out_line = phase(queries, low_placed, g_other, *out_line)
    out_pieces = gather_rest(out_line)
    att_heads, lse = attn_fwd(queries, keys, values, None)
    attended = heads_to_tokens(att_heads)
    out_full = assemble(place, out_pieces).reshape(H * HD, width)
    resid = tokens + dot(attended, out_full, 0, 0)

    z, x, core = dp_place()
    half, quarter = width // 2, width // 4
    xhat_f, inv_f = unit_rms(resid)
    x_own = xhat_f.astype(BF)
    x_other = seq_swap(x_own)
    sizes = (dp_n, d_dp, ff_w)
    *wide, dx_own, out_own = ffn_core(x_own, g_own, ff_full, None, 0, *sizes)
    x_other, wide[0] = phase(x_other, wide[0])
    x_placed = dot(place_mat, jnp.concatenate([x_own, x_other], axis=0), 0, 1).astype(BF)
    x_placed, x_other = phase(x_placed, x_other)
    *wide, dx_other, out_other = ffn_core(x_other, g_other, ff_full, wide, 1, *sizes)
    hidden, d_gate, d_up = wide

    dx_send, d_gate = phase(dx_other, d_gate)
    dx_got = seq_swap(dx_send)
    g_far = mm(x_placed, d_gate, 1, 0, 2, 2, quarter, BF)
    g_far, d_up = phase(g_far, d_up)
    g_got = to_core(g_far)
    u_far = mm(x_placed, d_up, 1, 0, 2, 2, quarter, BF)
    u_far, g_got, d_gate = phase(u_far, g_got, d_gate)
    u_got = to_core(u_far)
    g_xs = mm(x_placed, d_gate, 1, 0, 1, 1, quarter, BF, g_got, 1)
    g_xs, d_up, u_got = phase(g_xs, d_up, u_got)
    g_xgot = to_x(g_xs)
    u_xs = mm(x_placed, d_up, 1, 0, 1, 1, quarter, BF, u_got, 1)
    u_xs, d_gate, d_up, g_both = phase(u_xs, d_gate, d_up, g_other)
    g_all = jnp.concatenate([g_own, g_both], axis=0)
    g_kept = mm(x_placed, d_gate, 1, 0, 0, 1, quarter, F32, g_got)
    u_kept = mm(x_placed, d_up, 1, 0, 0, 1, quarter, F32, u_got)
    vals = phase(u_xs, dx_got, g_xgot, g_kept, u_kept, g_all)
    u_xs, dx_got, g_xgot, g_kept, u_kept, g_all = vals
    u_xgot = to_x(u_xs)

    d_resid, r_low = resid_back(dx_own, dx_got, cotangent, xhat_f, inv_f)
    d_att_all = dot(out_full, r_low, 1, 1).astype(BF)
    d_att_send = lax.dynamic_slice_in_dim(d_att_all, (1 - rank) * q_w, q_w, 0)
    g_own_part, g_zs = z_parts(g_kept, g_xgot)
    d_att_send, hidden, g_own_part, *g_zs = phase(d_att_send, hidden, g_own_part, *g_zs)
    d_att_got = seq_swap(d_att_send)
    g_zgot = z_send(g_zs)
    third = ff // 6
    d_far = mm(hidden, g_all, 0, 0, (1 - core) * 3, 3, third, BF, cost=LONG)
    d_far, attended = phase(d_far, attended)
    d_got = to_core(d_far)
    att_placed = dot(place_mat, attended, 0, 0).astype(BF)
    o_far = mm(att_placed, r_low, 1, 0, 2, 2, quarter, BF)
    o_far, d_got, hidden = phase(o_far, d_got, hidden)
    o_got = to_core(o_far)
    d_sum = mm(hidden, g_all, 0, 0, core * 3, 3, third, BF, d_got).reshape(2, ff // 4, width)
    d_xs = pick(d_sum, 1 - x, 0)
    d_att_mine = lax.dynamic_slice_in_dim(d_att_all, rank * q_w, q_w, 0)
    d_att = jnp.concatenate(
        [jnp.where(rank == 0, d_att_mine, d_att_got), jnp.where(rank == 0, d_att_got, d_att_mine)],
        axis=1,
    )
    d_xs, o_got, d_att = phase(d_xs, o_got, d_att)
    o_sum = mm(att_placed, r_low, 1, 0, 0, 2, quarter, F32, o_got)
    o_xs = o_sum[quarter:].astype(BF)
    o_xs, o_sum, u_xgot = phase(o_xs, o_sum, u_xgot)

    u_own_part, u_zs = z_parts(u_kept, u_xgot)
    vals = phase(d_att, o_xs, d_xs, out_other, *u_zs, *g_zgot)
    d_att, o_xs, d_xs, out_send = vals[:4]
    d_xgot = to_x(d_xs)
    u_zgot, g_zgot = z_send(vals[4:7]), vals[7:]
    out_got = seq_swap(out_send)
    lins = (lin, lin, gain_q[:, None], gain_k[:, None], cos_tab, sin_tab)
    d_q, d_k, d_v, d_gq, d_gk = attn_bwd(queries, keys, values, d_att, att_heads, lse, None, lins)
    vals = phase(d_q, d_k, d_v, d_gq, d_gk, d_xgot, out_got, o_xs, *u_zgot)
    d_q, d_k, d_v, d_gq, d_gk, d_xgot, out_got, o_xs = vals[:8]
    o_xgot = to_x(o_xs)
    u_zgot = vals[8:]

    d_lin = jnp.concatenate([d_q, d_k, d_v], axis=0)
    d_g = jnp.concatenate([d_gq.sum(axis=(0, 2)), d_gk.sum(axis=(0, 2))])

    def with_gains(arr, gains):
        high = gains.astype(BF)
        row = jnp.concatenate([high, (gains - high.astype(F32)).astype(BF)])[None]
        return jnp.concatenate([arr, jnp.pad(row, ((0, 7), (0, arr.shape[1] - row.shape[1])))], axis=0)

    def gains_of(arr):
        row = arr[-8].astype(F32)
        return row[: 2 * HD] + row[2 * HD : 4 * HD]

    d_sum_kept = pick(d_sum, x, 0).astype(F32) + d_xgot.astype(F32)
    d_line = d_sum_kept.reshape(4, ff_w, width)
    d_own_part = pick(d_line, z, 0)
    d_zs = [pick(d_line, (z + s) % 4, 0).astype(BF) for s in (1, 2, 3)]
    d_lin, d_own_part, *d_zs = phase(d_lin, d_own_part, *d_zs)
    d_zgot = z_send(d_zs)
    d_norm_send = mm(d_lin, qkv_full, 0, 1, (1 - rank) * 2, 2, own // 2, BF, cost=LONG)
    d_norm_send, d_lin = phase(d_norm_send, d_lin)
    d_norm_got = seq_swap(d_norm_send)
    x_far = with_gains(mm(low_placed, d_lin, 1, 1, 2, 2, quarter, BF, cost=LONG), d_g)
    x_got = to_core(x_far)
    x_sum = mm(low_placed, d_lin, 1, 1, 0, 2, quarter, F32, x_got)
    d_g = d_g + gains_of(x_got)
    x_xs = with_gains(x_sum[quarter:].astype(BF), d_g)
    x_xs, o_xgot = phase(x_xs, o_xgot)
    x_xgot = to_x(x_xs)
    o_own_part, o_zs = z_parts(o_sum[:quarter], o_xgot)
    gu_end = jnp.concatenate([z_total(g_own_part, g_zgot), z_total(u_own_part, u_zgot)], axis=0)
    gu_end = gu_end.astype(BF)
    block_out = resid + out_own + out_got.astype(F32)
    vals = phase(o_own_part, *o_zs, *d_zgot)
    o_own_part, o_zgot, d_zgot = vals[0], z_send(vals[1:4]), vals[4:]
    d_norm_got, gu_end, x_xgot, block_out, *o_zgot = phase(
        d_norm_got, gu_end, x_xgot, block_out, *o_zgot
    )
    x_own_part, x_zs = z_parts(x_sum[:quarter], x_xgot[:quarter])
    d_g = d_g + gains_of(x_xgot)
    x_own_part, gu_end, *x_zs = phase(x_own_part, gu_end, *[with_gains(part, d_g) for part in x_zs])
    x_zgot = z_send(x_zs)
    gu_swap = seq_swap(gu_end)
    d_norm = mm(d_lin, qkv_full, 0, 1, rank * 2, 2, own // 2, F32, d_norm_got, cost=LONG)
    d_tokens = d_resid + unit_rms_back(d_norm, xhat_a, inv_a)
    d_end = z_total(d_own_part, d_zgot).astype(BF)
    o_end = z_total(o_own_part, o_zgot).astype(BF)
    d_tokens, d_end, o_end, *x_zgot = phase(d_tokens, d_end, o_end, *x_zgot)
    for got_s in x_zgot:
        d_g = d_g + gains_of(got_s)
    x_end = z_total(x_own_part, [got_s[:d_dp] for got_s in x_zgot]).astype(BF)
    ends = jnp.concatenate([d_end, o_end, with_gains(x_end, d_g)], axis=0)
    ends, gu_swap = phase(ends, gu_swap)
    swaps = seq_swap(ends)
    d_w_g, dg_g = ff_finish(rank, gu_end[:d_dp], gu_swap[:d_dp], w_gate, gain_f, dp_n)
    d_w_u, dg_u = ff_finish(rank, gu_end[d_dp:], gu_swap[d_dp:], w_up, gain_f, dp_n)
    d_ffn_gain = (dg_g + dg_u)[:, 0]
    d_w_d = ordered(d_end, swaps[:ff_w], rank, 0).reshape(ff_dp, width).astype(F32)
    d_w_o = o_end.astype(F32) + swaps[ff_w : ff_w + d_dp].astype(F32)
    d_gains = d_g + gains_of(swaps)
    both = ordered(x_end, swaps[ff_w + d_dp : -8], rank, 0).astype(F32)
    join = lambda lo, n: both[:, :, lo : lo + n].transpose(1, 0, 2).reshape(d_dp, seq_n * n)
    d_w_q, d_w_k, d_w_v = join(0, q_w), join(q_w, kv_w), join(q_w + kv_w, kv_w)
    d_gq = lax.dynamic_slice_in_dim(d_gains, dp_rank * per, per)
    d_gk = lax.dynamic_slice_in_dim(d_gains, HD + dp_rank * per, per)
    d_attn_gain = jnp.sum(w_query.astype(F32) * d_w_q, axis=1) + jnp.sum(
        w_key.astype(F32) * d_w_k + w_value.astype(F32) * d_w_v, axis=1
    )
    return (
        block_out,
        d_tokens,
        d_attn_gain,
        d_w_q * gain_a,
        d_w_k * gain_a,
        d_w_v * gain_a,
        d_gq,
        d_gk,
        d_w_o,
        d_ffn_gain,
        d_w_g,
        d_w_u,
        d_w_d,
    )


def body_for(*args):
    tokens, lengths = args[:2]
    sizes = (lax.axis_size("dp"), lax.axis_size("seq"))
    exact = lengths.shape[1] == 1 and tokens.shape[0] * sizes[1] == MINLEN
    return (body_fast if sizes == (16, 2) and exact else body)(*args)


def solution(mesh):
    rows, shard, vec = P(("dp", "seq"), None), P("dp", None), P("dp")
    return jax.shard_map(
        body_for,
        mesh=mesh,
        in_specs=(
            rows, shard, vec, shard, shard, shard, vec, vec, shard, vec, shard, shard, shard, rows,
        ),
        out_specs=(
            rows, rows, vec, shard, shard, shard, vec, vec, shard, vec, shard, shard, shard,
        ),
        check_vma=False,
    )
```

```python
from functools import partial
import math

import jax
import jax.numpy as jnp
from jax import lax
from jax.experimental import pallas as pl
from jax.experimental.pallas import tpu as pltpu
from jax.sharding import PartitionSpec as P

H = 16
KV = 8
HD = 64
GROUP = H // KV
MINLEN = 1024

EPSILON = 1e-05
ROPE_BASE = 1000000.0
MASKED_SCORE = -1e30
BF = jnp.bfloat16
F32 = jnp.float32


LONG = pl.CostEstimate(flops=40 << 30, transcendentals=0, bytes_accessed=96 << 20)
SHORT = pl.CostEstimate(flops=1 << 20, transcendentals=0, bytes_accessed=1 << 14)


def dot(left, right, lc, rc):
    return lax.dot_general(left, right, (((lc,), (rc,)), ((), ())), preferred_element_type=F32)


def masked(scores, q0, k0, segs):
    row = lax.broadcasted_iota(jnp.int32, scores.shape, 0) + k0
    col = lax.broadcasted_iota(jnp.int32, scores.shape, 1) + q0
    allowed = row <= col
    if segs is not None:
        allowed = allowed & (segs[0] == segs[1])
    return jnp.where(allowed, scores, MASKED_SCORE)


def attn_fwd_kernel(blk, static, *refs):
    if static:
        q_ref, k_ref, v_ref, o_ref, lse_ref = refs
    else:
        q_ref, k_ref, v_ref, sc_ref, sr_ref, o_ref, lse_ref = refs
    length = q_ref.shape[1]
    keys = k_ref[...].T

    def finish(q0, parts):
        top = parts[0][0].max(axis=0, keepdims=True)
        for s, _ in parts[1:]:
            top = jnp.maximum(top, s.max(axis=0, keepdims=True))
        total, out = 0.0, 0.0
        for s, v in parts:
            p = jnp.exp(s - top)
            total = total + p.sum(axis=0, keepdims=True)
            out = out + dot(v, p.astype(BF), 1, 0)
        o_ref[:, pl.ds(q0, blk)] = (out / total).astype(BF)
        lse_ref[0, :, pl.ds(q0, blk)] = top + jnp.log(total)

    if static:
        for qb in range(length // blk):
            q0 = qb * blk
            q = q_ref[:, q0 : q0 + blk]
            parts = []
            if qb:
                parts.append((dot(keys[:q0], q, 1, 0), v_ref[:, :q0]))
            diag = masked(dot(keys[q0 : q0 + blk], q, 1, 0), 0, 0, None)
            parts.append((diag, v_ref[:, q0 : q0 + blk]))
            finish(q0, parts)
    else:

        @pl.loop(0, length // blk)
        def _(qb):
            q0 = pl.multiple_of(qb * blk, blk)
            s = dot(keys, q_ref[:, pl.ds(q0, blk)], 1, 0)
            s = masked(s, q0, 0, (sc_ref[...], sr_ref[:, pl.ds(q0, blk)]))
            finish(q0, [(s, v_ref[...])])


def lin_back(y, lin, gain, cos_tab, sin_tab):
    first, second = y[: HD // 2], y[HD // 2 :]
    y = jnp.concatenate(
        [first * cos_tab + second * sin_tab, second * cos_tab - first * sin_tab], axis=0
    )
    inv = lax.rsqrt(jnp.mean(lin * lin, axis=0, keepdims=True) + EPSILON)
    xhat = lin * inv
    d_gain = jnp.sum(y * xhat, axis=1, keepdims=True)
    y = y * gain
    return inv * (y - xhat * jnp.mean(y * xhat, axis=0, keepdims=True)), d_gain


def attn_bwd_kernel(blk, static, *refs):
    lin_refs = None
    if static:
        q_ref, k_ref, v_ref, do_ref, o_ref, lse_ref = refs[:6]
        lin_refs = refs[6:12]
        dq_ref, dk_ref, dv_ref, dgq_ref, dgk_ref, dk_acc, dv_acc = refs[12:]
        ql_ref, kl_ref, gq_ref, gk_ref, cos_ref, sin_ref = lin_refs
    else:
        (q_ref, k_ref, v_ref, do_ref, o_ref, lse_ref, sc_ref, sr_ref,
         dq_ref, dk_ref, dv_ref, dk_acc, dv_acc) = refs
    length = q_ref.shape[1]
    member = lax.rem(pl.program_id(0), GROUP)
    keys = k_ref[...].T
    values = v_ref[...].T

    @pl.when(member == 0)
    def _():
        dk_acc[...] = jnp.zeros_like(dk_acc)
        dv_acc[...] = jnp.zeros_like(dv_acc)

    def part(q, d_out, lse, delta, k_lo, k_n, q0, segs, mask):
        rows = pl.ds(k_lo, k_n)
        k_blk, v_blk = keys[k_lo : k_lo + k_n], values[k_lo : k_lo + k_n]
        s = dot(k_blk, q, 1, 0)
        if mask:
            s = masked(s, q0, k_lo, segs)
        p = jnp.exp(s - lse)
        dv_acc[rows, :] += dot(p.astype(BF), d_out, 1, 1)
        dp = dot(v_blk, d_out, 1, 0)
        ds = (p * (dp - delta)).astype(BF)
        dk_acc[rows, :] += dot(ds, q, 1, 1)
        return dot(k_ref[:, rows], ds, 1, 0)

    def prepare(q0):
        cols = pl.ds(q0, blk)
        d_out = do_ref[:, cols]
        delta = (d_out.astype(F32) * o_ref[:, cols].astype(F32)).sum(axis=0, keepdims=True)
        return cols, q_ref[:, cols], d_out, lse_ref[0, :, cols], delta

    scale = 1.0 / math.sqrt(HD)
    if static:
        for qb in range(length // blk):
            q0 = qb * blk
            cols, q, d_out, lse, delta = prepare(q0)
            dq = part(q, d_out, lse, delta, q0, blk, q0, None, True)
            if qb:
                dq = dq + part(q, d_out, lse, delta, 0, q0, q0, None, False)
            d_lin, d_gain = lin_back(
                dq * scale, ql_ref[:, cols], gq_ref[...], cos_ref[:, cols], sin_ref[:, cols]
            )
            dq_ref[:, cols] = d_lin.astype(BF)
            dgq_ref[0] = d_gain if qb == 0 else dgq_ref[0] + d_gain
    else:

        @pl.loop(0, length // blk)
        def _(qb):
            q0 = pl.multiple_of(qb * blk, blk)
            cols, q, d_out, lse, delta = prepare(q0)
            dq = part(q, d_out, lse, delta, 0, length, q0, (sc_ref[...], sr_ref[:, cols]), True)
            dq_ref[:, cols] = (dq * scale).astype(BF)

    @pl.when(member == GROUP - 1)
    def _():
        dk = dk_acc[...].T
        if static:
            dk, d_gain = lin_back(dk, kl_ref[...], gk_ref[...], cos_ref[...], sin_ref[...])
            dgk_ref[0] = d_gain
        dk_ref[...] = dk.astype(BF)
        dv_ref[...] = dv_acc[...].T.astype(BF)


def attn_specs(length):
    q_spec = pl.BlockSpec((HD, length), lambda h: (h, 0))
    kv_spec = pl.BlockSpec((HD, length), lambda h: (h // GROUP, 0))
    lse_spec = pl.BlockSpec((1, 1, length), lambda h: (h, 0, 0))
    seg_specs = [
        pl.BlockSpec((length, 1), lambda h: (0, 0)),
        pl.BlockSpec((1, length), lambda h: (0, 0)),
    ]
    return q_spec, kv_spec, lse_spec, seg_specs


def attn_fwd(q, k, v, segs):
    rows, length = q.shape
    heads = rows // HD
    static = segs is None
    q_spec, kv_spec, lse_spec, seg_specs = attn_specs(length)
    extra = () if static else (segs[:, None], segs[None, :])
    return pl.pallas_call(
        partial(attn_fwd_kernel, min(256, length), static),
        grid=(heads,),
        in_specs=[q_spec, kv_spec, kv_spec] + ([] if static else seg_specs),
        out_specs=[q_spec, lse_spec],
        out_shape=[
            jax.ShapeDtypeStruct((rows, length), BF),
            jax.ShapeDtypeStruct((heads, 1, length), F32),
        ],
        cost_estimate=SHORT,
        name="attn_fwd",
    )(q, k, v, *extra)


def attn_bwd(q, k, v, d_out, out, lse, segs, lins=()):
    rows, length = q.shape
    heads = rows // HD
    static = segs is None
    q_spec, kv_spec, lse_spec, seg_specs = attn_specs(length)
    extra = tuple(lins) if static else (segs[:, None], segs[None, :])
    whole = lambda arr: pl.BlockSpec(arr.shape, lambda h: (0, 0))
    lin_specs = [q_spec, pl.BlockSpec((HD, length), lambda h: (heads + h // GROUP, 0))]
    lin_specs += [whole(arr) for arr in lins[2:]]
    gain_specs = [
        pl.BlockSpec((1, HD, 1), lambda h: (h, 0, 0)),
        pl.BlockSpec((1, HD, 1), lambda h: (h // GROUP, 0, 0)),
    ]
    gain_shapes = [
        jax.ShapeDtypeStruct((heads, HD, 1), F32),
        jax.ShapeDtypeStruct((heads // GROUP, HD, 1), F32),
    ]
    return pl.pallas_call(
        partial(attn_bwd_kernel, min(256, length), static),
        grid=(heads,),
        in_specs=[q_spec, kv_spec, kv_spec, q_spec, q_spec, lse_spec]
        + (lin_specs if static else seg_specs),
        out_specs=[q_spec, kv_spec, kv_spec] + (gain_specs if static else []),
        out_shape=[
            jax.ShapeDtypeStruct((rows, length), BF),
            jax.ShapeDtypeStruct(k.shape, BF),
            jax.ShapeDtypeStruct(v.shape, BF),
        ]
        + (gain_shapes if static else []),
        scratch_shapes=[pltpu.VMEM((length, HD), F32), pltpu.VMEM((length, HD), F32)],
        cost_estimate=LONG,
        name="attn_bwd",
    )(q, k, v, d_out, out, lse, *extra)


def ff_prep_kernel(rank_ref, gate_ref, up_ref, down_ref, gain_ref, out_ref):
    first = rank_ref[0] == 0
    d_dp, ff_all = gate_ref.shape
    ff_w = down_ref.shape[0] // 2
    dp_n = ff_all // (2 * ff_w)
    gain = gain_ref[...]
    for half, ref in enumerate((gate_ref, up_ref)):
        for i in range(dp_n):
            lo = ref[:, 2 * i * ff_w : (2 * i + 1) * ff_w].astype(F32)
            hi = ref[:, (2 * i + 1) * ff_w : (2 * i + 2) * ff_w].astype(F32)
            at = (half * dp_n + hidden_place(i)) * ff_w
            out_ref[:d_dp, at : at + ff_w] = (jnp.where(first, lo, hi) * gain).astype(BF)
    for b in range(ff_w // 16):
        lo = down_ref[16 * b : 16 * b + 16, :]
        hi = down_ref[ff_w + 16 * b : ff_w + 16 * b + 16, :]
        rows = jnp.where(first, lo.astype(F32), hi.astype(F32)).astype(BF)
        for band, at, frm, to in down_places(b, rows.shape[1], ff_all):
            out_ref[d_dp + 16 * band : d_dp + 16 * band + 16, at : at + to - frm] = rows[:, frm:to]


def hidden_place(i):
    return (i % 2 * 2 + i // 2 % 2) * 4 + i // 4


def down_places(b, width, ff_all):
    places, start = [], b * width
    while start < (b + 1) * width:
        band = start // ff_all
        end = min((band + 1) * ff_all, (b + 1) * width)
        places.append((band, start - band * ff_all, start - b * width, end - b * width))
        start = end
    return places


def ff_prep(rank, w_gate, w_up, w_down, gain):
    d_dp, ff_all = w_gate.shape
    bands = w_down.shape[0] // 2 * w_down.shape[1] // ff_all
    whole = lambda arr: pl.BlockSpec(arr.shape, lambda i, r: (0, 0))
    return pl.pallas_call(
        ff_prep_kernel,
        grid_spec=pltpu.PrefetchScalarGridSpec(
            num_scalar_prefetch=1,
            grid=(1,),
            in_specs=[whole(w_gate), whole(w_up), whole(w_down), whole(gain)],
            out_specs=pl.BlockSpec((d_dp + bands, ff_all), lambda i, r: (0, 0)),
        ),
        out_shape=jax.ShapeDtypeStruct((d_dp + bands, ff_all), BF),
        name="ff_prep",
    )(rank[None], w_gate, w_up, w_down, gain)


def ffn_core_kernel(sub, fresh, *refs):
    x_ref, g_ref, wg_ref, wu_ref, wd_ref = refs[:5]
    hid_ref, dg_ref, du_ref, dx_out, out_out, down, dx_ref, out_ref = refs[5:] if fresh else refs[8:]
    dp_n, d_dp, blk = wg_ref.shape
    width = g_ref.shape[1]
    ff_all = wd_ref.shape[2]
    ff_w = down.shape[0] // dp_n
    step = pl.program_id(0)

    @pl.when(step == 0)
    def _():
        dx_ref[...] = jnp.zeros_like(dx_ref)
        out_ref[...] = jnp.zeros_like(out_ref)

        @pl.loop(0, dp_n)
        def _(i):
            for b in range(ff_w // 16):
                at_i = (lax.rem(i, 2) * 2 + lax.rem(lax.div(i, 2), 2)) * 4 + lax.div(i, 4)
                rows = pl.ds(pl.multiple_of(at_i * ff_w + 16 * b, 16), 16)
                for band, at, frm, to in down_places(b, width, ff_all):
                    down[rows, frm:to] = wd_ref[i, 16 * band : 16 * band + 16, at : at + to - frm]

    @pl.loop(0, blk // sub)
    def _(s):
        cols = pl.ds(pl.multiple_of(s * sub, 128), sub)
        rows = pl.ds(pl.multiple_of(step * blk + s * sub, 128), sub)
        x = x_ref[...]
        w_gate = wg_ref[:, :, cols].reshape(dp_n * d_dp, sub)
        w_up = wu_ref[:, :, cols].reshape(dp_n * d_dp, sub)
        w_down = down[rows, :]
        gate = dot(x, w_gate, 1, 0)
        up = dot(x, w_up, 1, 0)
        d_hid = dot(g_ref[...], w_down, 1, 1)
        sig = 1.0 / (1.0 + jnp.exp(-gate))
        silu = gate * sig
        hidden = (silu * up).astype(BF)
        d_gate = (d_hid * up * (sig * (1.0 + gate * (1.0 - sig)))).astype(BF)
        d_up = (d_hid * silu).astype(BF)
        hid_ref[:, cols] = hidden
        dg_ref[:, cols] = d_gate
        du_ref[:, cols] = d_up
        dx_ref[...] += dot(d_gate, w_gate, 1, 1) + dot(d_up, w_up, 1, 1)
        out_ref[...] += dot(hidden, w_down, 1, 0)

    @pl.when(step == pl.num_programs(0) - 1)
    def _():
        dx_out[...] = dx_ref[...].astype(dx_out.dtype)
        out_out[...] = out_ref[...].astype(out_out.dtype)


def ffn_core(x, g, packed, earlier, half, dp_n, d_dp, ff_w):
    rows, width = x.shape
    ff = dp_n * ff_w
    blk = ff // 2
    fresh = earlier is None
    whole = pl.BlockSpec((rows, width), lambda j: (0, 0))
    wide = pl.BlockSpec((rows, blk), lambda j: (half, j))
    bands = packed.shape[1] - d_dp
    keep = pl.BlockSpec(memory_space=pl.ANY)
    wide_shape = jax.ShapeDtypeStruct((2 * rows, ff), BF)
    return pl.pallas_call(
        partial(ffn_core_kernel, 384, fresh),
        grid=(2,),
        in_specs=[
            whole,
            whole,
            pl.BlockSpec((dp_n, d_dp, blk), lambda j: (0, 0, j)),
            pl.BlockSpec((dp_n, d_dp, blk), lambda j: (0, 0, 2 + j)),
            pl.BlockSpec(
                (dp_n, bands, 2 * ff), lambda j: (0, d_dp // bands, 0), pipeline_mode=pl.Buffered(1)
            ),
        ]
        + ([] if fresh else [keep] * 3),
        out_specs=[wide, wide, wide, whole, whole],
        out_shape=[wide_shape] * 3
        + [jax.ShapeDtypeStruct((rows, width), F32 if fresh else BF)] * 2,
        scratch_shapes=[pltpu.VMEM((ff, width), BF)] + [pltpu.VMEM((rows, width), F32)] * 2,
        input_output_aliases={} if fresh else {5: 0, 6: 1, 7: 2},
        compiler_params=pltpu.CompilerParams(vmem_limit_bytes=60 << 20),
        cost_estimate=SHORT,
        name="ffn_core",
    )(x, g, packed, packed, packed, *(() if fresh else earlier))


def mm_kernel(lc, rc, first_ref, a_ref, b_ref, *refs):
    total = dot(a_ref[...], b_ref[...], lc, rc)
    if len(refs) == 2:
        total = total + refs[0][...].astype(F32)
    refs[-1][...] = total.astype(refs[-1].dtype)


def mm(a, b, lc, rc, first, count, rows, dtype, add=None, add_first=0, cost=SHORT):
    cols = b.shape[1 - rc]
    a_spec = (
        pl.BlockSpec((rows, a.shape[1]), lambda i, f: (f[0] + i, 0))
        if lc
        else pl.BlockSpec((a.shape[0], rows), lambda i, f: (0, f[0] + i))
    )
    in_specs = [a_spec, pl.BlockSpec(b.shape, lambda i, f: (0, 0))]
    args = [a, b]
    if add is not None:
        in_specs.append(pl.BlockSpec((rows, cols), lambda i, f: (add_first + i, 0)))
        args.append(add)
    return pl.pallas_call(
        partial(mm_kernel, lc, rc),
        grid_spec=pltpu.PrefetchScalarGridSpec(
            num_scalar_prefetch=1,
            grid=(count,),
            in_specs=in_specs,
            out_specs=pl.BlockSpec((rows, cols), lambda i, f: (i, 0)),
        ),
        out_shape=jax.ShapeDtypeStruct((count * rows, cols), dtype),
        compiler_params=pltpu.CompilerParams(vmem_limit_bytes=48 << 20),
        cost_estimate=cost,
        name="mm",
    )(jnp.asarray(first, jnp.int32)[None], *args)


def resid_back_kernel(dx_ref, got_ref, cot_ref, xhat_ref, inv_ref, out_ref, low_ref):
    y = dx_ref[...] + got_ref[...].astype(F32)
    d_resid = cot_ref[...] + unit_rms_back(y, xhat_ref[...], inv_ref[...])
    out_ref[...] = d_resid
    low_ref[...] = d_resid.astype(BF)


def resid_back(dx_own, dx_got, cotangent, xhat, inv):
    rows, width = dx_own.shape
    wide = pl.BlockSpec((rows // 4, width), lambda i: (i, 0))
    return pl.pallas_call(
        resid_back_kernel,
        grid=(4,),
        in_specs=[wide, wide, wide, wide, pl.BlockSpec((rows // 4, 1), lambda i: (i, 0))],
        out_specs=[wide, wide],
        out_shape=[
            jax.ShapeDtypeStruct((rows, width), F32),
            jax.ShapeDtypeStruct((rows, width), BF),
        ],
        cost_estimate=LONG,
        name="resid_back",
    )(dx_own, dx_got, cotangent, xhat, inv)


def ff_finish_kernel(rank_ref, mine_ref, theirs_ref, w_ref, gain_ref, out_ref, d_gain_ref):
    first = rank_ref[0] == 0
    mine, theirs = mine_ref[...].astype(F32), theirs_ref[...].astype(F32)
    low_ = jnp.where(first, mine, theirs)
    high = jnp.where(first, theirs, mine)
    gain = gain_ref[...]
    dp_n = gain_ref.shape[1]
    n = mine.shape[1] // dp_n
    total = jnp.zeros((mine.shape[0], 2 * n), F32)
    for i in range(dp_n):
        cols = slice(2 * i * n, 2 * (i + 1) * n)
        at = hidden_place(i) * n
        pair = jnp.concatenate([low_[:, at : at + n], high[:, at : at + n]], axis=1)
        total = total + pair * w_ref[:, cols].astype(F32)
        out_ref[:, cols] = pair * gain[:, :1]
    d_gain_ref[...] = total.sum(axis=1, keepdims=True)


def ff_finish(rank, mine, theirs, weight, gain, dp_n):
    gain = jnp.broadcast_to(gain, (gain.shape[0], dp_n))
    whole = lambda arr: pl.BlockSpec(arr.shape, lambda i, r: (0, 0))
    return pl.pallas_call(
        ff_finish_kernel,
        grid_spec=pltpu.PrefetchScalarGridSpec(
            num_scalar_prefetch=1,
            grid=(1,),
            in_specs=[whole(mine), whole(theirs), whole(weight), whole(gain)],
            out_specs=[
                pl.BlockSpec(weight.shape, lambda i, r: (0, 0)),
                pl.BlockSpec((weight.shape[0], 1), lambda i, r: (0, 0)),
            ],
        ),
        out_shape=[
            jax.ShapeDtypeStruct(weight.shape, F32),
            jax.ShapeDtypeStruct((weight.shape[0], 1), F32),
        ],
        name="ff_finish",
    )(rank[None], mine, theirs, weight, gain)


def assemble_kernel(place_ref, *refs):
    out_ref = refs[-1]
    rows = refs[0].shape[0]
    z, x, core = place_ref[0], place_ref[1], place_ref[2]
    for n, ref in enumerate(refs[:-1]):
        b, a, s = n // 8, n // 4 % 2, n % 4
        at = (lax.rem(z + s, 4) * 2 + (a + x - 2 * a * x)) * 2 + (b + core - 2 * b * core)
        out_ref[at] = ref[...]


def assemble(place, pieces):
    shape = pieces[0].shape
    return pl.pallas_call(
        assemble_kernel,
        grid_spec=pltpu.PrefetchScalarGridSpec(
            num_scalar_prefetch=1,
            grid=(1,),
            in_specs=[pl.BlockSpec(shape, lambda i, p: (0, 0))] * 16,
            out_specs=pl.BlockSpec((16,) + shape, lambda i, p: (0, 0, 0)),
        ),
        out_shape=jax.ShapeDtypeStruct((16,) + shape, BF),
        name="assemble",
    )(place, *pieces)


def pick(arr, index, axis):
    return lax.dynamic_index_in_dim(arr, index, axis, keepdims=False)


def ordered(mine, other, rank, axis):
    low_ = jnp.where(rank == 0, mine, other)
    high = jnp.where(rank == 0, other, mine)
    return jnp.stack([low_, high], axis=axis)


def dp_gather(shard):
    return lax.all_gather(shard, "dp", axis=0, tiled=False)


def dp_scatter(parts):
    flat = parts.reshape((-1,) + parts.shape[2:])
    return lax.psum_scatter(flat, "dp", scatter_dimension=0, tiled=True).astype(F32)


def dp_place():
    index = lax.axis_index("dp")
    return index // 4, (index // 2) % 2, index % 2


def to_core(arr):
    return lax.ppermute(arr, "dp", [(j, j ^ 1) for j in range(16)])


def to_x(arr):
    return lax.ppermute(arr, "dp", [(j, j ^ 2) for j in range(16)])


def to_z(arr, s):
    return lax.ppermute(arr, "dp", [(j, (j + 4 * s) % 16) for j in range(16)])


def gather_z(shard):
    return [shard] + [to_z(shard, 4 - s) for s in (1, 2, 3)]


def gather_rest(line):
    plane = line + [to_x(piece) for piece in line]
    return plane + [to_core(piece) for piece in plane]


def place_matrix(width):
    z, x, core = dp_place()
    n = jnp.arange(width, dtype=jnp.int32)
    part = width // 16
    block = (
        (z + n // part % 4) % 4 * 4
        + jnp.bitwise_xor(x, n // (4 * part) % 2) * 2
        + jnp.bitwise_xor(core, n // (8 * part))
    )
    source = block * part + n % part
    return (n[:, None] == source[None, :]).astype(BF)


def phase(*values):
    return lax.optimization_barrier(values)


def z_parts(kept, got):
    r = kept.shape[0] // 4
    sums = [kept[s * r : s * r + r] + got[s * r : s * r + r].astype(F32) for s in range(4)]
    return sums[0], [part.astype(BF) for part in sums[1:]]


def z_send(parts):
    return [to_z(part, s + 1) for s, part in enumerate(parts)]


def z_total(kept, got):
    total = kept
    for term in got:
        total = total + term.astype(F32)
    return total


def after(value, *others):
    return lax.optimization_barrier((value,) + tuple(others))[0]


def seq_swap(arr):
    return lax.ppermute(arr, "seq", [(0, 1), (1, 0)])


def seq_tokens(rows):
    if lax.axis_size("seq") == 2:
        return jnp.concatenate([rows, seq_swap(rows)], axis=0)
    return lax.all_gather(rows, "seq", axis=0, tiled=True)


def seq_tokens_sum(parts):
    if lax.axis_size("seq") == 2:
        own = parts.shape[0] // 2
        return parts[:own] + seq_swap(parts[own:].astype(BF)).astype(F32)
    return lax.psum_scatter(parts.astype(BF), "seq", scatter_dimension=0, tiled=True).astype(F32)


def seq_stack(arr):
    if lax.axis_size("seq") == 2:
        return ordered(arr, seq_swap(arr), lax.axis_index("seq"), 0)
    return lax.all_gather(arr, "seq", axis=0, tiled=False)


def heads_to_tokens(arr):
    count = lax.axis_size("seq")
    rows, length = arr.shape
    if count == 2:
        rank = lax.axis_index("seq")
        own = length // 2
        mine = lax.dynamic_slice_in_dim(arr, rank * own, own, 1)
        theirs = seq_swap(lax.dynamic_slice_in_dim(arr, (1 - rank) * own, own, 1))
        return ordered(mine, theirs, rank, 0).reshape(2 * rows, own)
    return lax.all_to_all(arr, "seq", split_axis=1, concat_axis=0, tiled=True)


def tokens_to_heads(arr):
    count = lax.axis_size("seq")
    rows, own = arr.shape
    if count == 2:
        rank = lax.axis_index("seq")
        half = rows // 2
        mine = lax.dynamic_slice_in_dim(arr, rank * half, half, 0)
        theirs = seq_swap(lax.dynamic_slice_in_dim(arr, (1 - rank) * half, half, 0))
        first = jnp.where(rank == 0, mine, theirs)
        second = jnp.where(rank == 0, theirs, mine)
        return jnp.concatenate([first, second], axis=1)
    return lax.all_to_all(arr, "seq", split_axis=0, concat_axis=1, tiled=True)


def pack_layout(seq_lens, total):
    places = jnp.arange(total, dtype=jnp.int32)
    ends = jnp.cumsum(seq_lens)
    starts = ends - seq_lens
    segment = jnp.sum((places[:, None] >= ends[None, :]).astype(jnp.int32), axis=1)
    starts_ext = jnp.concatenate([starts, ends[-1:]])
    labels = jnp.arange(seq_lens.shape[0] + 1, dtype=jnp.int32)
    offset = jnp.sum(jnp.where(segment[:, None] == labels[None, :], starts_ext[None, :], 0), axis=1)
    return segment, places - offset, segment < seq_lens.shape[0]


def unit_rms(values):
    inv = lax.rsqrt(jnp.mean(values * values, axis=-1, keepdims=True) + EPSILON)
    return values * inv, inv


def unit_rms_back(y, xhat, inv):
    return inv * (y - xhat * jnp.mean(y * xhat, axis=-1, keepdims=True))


def head_prep(lin, gain, cos_tab, sin_tab, scale):
    u = lin.reshape(-1, HD, lin.shape[1])
    inv = lax.rsqrt(jnp.mean(u * u, axis=1, keepdims=True) + EPSILON)
    u = u * inv * gain[None, :, None]
    first, second = u[:, : HD // 2], u[:, HD // 2 :]
    out = jnp.concatenate(
        [first * cos_tab - second * sin_tab, second * cos_tab + first * sin_tab], axis=1
    )
    return (out * scale).astype(BF).reshape(lin.shape)


def head_prep_back(grad, lin, gain, cos_tab, sin_tab):
    y = grad.astype(F32).reshape(-1, HD, lin.shape[1])
    first, second = y[:, : HD // 2], y[:, HD // 2 :]
    y = jnp.concatenate(
        [first * cos_tab + second * sin_tab, second * cos_tab - first * sin_tab], axis=1
    )
    u = lin.reshape(y.shape)
    inv = lax.rsqrt(jnp.mean(u * u, axis=1, keepdims=True) + EPSILON)
    xhat = u * inv
    d_gain = jnp.sum(y * xhat, axis=(0, 2))
    y = y * gain[None, :, None]
    d_lin = inv * (y - xhat * jnp.mean(y * xhat, axis=1, keepdims=True))
    return d_lin.astype(BF).reshape(lin.shape), d_gain


def body(
    tokens, lengths, attn_gain, w_query, w_key, w_value, query_gain, key_gain, w_out,
    ffn_gain, w_gate, w_up, w_down, cotangent,
):
    seq_n = lax.axis_size("seq")
    dp_n = lax.axis_size("dp")
    rank = lax.axis_index("seq")
    dp_rank = lax.axis_index("dp")
    own, width = tokens.shape
    length = own * seq_n
    q_w, kv_w = H * HD // seq_n, KV * HD // seq_n
    ff_dp = w_down.shape[0]
    ff_w = ff_dp // seq_n
    ff = ff_w * dp_n
    d_dp = w_query.shape[0]

    full = length == MINLEN * lengths.shape[1]
    segment, positions, valid = pack_layout(lengths[0], length)
    segs = None if full and lengths.shape[1] == 1 else segment
    my_valid = lax.dynamic_slice_in_dim(valid, rank * own, own).astype(F32)[:, None]

    def keep_valid(arr):
        return arr if full else arr * my_valid

    gain_a = attn_gain.astype(F32)[:, None]
    gain_f = ffn_gain.astype(F32)[:, None]

    def my_cols(w, n):
        return lax.dynamic_slice_in_dim(w, rank * n, n, 1)

    qkv_part = jnp.concatenate(
        [my_cols(w_query, q_w), my_cols(w_key, kv_w), my_cols(w_value, kv_w)], axis=1
    )
    qkv_part = (qkv_part.astype(F32) * gain_a).astype(BF)
    gains = jnp.concatenate([query_gain, key_gain])
    gains = jnp.pad(gains[None, :], ((0, 7), (0, qkv_part.shape[1] - gains.shape[0])))
    pick_ff = lambda w: pick(w.reshape(d_dp, dp_n, seq_n, ff_w), rank, 2).reshape(d_dp, ff)
    gu_part = jnp.concatenate([pick_ff(w_gate), pick_ff(w_up)], axis=1)
    gu_part = (gu_part.astype(F32) * gain_f).astype(BF)
    down_part = pick(w_down.reshape(seq_n, ff_w, width), rank, 0)

    gu_full = lax.all_gather(gu_part, "dp", axis=0, tiled=True)
    down_full = lax.all_gather(down_part, "dp", axis=0, tiled=True)
    got = dp_gather(jnp.concatenate([qkv_part, gains], axis=0))
    qkv_full = got[:, :d_dp].reshape(width, -1)
    per = query_gain.shape[0]
    gain_q = got[:, d_dp, :per].reshape(-1).astype(F32)
    gain_k = got[:, d_dp, per : 2 * per].reshape(-1).astype(F32)
    out_full = dp_gather(w_out).reshape(H * HD, width)

    xhat_a, inv_a = unit_rms(tokens)
    low_own = xhat_a.astype(BF)
    if seq_n == 2:
        low_a = ordered(low_own, seq_swap(low_own), rank, 0).reshape(length, width)
    else:
        low_a = lax.all_gather(low_own, "seq", axis=0, tiled=True)
    lin = dot(qkv_full, low_a, 0, 1)
    q_lin, k_lin = lin[:q_w], lin[q_w : q_w + kv_w]
    values = lin[q_w + kv_w :].astype(BF)
    freqs = ROPE_BASE ** (-(jnp.arange(HD // 2, dtype=F32) * (2.0 / HD)))
    angles = freqs[:, None] * positions.astype(F32)[None, :]
    cos_tab, sin_tab = jnp.cos(angles), jnp.sin(angles)
    queries = head_prep(q_lin, gain_q, cos_tab, sin_tab, 1.0 / math.sqrt(HD))
    keys = head_prep(k_lin, gain_k, cos_tab, sin_tab, 1.0)
    att_heads, lse = attn_fwd(queries, keys, values, segs)
    attended = heads_to_tokens(att_heads)
    resid = tokens + dot(attended, out_full, 0, 0)

    xhat_f, inv_f = unit_rms(resid)
    grad = keep_valid(cotangent)
    x_all = seq_tokens(xhat_f.astype(BF))
    g_all = seq_tokens(grad.astype(BF))
    gate = dot(x_all, gu_full[:, :ff], 1, 0)
    up = dot(x_all, gu_full[:, ff:], 1, 0)
    d_hidden = dot(g_all, down_full, 1, 1)
    sig = jax.nn.sigmoid(gate)
    silu = gate * sig
    hidden = (silu * up).astype(BF)
    d_gate = (d_hidden * up * sig * (1.0 + gate * (1.0 - sig))).astype(BF)
    d_up = (d_hidden * silu).astype(BF)
    d_ffn = dot(d_gate, gu_full[:, :ff], 1, 1) + dot(d_up, gu_full[:, ff:], 1, 1)
    d_ffn = seq_tokens_sum(d_ffn)
    d_resid = grad + unit_rms_back(d_ffn, xhat_f, inv_f)

    block_out = keep_valid(resid + seq_tokens_sum(dot(hidden, down_full, 1, 0)))
    d_w_g = dp_scatter(dot(x_all, d_gate, 0, 0).astype(BF).reshape(dp_n, d_dp, ff))
    d_w_u = dp_scatter(dot(x_all, d_up, 0, 0).astype(BF).reshape(dp_n, d_dp, ff))
    d_w_d = dp_scatter(dot(hidden, g_all, 0, 0).astype(BF).reshape(dp_n, ff_w, width))

    def full_ff(shard):
        both = seq_stack(shard.astype(BF)).reshape(seq_n, d_dp, dp_n, ff_w)
        return both.transpose(1, 2, 0, 3).reshape(d_dp, dp_n * seq_n * ff_w).astype(F32)

    d_w_g, d_w_u = full_ff(d_w_g), full_ff(d_w_u)
    d_w_d = seq_stack(d_w_d.astype(BF)).reshape(ff_dp, width).astype(F32)
    d_ffn_gain = jnp.sum(w_gate.astype(F32) * d_w_g + w_up.astype(F32) * d_w_u, axis=1)

    r_low = d_resid.astype(BF)
    d_att = tokens_to_heads(dot(out_full, r_low, 1, 1).astype(BF))
    d_w_o = dp_scatter(dot(attended, r_low, 1, 0).astype(BF).reshape(dp_n, d_dp, width))
    if segs is None:
        lins = (lin, lin, gain_q[:, None], gain_k[:, None], cos_tab, sin_tab)
        d_q, d_k, d_v, d_gq, d_gk = attn_bwd(queries, keys, values, d_att, att_heads, lse, None, lins)
        d_gq, d_gk = d_gq.sum(axis=(0, 2)), d_gk.sum(axis=(0, 2))
    else:
        d_q, d_k, d_v = attn_bwd(queries, keys, values, d_att, att_heads, lse, segs)
        d_q, d_gq = head_prep_back(d_q, q_lin, gain_q, cos_tab, sin_tab)
        d_k, d_gk = head_prep_back(d_k, k_lin, gain_k, cos_tab, sin_tab)
    d_lin = jnp.concatenate([d_q, d_k, d_v], axis=0)
    d_norm = dot(d_lin, qkv_full, 0, 1)
    if seq_n == 2:
        other = lax.dynamic_slice_in_dim(d_norm, (1 - rank) * own, own, 0)
        d_norm = lax.dynamic_slice_in_dim(d_norm, rank * own, own, 0)
        d_norm = d_norm + seq_swap(other.astype(BF)).astype(F32)
    else:
        d_norm = seq_tokens_sum(d_norm)
    d_tokens = d_resid + unit_rms_back(d_norm, xhat_a, inv_a)

    d_w_x = dot(low_a, d_lin, 0, 1).astype(BF).reshape(dp_n, d_dp, -1)
    d_g = jnp.concatenate([d_gq, d_gk]).astype(BF)
    d_g = jnp.pad(d_g[None, :], ((0, 7), (0, d_w_x.shape[2] - d_g.shape[0])))
    d_g = jnp.broadcast_to(d_g[None], (dp_n,) + d_g.shape)
    d_w_x = dp_scatter(jnp.concatenate([d_w_x, d_g], axis=1))
    d_w_x = seq_stack(d_w_x.astype(BF)).astype(F32)
    both = d_w_x[:, :d_dp]
    join = lambda lo, n: both[:, :, lo : lo + n].transpose(1, 0, 2).reshape(d_dp, seq_n * n)
    d_w_q, d_w_k, d_w_v = join(0, q_w), join(q_w, kv_w), join(q_w + kv_w, kv_w)
    d_gains = jnp.sum(d_w_x[:, d_dp, : 2 * HD], axis=0)
    d_gq = lax.dynamic_slice_in_dim(d_gains, dp_rank * per, per)
    d_gk = lax.dynamic_slice_in_dim(d_gains, HD + dp_rank * per, per)
    d_attn_gain = jnp.sum(w_query.astype(F32) * d_w_q, axis=1) + jnp.sum(
        w_key.astype(F32) * d_w_k + w_value.astype(F32) * d_w_v, axis=1
    )
    d_w_o = jnp.sum(seq_stack(d_w_o.astype(BF)).astype(F32), axis=0)
    return (
        block_out,
        d_tokens,
        d_attn_gain,
        d_w_q * gain_a,
        d_w_k * gain_a,
        d_w_v * gain_a,
        d_gq,
        d_gk,
        d_w_o,
        d_ffn_gain,
        d_w_g * gain_f,
        d_w_u * gain_f,
        d_w_d,
    )


def body_fast(
    tokens, lengths, attn_gain, w_query, w_key, w_value, query_gain, key_gain, w_out,
    ffn_gain, w_gate, w_up, w_down, cotangent,
):
    seq_n, dp_n = 2, 16
    rank = lax.axis_index("seq")
    dp_rank = lax.axis_index("dp")
    place = jnp.stack(dp_place()).astype(jnp.int32)
    own, width = tokens.shape
    length = own * seq_n
    q_w, kv_w = H * HD // seq_n, KV * HD // seq_n
    ff_dp = w_down.shape[0]
    ff_w = ff_dp // seq_n
    ff = ff_w * dp_n
    d_dp = w_query.shape[0]
    gain_a = attn_gain.astype(F32)[:, None]
    gain_f = ffn_gain.astype(F32)[:, None]
    per = query_gain.shape[0]

    packed = ff_prep(rank, w_gate, w_up, w_down, gain_f)
    ff_full = lax.all_gather(packed, "dp", axis=0, tiled=False)

    def my_cols(w, n):
        return lax.dynamic_slice_in_dim(w, rank * n, n, 1)

    qkv_part = jnp.concatenate(
        [my_cols(w_query, q_w), my_cols(w_key, kv_w), my_cols(w_value, kv_w)], axis=1
    )
    qkv_part = (qkv_part.astype(F32) * gain_a).astype(BF)
    gains = jnp.concatenate([query_gain, key_gain])
    gains = jnp.pad(gains[None, :], ((0, 7), (0, qkv_part.shape[1] - gains.shape[0])))
    qkv_line = gather_z(jnp.concatenate([qkv_part, gains], axis=0))
    xhat_a, inv_a = unit_rms(tokens)
    low_own = xhat_a.astype(BF)
    low_other = seq_swap(low_own)
    qkv_pieces = gather_rest(qkv_line)
    g_own = cotangent.astype(BF)
    g_other = seq_swap(g_own)
    got = assemble(place, qkv_pieces)
    qkv_full = got[:, :d_dp].reshape(width, -1)
    gain_q = got[:, d_dp, :per].reshape(-1).astype(F32)
    gain_k = got[:, d_dp, per : 2 * per].reshape(-1).astype(F32)
    out_line = gather_z(after(w_out, *qkv_line))

    low_a = ordered(low_own, low_other, rank, 0).reshape(length, width)
    lin = dot(qkv_full, low_a, 0, 1)
    q_lin, k_lin = lin[:q_w], lin[q_w : q_w + kv_w]
    values = lin[q_w + kv_w :].astype(BF)
    freqs = ROPE_BASE ** (-(jnp.arange(HD // 2, dtype=F32) * (2.0 / HD)))
    angles = freqs[:, None] * jnp.arange(length, dtype=jnp.int32).astype(F32)[None, :]
    cos_tab, sin_tab = jnp.cos(angles), jnp.sin(angles)
    queries = head_prep(q_lin, gain_q, cos_tab, sin_tab, 1.0 / math.sqrt(HD))
    keys = head_prep(k_lin, gain_k, cos_tab, sin_tab, 1.0)
    place_mat = place_matrix(width)
    low_placed = dot(place_mat, low_a, 0, 1).astype(BF)
    queries, low_placed, g_other, *out_line = phase(queries, low_placed, g_other, *out_line)
    out_pieces = gather_rest(out_line)
    att_heads, lse = attn_fwd(queries, keys, values, None)
    attended = heads_to_tokens(att_heads)
    out_full = assemble(place, out_pieces).reshape(H * HD, width)
    resid = tokens + dot(attended, out_full, 0, 0)

    z, x, core = dp_place()
    half, quarter = width // 2, width // 4
    xhat_f, inv_f = unit_rms(resid)
    x_own = xhat_f.astype(BF)
    x_other = seq_swap(x_own)
    sizes = (dp_n, d_dp, ff_w)
    *wide, dx_own, out_own = ffn_core(x_own, g_own, ff_full, None, 0, *sizes)
    x_other, wide[0] = phase(x_other, wide[0])
    x_placed = dot(place_mat, jnp.concatenate([x_own, x_other], axis=0), 0, 1).astype(BF)
    x_placed, x_other = phase(x_placed, x_other)
    *wide, dx_other, out_other = ffn_core(x_other, g_other, ff_full, wide, 1, *sizes)
    hidden, d_gate, d_up = wide

    dx_send, d_gate = phase(dx_other, d_gate)
    dx_got = seq_swap(dx_send)
    g_far = mm(x_placed, d_gate, 1, 0, 2, 2, quarter, BF)
    g_far, d_up = phase(g_far, d_up)
    g_got = to_core(g_far)
    u_far = mm(x_placed, d_up, 1, 0, 2, 2, quarter, BF)
    u_far, g_got, d_gate = phase(u_far, g_got, d_gate)
    u_got = to_core(u_far)
    g_xs = mm(x_placed, d_gate, 1, 0, 1, 1, quarter, BF, g_got, 1)
    g_xs, d_up, u_got = phase(g_xs, d_up, u_got)
    g_xgot = to_x(g_xs)
    u_xs = mm(x_placed, d_up, 1, 0, 1, 1, quarter, BF, u_got, 1)
    u_xs, d_gate, d_up, g_both = phase(u_xs, d_gate, d_up, g_other)
    g_all = jnp.concatenate([g_own, g_both], axis=0)
    g_kept = mm(x_placed, d_gate, 1, 0, 0, 1, quarter, F32, g_got)
    u_kept = mm(x_placed, d_up, 1, 0, 0, 1, quarter, F32, u_got)
    vals = phase(u_xs, dx_got, g_xgot, g_kept, u_kept, g_all)
    u_xs, dx_got, g_xgot, g_kept, u_kept, g_all = vals
    u_xgot = to_x(u_xs)

    d_resid, r_low = resid_back(dx_own, dx_got, cotangent, xhat_f, inv_f)
    d_att_all = dot(out_full, r_low, 1, 1).astype(BF)
    d_att_send = lax.dynamic_slice_in_dim(d_att_all, (1 - rank) * q_w, q_w, 0)
    g_own_part, g_zs = z_parts(g_kept, g_xgot)
    d_att_send, hidden, g_own_part, *g_zs = phase(d_att_send, hidden, g_own_part, *g_zs)
    d_att_got = seq_swap(d_att_send)
    g_zgot = z_send(g_zs)
    third = ff // 6
    d_far = mm(hidden, g_all, 0, 0, (1 - core) * 3, 3, third, BF, cost=LONG)
    d_far, attended = phase(d_far, attended)
    d_got = to_core(d_far)
    att_placed = dot(place_mat, attended, 0, 0).astype(BF)
    o_far = mm(att_placed, r_low, 1, 0, 2, 2, quarter, BF)
    o_far, d_got, hidden = phase(o_far, d_got, hidden)
    o_got = to_core(o_far)
    d_sum = mm(hidden, g_all, 0, 0, core * 3, 3, third, BF, d_got).reshape(2, ff // 4, width)
    d_xs = pick(d_sum, 1 - x, 0)
    d_att_mine = lax.dynamic_slice_in_dim(d_att_all, rank * q_w, q_w, 0)
    d_att = jnp.concatenate(
        [jnp.where(rank == 0, d_att_mine, d_att_got), jnp.where(rank == 0, d_att_got, d_att_mine)],
        axis=1,
    )
    d_xs, o_got, d_att = phase(d_xs, o_got, d_att)
    o_sum = mm(att_placed, r_low, 1, 0, 0, 2, quarter, F32, o_got)
    o_xs = o_sum[quarter:].astype(BF)
    o_xs, o_sum, u_xgot = phase(o_xs, o_sum, u_xgot)

    u_own_part, u_zs = z_parts(u_kept, u_xgot)
    vals = phase(d_att, o_xs, d_xs, out_other, *u_zs, *g_zgot)
    d_att, o_xs, d_xs, out_send = vals[:4]
    d_xgot = to_x(d_xs)
    u_zgot, g_zgot = z_send(vals[4:7]), vals[7:]
    out_got = seq_swap(out_send)
    lins = (lin, lin, gain_q[:, None], gain_k[:, None], cos_tab, sin_tab)
    d_q, d_k, d_v, d_gq, d_gk = attn_bwd(queries, keys, values, d_att, att_heads, lse, None, lins)
    vals = phase(d_q, d_k, d_v, d_gq, d_gk, d_xgot, out_got, o_xs, *u_zgot)
    d_q, d_k, d_v, d_gq, d_gk, d_xgot, out_got, o_xs = vals[:8]
    o_xgot = to_x(o_xs)
    u_zgot = vals[8:]

    d_lin = jnp.concatenate([d_q, d_k, d_v], axis=0)
    d_g = jnp.concatenate([d_gq.sum(axis=(0, 2)), d_gk.sum(axis=(0, 2))])

    def with_gains(arr, gains):
        high = gains.astype(BF)
        row = jnp.concatenate([high, (gains - high.astype(F32)).astype(BF)])[None]
        return jnp.concatenate([arr, jnp.pad(row, ((0, 7), (0, arr.shape[1] - row.shape[1])))], axis=0)

    def gains_of(arr):
        row = arr[-8].astype(F32)
        return row[: 2 * HD] + row[2 * HD : 4 * HD]

    d_sum_kept = pick(d_sum, x, 0).astype(F32) + d_xgot.astype(F32)
    d_line = d_sum_kept.reshape(4, ff_w, width)
    d_own_part = pick(d_line, z, 0)
    d_zs = [pick(d_line, (z + s) % 4, 0).astype(BF) for s in (1, 2, 3)]
    d_lin, d_own_part, *d_zs = phase(d_lin, d_own_part, *d_zs)
    d_zgot = z_send(d_zs)
    d_norm_send = mm(d_lin, qkv_full, 0, 1, (1 - rank) * 2, 2, own // 2, BF, cost=LONG)
    d_norm_send, d_lin = phase(d_norm_send, d_lin)
    d_norm_got = seq_swap(d_norm_send)
    x_far = with_gains(mm(low_placed, d_lin, 1, 1, 2, 2, quarter, BF, cost=LONG), d_g)
    x_got = to_core(x_far)
    x_sum = mm(low_placed, d_lin, 1, 1, 0, 2, quarter, F32, x_got)
    d_g = d_g + gains_of(x_got)
    x_xs = with_gains(x_sum[quarter:].astype(BF), d_g)
    x_xs, o_xgot = phase(x_xs, o_xgot)
    x_xgot = to_x(x_xs)
    o_own_part, o_zs = z_parts(o_sum[:quarter], o_xgot)
    gu_end = jnp.concatenate([z_total(g_own_part, g_zgot), z_total(u_own_part, u_zgot)], axis=0)
    gu_end = gu_end.astype(BF)
    block_out = resid + out_own + out_got.astype(F32)
    vals = phase(o_own_part, *o_zs, *d_zgot)
    o_own_part, o_zgot, d_zgot = vals[0], z_send(vals[1:4]), vals[4:]
    d_norm_got, gu_end, x_xgot, block_out, *o_zgot = phase(
        d_norm_got, gu_end, x_xgot, block_out, *o_zgot
    )
    x_own_part, x_zs = z_parts(x_sum[:quarter], x_xgot[:quarter])
    d_g = d_g + gains_of(x_xgot)
    x_zs = [with_gains(part, d_g) for part in x_zs]
    x_own_part, d_norm_got, *x_zs = phase(x_own_part, d_norm_got, *x_zs)
    x_zgot = z_send(x_zs)
    gu_swap = seq_swap(gu_end)
    d_norm = mm(d_lin, qkv_full, 0, 1, rank * 2, 2, own // 2, F32, d_norm_got, cost=LONG)
    d_tokens = d_resid + unit_rms_back(d_norm, xhat_a, inv_a)
    d_end = z_total(d_own_part, d_zgot).astype(BF)
    o_end = z_total(o_own_part, o_zgot).astype(BF)
    d_tokens, d_end, o_end, *x_zgot = phase(d_tokens, d_end, o_end, *x_zgot)
    for got_s in x_zgot:
        d_g = d_g + gains_of(got_s)
    x_end = z_total(x_own_part, [got_s[:d_dp] for got_s in x_zgot]).astype(BF)
    ends = jnp.concatenate([d_end, o_end, with_gains(x_end, d_g)], axis=0)
    ends, gu_swap = phase(ends, gu_swap)
    swaps = seq_swap(ends)
    d_w_g, dg_g = ff_finish(rank, gu_end[:d_dp], gu_swap[:d_dp], w_gate, gain_f, dp_n)
    d_w_u, dg_u = ff_finish(rank, gu_end[d_dp:], gu_swap[d_dp:], w_up, gain_f, dp_n)
    d_ffn_gain = (dg_g + dg_u)[:, 0]
    d_w_d = ordered(d_end, swaps[:ff_w], rank, 0).reshape(ff_dp, width).astype(F32)
    d_w_o = o_end.astype(F32) + swaps[ff_w : ff_w + d_dp].astype(F32)
    d_gains = d_g + gains_of(swaps)
    both = ordered(x_end, swaps[ff_w + d_dp : -8], rank, 0).astype(F32)
    join = lambda lo, n: both[:, :, lo : lo + n].transpose(1, 0, 2).reshape(d_dp, seq_n * n)
    d_w_q, d_w_k, d_w_v = join(0, q_w), join(q_w, kv_w), join(q_w + kv_w, kv_w)
    d_gq = lax.dynamic_slice_in_dim(d_gains, dp_rank * per, per)
    d_gk = lax.dynamic_slice_in_dim(d_gains, HD + dp_rank * per, per)
    d_attn_gain = jnp.sum(w_query.astype(F32) * d_w_q, axis=1) + jnp.sum(
        w_key.astype(F32) * d_w_k + w_value.astype(F32) * d_w_v, axis=1
    )
    return (
        block_out,
        d_tokens,
        d_attn_gain,
        d_w_q * gain_a,
        d_w_k * gain_a,
        d_w_v * gain_a,
        d_gq,
        d_gk,
        d_w_o,
        d_ffn_gain,
        d_w_g,
        d_w_u,
        d_w_d,
    )


def body_for(*args):
    tokens, lengths = args[:2]
    sizes = (lax.axis_size("dp"), lax.axis_size("seq"))
    exact = lengths.shape[1] == 1 and tokens.shape[0] * sizes[1] == MINLEN
    return (body_fast if sizes == (16, 2) and exact else body)(*args)


def solution(mesh):
    rows, shard, vec = P(("dp", "seq"), None), P("dp", None), P("dp")
    return jax.shard_map(
        body_for,
        mesh=mesh,
        in_specs=(
            rows, shard, vec, shard, shard, shard, vec, vec, shard, vec, shard, shard, shard, rows,
        ),
        out_specs=(
            rows, rows, vec, shard, shard, shard, vec, vec, shard, vec, shard, shard, shard,
        ),
        check_vma=False,
    )
```
